32 devices in a mesh: dp: 8 (over y, x, core), tensor: 4 (over z).
Axes of the slice: x: 2, y: 2, z: 4, core: 2. Of those that a mesh axis runs over, the one named last changes fastest.
Arguments:
- block_input: float32 [16384, 768], P(('dp', 'tensor'))
- cotangent: float32 [16384, 768], P(('dp', 'tensor')), may hold values from -6 to 6
- segment_ids: int32 [16384], P('dp'), may hold values from 0 to 2047, as said below
- token_offset: int32 [16384], P('dp'), may hold values from 0 to 2047, as said below
- first_gain: float32 [768], P(('dp', 'tensor')), may hold values from 0.1 to 1.9
- first_shift: float32 [768], P(('dp', 'tensor')), may hold values from -3 to 3
- second_gain: float32 [768], P(('dp', 'tensor')), may hold values from 0.1 to 1.9
- second_shift: float32 [768], P(('dp', 'tensor')), may hold values from -3 to 3
- qkv_weight: bfloat16 [3, 768, 768], P(None, 'dp', 'tensor')
- qkv_bias: bfloat16 [3, 768], P(None, ('tensor', 'dp')), may hold values from -3 to 3
- proj_weight: bfloat16 [768, 768], P('tensor', 'dp'), may hold values from -0.875 to 0.875
- up_weight: bfloat16 [768, 3072], P('dp', 'tensor'), may hold values from -0.21875 to 0.21875
- up_bias: bfloat16 [3072], P(('tensor', 'dp')), may hold values from -3 to 3
- down_weight: bfloat16 [3072, 768], P('tensor', 'dp'), may hold values from -0.109375 to 0.109375
- out_bias: float32 [768], P(('dp', 'tensor')), may hold values from -3 to 3
Outputs:
- block_output: float32 [16384, 768], P(('dp', 'tensor'))
- input_grad: float32 [16384, 768], P(('dp', 'tensor'))
- first_gain_grad: float32 [768], P(('dp', 'tensor'))
- first_shift_grad: float32 [768], P(('dp', 'tensor'))
- second_gain_grad: float32 [768], P(('dp', 'tensor'))
- second_shift_grad: float32 [768], P(('dp', 'tensor'))
- qkv_weight_grad: float32 [3, 768, 768], P(None, 'dp', 'tensor')
- qkv_bias_grad: float32 [3, 768], P(None, ('tensor', 'dp'))
- proj_weight_grad: float32 [768, 768], P('tensor', 'dp')
- up_weight_grad: float32 [768, 3072], P('dp', 'tensor')
- up_bias_grad: float32 [3072], P(('tensor', 'dp'))
- down_weight_grad: float32 [3072, 768], P('tensor', 'dp')
- out_bias_grad: float32 [768], P(('dp', 'tensor'))
The draws below stay inside these ranges and needn't reach their ends.
Inputs may be any that keep to these rules, and one draw needn't show every extreme that they name: `segment_ids`: within each block of 2048 tokens of one index of dp, segment numbers start at 0 and rise by one where a new sequence begins; in every draw some block holds one sequence and some other block gives every token a sequence of its own. `token_offset`: 0 at a sequence's first token, one more than the previous token's otherwise; in every draw some block of 2048 tokens holds one sequence.
All inputs are finite; a program needn't handle non-finite values.
Results may differ from the reference program's by a relative error of at most 0.009.
Values may be sent and summed in bfloat16 or wider, within the bound.
A program may use at most 192 MiB of HBM per device.

```python
import jax
import jax.numpy as jnp
from jax import lax

D = 768
H = 12
HD = 64
FF = 3072
ROT = 16
TOK_DEV = 2048
TOKENS = 16384


def documents(key):
    groups = TOKENS // TOK_DEV
    level_key, cut_key, whole_key, other_key = jax.random.split(jax.random.fold_in(key, 5), 4)
    level = jax.random.randint(level_key, (groups, 1), 3, 13)
    draws = jax.random.randint(cut_key, (groups, TOK_DEV), 0, 1 << 20)
    limit = jnp.left_shift(jnp.ones_like(level), 20 - level)
    position = jnp.arange(TOK_DEV, dtype=jnp.int32)[None, :]
    chosen = jax.random.randint(whole_key, (), 0, groups)
    other = (chosen + 1 + jax.random.randint(other_key, (), 0, groups - 1)) % groups
    numbers = jnp.arange(groups, dtype=jnp.int32)
    single = (numbers == chosen)[:, None]
    scattered = (numbers == other)[:, None]
    starts = (draws < limit) & jnp.logical_not(single) | scattered | (position == 0)
    segment = jnp.cumsum(starts.astype(jnp.int32), axis=1) - 1
    begin = lax.cummax(jnp.where(starts, position, 0), axis=1)
    return (segment.reshape(-1).astype(jnp.int32), (position - begin).reshape(-1).astype(jnp.int32))


def draw_segment_ids(key, part):
    return documents(key)[0]


def draw_token_offset(key, part):
    return documents(key)[1]


def draw_block_input(key, part):
    base = jax.random.normal(jax.random.fold_in(key, 1), (TOKENS, D), jnp.float32)
    return base


def draw_qkv_weight(key, part):
    return (jax.random.normal(jax.random.fold_in(key, 3), (3, D, D), jnp.float32) * D ** (-0.5)).astype(jnp.bfloat16)


def spiked(entries, own_key, source, target, shards_of, factor):
    def block_of(axis_at):
        return (jnp.arange(entries.shape[axis_at]) // (entries.shape[axis_at] // shards_of)).reshape((-1,) + (1,) * (entries.ndim - 1 - axis_at))

    first = jax.random.permutation(own_key, shards_of)[block_of(target)]
    second = (block_of(target) + shards_of // 2) % shards_of
    return jnp.where((block_of(source) == first) | (block_of(source) == second), factor * entries, entries)


def shard_levels(stream_key, shape, shards, low, high):
    def one(dim, parts):
        steps = jax.random.uniform(jax.random.fold_in(jax.random.fold_in(stream_key, 6), dim), (parts,), jnp.float32, low / len(shards), high / len(shards))
        return jnp.repeat(jnp.exp(steps), shape[dim] // parts).reshape((-1,) + (1,) * (len(shape) - dim - 1))

    level = one(*shards[0])
    for cut in shards[1:]:
        level = level * one(*cut)
    return level


def centred(stream_key, shape, deviation, bound, cuts=(), kind=jnp.bfloat16):
    array = jax.random.normal(stream_key, shape, jnp.float32) * deviation
    if len(cuts) > 0:
        array = shard_levels(stream_key, shape, cuts, -0.22, 0.18) * array
    return jnp.clip(array, min=-bound, max=bound).astype(kind)


def gaussian_with(rng, dims, deviation, reach, cuts, heavy, held_as=jnp.bfloat16):
    array = deviation * jax.random.normal(rng, dims, jnp.float32)
    if cuts:
        array = array * shard_levels(rng, dims, cuts, -0.22, 0.18)
    return jnp.clip(spiked(array, jax.random.fold_in(rng, 3), *heavy), -reach, reach).astype(held_as)


def setup_inputs(seed: int = 0) -> dict:
    arg_keys = jax.random.split(jax.random.key(seed), 16)
    return {
        "block_input": draw_block_input(jax.random.fold_in(arg_keys[15], 71), 0),
        "cotangent": gaussian_with(arg_keys[1], (TOKENS, D), 1.0, 6.0, ((0, 32),), (0, 1, 32, 2.75), jnp.float32),
        "segment_ids": draw_segment_ids(jax.random.fold_in(arg_keys[15], 71), 0),
        "token_offset": draw_token_offset(jax.random.fold_in(arg_keys[15], 71), 0),
        "first_gain": jnp.clip(1.0 + 0.18 * jax.random.normal(arg_keys[4], (D,), jnp.float32), 0.1, 1.9),
        "first_shift": centred(arg_keys[5], (D,), 0.5, 3.0, ((0, 32),), jnp.float32),
        "second_gain": jnp.clip(1.0 + 0.18 * jax.random.normal(arg_keys[6], (D,), jnp.float32), 0.1, 1.9),
        "second_shift": centred(arg_keys[7], (D,), 0.5, 3.0, ((0, 32),), jnp.float32),
        "qkv_weight": draw_qkv_weight(jax.random.fold_in(arg_keys[15], 71), 0),
        "qkv_bias": centred(arg_keys[9], (3, D), 0.5, 3.0, ((1, 32),)),
        "proj_weight": centred(arg_keys[10], (D, D), (D // 16) ** -0.5, 0.875, ((0, 4), (1, 8))),
        "up_weight": centred(arg_keys[11], (D, FF), D ** -0.5, 0.21875, ((0, 8), (1, 4))),
        "up_bias": centred(arg_keys[12], (FF,), 0.5, 3.0, ((0, 32),)),
        "down_weight": centred(arg_keys[13], (FF, D), FF ** -0.5, 0.109375, ((0, 4), (1, 8))),
        "out_bias": centred(arg_keys[14], (D,), 0.5, 3.0, ((0, 32),), jnp.float32),
    }


EPSILON = 1e-05
NEGATIVE = -1e+30

def widen(values):
    return lax.optimization_barrier(values.astype(jnp.bfloat16)).astype(jnp.float32)

def gelu_exact(values):
    return 0.5 * values * (1.0 + jax.scipy.special.erf(values * 0.7071067811865476))

def gelu_slope(values):
    return 0.5 * (1.0 + jax.scipy.special.erf(values * 0.7071067811865476)) + values * jnp.exp(-0.5 * values * values) * 0.3989422804014327

def norm_rows(rows, gain, shift):
    center = rows - lax.optimization_barrier(jnp.mean(rows, axis=1, keepdims=True))
    inverse = lax.rsqrt(lax.optimization_barrier(jnp.mean(center * center, axis=1, keepdims=True)) + EPSILON)
    normal = center * inverse
    return (normal, inverse, normal * gain + shift)

def norm_back(grad_out, normal, inverse, gain):
    scaled = grad_out * gain
    return inverse * (scaled - lax.optimization_barrier(jnp.mean(scaled, axis=1, keepdims=True)) - normal * lax.optimization_barrier(jnp.mean(scaled * normal, axis=1, keepdims=True)))

def rotary_tables(offsets):
    half = ROT // 2
    freq = 10000.0 ** (-(2.0 * jnp.arange(half, dtype=jnp.float32)) / ROT)
    angles = offsets.astype(jnp.float32)[:, None] * freq[None, :]
    return (jnp.cos(angles)[:, None, :], jnp.sin(angles)[:, None, :])

def rotate(values, cosine, sine):
    half = ROT // 2
    first = values[..., :half]
    second = values[..., half:ROT]
    return jnp.concatenate([first * cosine - second * sine, second * cosine + first * sine, values[..., ROT:]], axis=-1)

def masked_scores(block_query, keys, block_seg, segments, start, scale):
    scores = jnp.einsum('qhd,khd->hqk', block_query, keys) * scale
    rows = start + jnp.arange(block_query.shape[0], dtype=jnp.int32)[:, None]
    cols = jnp.arange(keys.shape[0], dtype=jnp.int32)[None, :]
    allowed = (block_seg[:, None] == segments[None, :]) & (cols <= rows)
    return jnp.where(allowed[None], scores, NEGATIVE)

def group_pass(params, rows, grad_rows, segments, offsets):
    gain_one, shift_one, gain_two, shift_two, qkv_weight, qkv_bias, proj_weight, up_weight, up_bias, down_weight, out_bias = params
    count = rows.shape[0]
    scale = HD ** (-0.5)
    normal_one, inverse_one, mixed_one = norm_rows(rows, gain_one, shift_one)
    normal_two, inverse_two, mixed_two = norm_rows(rows, gain_two, shift_two)
    normed_one = mixed_one.astype(jnp.bfloat16)
    normed_two = mixed_two.astype(jnp.bfloat16)
    weight_qkv = qkv_weight.astype(jnp.float32)
    projected = jnp.einsum('td,kde->kte', widen(normed_one), weight_qkv) + qkv_bias.astype(jnp.float32)[:, None, :]
    cosine, sine = rotary_tables(offsets)
    query = rotate(projected[0].reshape(count, H, HD), cosine, sine).astype(jnp.bfloat16)
    keys = rotate(projected[1].reshape(count, H, HD), cosine, sine).astype(jnp.bfloat16)
    values = projected[2].reshape(count, H, HD).astype(jnp.bfloat16)
    query_f = widen(query)
    keys_f = widen(keys)
    values_f = widen(values)
    width = min(512, count)
    starts = jnp.arange(count // width, dtype=jnp.int32) * width

    def forward_block(start):
        block_query = lax.dynamic_slice_in_dim(query_f, start, width, 0)
        block_seg = lax.dynamic_slice_in_dim(segments, start, width, 0)
        scores = masked_scores(block_query, keys_f, block_seg, segments, start, scale)
        peak = lax.optimization_barrier(jnp.max(scores, axis=2, keepdims=True))
        weights = jnp.exp(scores - peak)
        mass = lax.optimization_barrier(jnp.sum(weights, axis=2, keepdims=True))
        probs = widen(weights / mass)
        return (jnp.einsum('hqk,khd->qhd', probs, values_f), peak + jnp.log(mass))
    outs, logs = lax.map(forward_block, starts)
    attended = outs.reshape(count, H, HD).astype(jnp.bfloat16)
    logsum = jnp.transpose(logs, (1, 0, 2, 3)).reshape(H, count, 1)
    hidden_pre = jnp.dot(normed_two, up_weight, preferred_element_type=jnp.float32) + up_bias.astype(jnp.float32)
    activ = gelu_exact(hidden_pre).astype(jnp.bfloat16)
    flat = attended.reshape(count, D)
    branch = jnp.dot(flat, proj_weight, preferred_element_type=jnp.float32) + jnp.dot(activ, down_weight, preferred_element_type=jnp.float32)
    output = rows + branch + out_bias
    cot_round = grad_rows.astype(jnp.bfloat16)
    out_bias_grad = lax.optimization_barrier(jnp.sum(grad_rows, axis=0))
    proj_grad = jnp.dot(flat.T, cot_round, preferred_element_type=jnp.float32)
    down_grad = jnp.dot(activ.T, cot_round, preferred_element_type=jnp.float32)
    attended_grad = jnp.dot(cot_round, proj_weight.T, preferred_element_type=jnp.float32).astype(jnp.bfloat16).reshape(count, H, HD)
    pre_grad = jnp.dot(cot_round, down_weight.T, preferred_element_type=jnp.float32) * gelu_slope(hidden_pre)
    up_bias_grad = lax.optimization_barrier(jnp.sum(pre_grad, axis=0))
    pre_round = pre_grad.astype(jnp.bfloat16)
    up_grad = jnp.dot(normed_two.T, pre_round, preferred_element_type=jnp.float32)
    grad_f = widen(attended_grad)
    delta = jnp.einsum('thd,thd->ht', grad_f, widen(attended))

    def backward_block(carry, start):
        key_acc, value_acc = carry
        block_query = lax.dynamic_slice_in_dim(query_f, start, width, 0)
        block_seg = lax.dynamic_slice_in_dim(segments, start, width, 0)
        scores = masked_scores(block_query, keys_f, block_seg, segments, start, scale)
        probs = jnp.exp(scores - lax.dynamic_slice_in_dim(logsum, start, width, 1))
        block_grad = lax.dynamic_slice_in_dim(grad_f, start, width, 0)
        value_acc = value_acc + jnp.einsum('hqk,qhd->khd', widen(probs), block_grad)
        prob_grad = jnp.einsum('qhd,khd->hqk', block_grad, values_f)
        block_delta = lax.dynamic_slice_in_dim(delta, start, width, 1)[:, :, None]
        score_round = widen(probs * (prob_grad - block_delta) * scale)
        query_part = jnp.einsum('hqk,khd->qhd', score_round, keys_f)
        key_acc = key_acc + jnp.einsum('hqk,qhd->khd', score_round, block_query)
        return ((key_acc, value_acc), query_part)
    zeros = jnp.zeros((count, H, HD), jnp.float32)
    (key_grad, value_grad), query_parts = lax.scan(backward_block, (zeros, zeros), starts)
    query_grad = rotate(query_parts.reshape(count, H, HD), cosine, -sine)
    key_grad = rotate(key_grad, cosine, -sine)
    stacked = jnp.stack([query_grad, key_grad, value_grad]).reshape(3, count, D)
    qkv_bias_grad = lax.optimization_barrier(jnp.sum(stacked, axis=1))
    stacked_f = widen(stacked)
    qkv_grad = jnp.einsum('td,kte->kde', widen(normed_one), stacked_f)
    grad_one = jnp.einsum('kte,kde->td', stacked_f, weight_qkv)
    grad_two = jnp.dot(pre_round, up_weight.T, preferred_element_type=jnp.float32)
    input_grad = grad_rows + norm_back(grad_one, normal_one, inverse_one, gain_one) + norm_back(grad_two, normal_two, inverse_two, gain_two)
    grads = (lax.optimization_barrier(jnp.sum(grad_one * normal_one, axis=0)), lax.optimization_barrier(jnp.sum(grad_one, axis=0)), lax.optimization_barrier(jnp.sum(grad_two * normal_two, axis=0)), lax.optimization_barrier(jnp.sum(grad_two, axis=0)), qkv_grad, qkv_bias_grad, proj_grad, up_grad, up_bias_grad, down_grad, out_bias_grad)
    return (output, input_grad, grads)

def reference(block_input, cotangent, segment_ids, token_offset, first_gain, first_shift, second_gain, second_shift, qkv_weight, qkv_bias, proj_weight, up_weight, up_bias, down_weight, out_bias):
    groups = TOKENS // TOK_DEV
    params = (first_gain, first_shift, second_gain, second_shift, qkv_weight, qkv_bias, proj_weight, up_weight, up_bias, down_weight, out_bias)

    def group_step(carry, item):
        rows, grad_rows, segments, offsets = item
        output, input_grad, grads = group_pass(params, rows, grad_rows, segments, offsets)
        return (tuple((total + part for total, part in zip(carry, grads))), (output, input_grad))
    shapes = ((D,), (D,), (D,), (D,), (3, D, D), (3, D), (D, D), (D, FF), (FF,), (FF, D), (D,))
    init = tuple((jnp.zeros(shape, jnp.float32) for shape in shapes))
    items = (block_input.reshape(groups, TOK_DEV, D), cotangent.reshape(groups, TOK_DEV, D), segment_ids.reshape(groups, TOK_DEV), token_offset.reshape(groups, TOK_DEV))
    totals, (outputs, input_grads) = lax.scan(group_step, init, items)
    return (outputs.reshape(TOKENS, D), input_grads.reshape(TOKENS, D), totals[0], totals[1], totals[2], totals[3], totals[4], totals[5], totals[6], totals[7], totals[8], totals[9], totals[10])
```

```python
import functools

import jax
import jax.numpy as jnp
from jax import lax
from jax.experimental import pallas as pl
from jax.experimental.pallas import tpu as pltpu
from jax.sharding import PartitionSpec as P

HD = 64
ROT = 16
EPSILON = 1e-05
NEGATIVE = -1e30
LANES = 128
BF = jnp.bfloat16
F32 = jnp.float32
ANY = pl.BlockSpec(memory_space=pl.ANY)
VMEM = pl.BlockSpec(memory_space=pltpu.VMEM)
VMEM_LIMIT = 60 * 1024 * 1024


def dot(a, b, ca, cb):
    return lax.dot_general(a, b, (((ca,), (cb,)), ((), ())), preferred_element_type=F32)


def flip(index, mask):
    out = index
    bit = 0
    while (1 << bit) <= mask:
        if (mask >> bit) & 1:
            step = 1 << bit
            out = out + (1 - 2 * ((index // step) % 2)) * step
        bit += 1
    return out


def span(bits):
    masks = [0]
    for bit in bits:
        masks = masks + [m | (1 << bit) for m in masks]
    return masks


def remote(src, dst, send_sem, recv_sem, device):
    return pltpu.make_async_remote_copy(
        src_ref=src,
        dst_ref=dst,
        send_sem=send_sem,
        recv_sem=recv_sem,
        device_id=device,
        device_id_type=pl.DeviceIdType.MESH,
    )


def shift_order(count):
    return sorted(range(1, count), key=lambda s: (min(s, count - s), s))


def gather_plan(count, places, arrays):
    nbits = count.bit_length() - 1
    first = list(range(nbits - 1, -1, -1))
    second = [first[1], first[0]] + first[2:] if nbits >= 3 else first
    chunks = []
    for a in range(arrays):
        for s in [0] + shift_order(places):
            chunks.append((a, s, (first, second)[len(chunks) % 2]))
    return nbits, chunks


def gather_kernel(
    count, places, arrays, w_ref, vec_ref, g_ref, vout_ref, zs, zr, ds, dr, vs, vr, ls
):
    me, mz = lax.axis_index("dp"), lax.axis_index("tensor")
    total = count * places

    def vec_copy(i, sending):
        di, zi = i // places, i % places
        if sending:
            slot = (me, mz)
        else:
            slot = ((me + count - di) % count, (mz + places - zi) % places)
        return remote(
            vec_ref,
            vout_ref.at[slot[0], slot[1]],
            vs.at[i],
            vr.at[i],
            ((me + di) % count, (mz + zi) % places),
        )

    def send_vec(i, carry):
        vec_copy(i, True).start()
        return carry

    lax.fori_loop(1, total, send_vec, 0)

    nbits, chunks = gather_plan(count, places, arrays)
    own = [
        pltpu.make_async_copy(w_ref.at[a], g_ref.at[a, mz, me], ls.at[a]) for a in range(arrays)
    ]
    own_vec = pltpu.make_async_copy(vec_ref, vout_ref.at[me, mz], ls.at[arrays])

    def z_copy(a, s, sending):
        slot = mz if sending else (mz + places - s) % places
        n = a * (places - 1) + s - 1
        return remote(
            w_ref.at[a],
            g_ref.at[a, slot, me],
            zs.at[n],
            zr.at[n],
            (me, (mz + s) % places),
        )

    def d_copies(j, k, sending):
        a, s, order = chunks[j]
        place = (mz + places - s) % places
        bit = order[k]
        out = []
        for i, m in enumerate(span(order[:k])):
            slot = flip(me, m if sending else m | (1 << bit))
            src = w_ref.at[a] if s == 0 and m == 0 and sending else g_ref.at[a, place, slot]
            n = j * (count - 1) + (1 << k) - 1 + i
            out.append(
                remote(
                    src,
                    g_ref.at[a, place, slot],
                    ds.at[n],
                    dr.at[n],
                    (flip(me, 1 << bit), mz),
                )
            )
        return out

    for a in range(arrays):
        for s in shift_order(places):
            z_copy(a, s, True).start()
    for copy in own:
        copy.start()
    own_vec.start()
    for slot in range(len(chunks) + nbits):
        for k in range(nbits, -1, -1):
            j = slot - k
            if not 0 <= j < len(chunks):
                continue
            if k == 0:
                if chunks[j][1] > 0:
                    z_copy(chunks[j][0], chunks[j][1], False).wait_recv()
            else:
                for copy in d_copies(j, k - 1, False):
                    copy.wait_recv()
            if k < nbits:
                for copy in d_copies(j, k, True):
                    copy.start()
    for copy in own:
        copy.wait()
    own_vec.wait()

    def wait_vec(i, carry):
        vec_copy(i, False).wait_recv()
        vec_copy(i, True).wait_send()
        return carry

    lax.fori_loop(1, total, wait_vec, 0)
    for a in range(arrays):
        for s in range(1, places):
            z_copy(a, s, True).wait_send()
    for j in range(len(chunks)):
        for k in range(nbits):
            for copy in d_copies(j, k, True):
                copy.wait_send()


def gather_all(weights, vector, count, places):
    arrays, rows, width = weights.shape
    chunks = arrays * places
    sem = pltpu.SemaphoreType.DMA
    return pl.pallas_call(
        functools.partial(gather_kernel, count, places, arrays),
        out_shape=(
            jax.ShapeDtypeStruct((arrays, places, count, rows, width), weights.dtype),
            jax.ShapeDtypeStruct((count, places) + vector.shape, vector.dtype),
        ),
        in_specs=[VMEM, VMEM],
        out_specs=(ANY, ANY),
        scratch_shapes=[
            sem((arrays * (places - 1),)),
            sem((arrays * (places - 1),)),
            sem((chunks * (count - 1),)),
            sem((chunks * (count - 1),)),
            sem((count * places,)),
            sem((count * places,)),
            sem((arrays + 1,)),
        ],
        compiler_params=pltpu.CompilerParams(has_side_effects=True),
        name="gather_all",
    )(weights, vector)


def exchange_kernel(places, x_ref, y_ref, stage, ss, rs, ls):
    me, mz = lax.axis_index("dp"), lax.axis_index("tensor")

    def copy(s, sending):
        to = (mz + s) % places
        slot = mz if sending else (mz + places - s) % places
        return remote(x_ref.at[to], y_ref.at[slot], ss.at[s], rs.at[s], (me, to))

    for s in shift_order(places)[::-1]:
        copy(s, True).start()
    inward = pltpu.make_async_copy(x_ref.at[mz], stage, ls.at[0])
    inward.start()
    inward.wait()
    outward = pltpu.make_async_copy(stage, y_ref.at[mz], ls.at[1])
    outward.start()
    outward.wait()
    for s in range(1, places):
        copy(s, False).wait_recv()
    for s in range(1, places):
        copy(s, True).wait_send()


def exchange(x, places):
    sem = pltpu.SemaphoreType.DMA
    return pl.pallas_call(
        functools.partial(exchange_kernel, places),
        out_shape=jax.ShapeDtypeStruct(x.shape, x.dtype),
        in_specs=[ANY],
        out_specs=ANY,
        scratch_shapes=[
            pltpu.VMEM(x.shape[1:], x.dtype),
            sem((places,)),
            sem((places,)),
            sem((2,)),
        ],
        compiler_params=pltpu.CompilerParams(has_side_effects=True),
        name="exchange",
    )(x)


def scatter_plan(count, places, arrays):
    nbits = count.bit_length() - 1
    first = list(range(nbits))
    second = [first[0], first[2], first[1]] + first[3:] if nbits >= 3 else first
    chunks = []
    for a in range(arrays):
        for s in shift_order(places)[::-1] + [0]:
            chunks.append((a, s, (first, second)[len(chunks) % 2]))
    return nbits, chunks


def add_rows(acc_ref, other_ref):
    rows = acc_ref.shape[0]
    step = 32 if rows % 32 == 0 else rows

    def body(i, carry):
        at = pl.ds(i * step, step)
        acc_ref[at, :] = (acc_ref[at, :].astype(F32) + other_ref[at, :].astype(F32)).astype(BF)
        return carry

    lax.fori_loop(0, rows // step, body, 0)


def scatter_kernel(count, places, arrays, *refs):
    nbits, chunks = scatter_plan(count, places, arrays)
    gr_ref, vec_ref, out_ref, vout_ref, acc = refs[:5]
    rbs = refs[5 : 5 + nbits]
    zb, vb, ks, kr, zs, zr, vs, vr, ls = refs[5 + nbits :]
    me, mz = lax.axis_index("dp"), lax.axis_index("tensor")
    total = count * places

    def vec_copy(i, sending):
        to = ((me + i // places) % count, (mz + i % places) % places)
        return remote(vec_ref.at[to[0], to[1]], vb.at[i], vs.at[i], vr.at[i], to)

    def send_vec(i, carry):
        vec_copy(i, True).start()
        return carry

    lax.fori_loop(1, total, send_vec, 0)
    own_vec = pltpu.make_async_copy(vec_ref.at[me, mz], vb.at[0], ls.at[0])
    own_vec.start()

    def loads(j):
        a, s, order = chunks[j]
        place = (mz + s) % places
        out = []
        for i, m in enumerate(span(order[1:])):
            n = 1 + j * (count // 2) + i
            out.append(
                pltpu.make_async_copy(gr_ref.at[a, place, flip(me, m)], acc.at[j, i], ls.at[n])
            )
        return out

    def copies(j, k):
        a, s, order = chunks[j]
        place = (mz + s) % places
        base = span(order[1:])
        out = []
        for i, m in enumerate(span(order[k + 1 :])):
            far = m | (1 << order[k])
            if k == 0:
                src = gr_ref.at[a, place, flip(me, far)]
            else:
                src = acc.at[j, base.index(far)]
            n = j * (count - 1) + (count - (count >> k)) + i
            out.append(
                remote(
                    src, rbs[k].at[j, i], ks.at[n], kr.at[n], (flip(me, 1 << order[k]), mz)
                )
            )
        return out

    def z_copy(j):
        a, s, _ = chunks[j]
        n = a * (places - 1) + s - 1
        return remote(acc.at[j, 0], zb.at[a, s - 1], zs.at[n], zr.at[n], (me, (mz + s) % places))

    for j in range(len(chunks)):
        for copy in copies(j, 0):
            copy.start()
        for copy in loads(j):
            copy.start()
    for slot in range(len(chunks) + nbits - 1):
        for k in range(nbits - 1, -1, -1):
            j = slot - k
            if not 0 <= j < len(chunks):
                continue
            _, s, order = chunks[j]
            base = span(order[1:])
            if k == 0:
                for copy in loads(j):
                    copy.wait()
            for i, (m, copy) in enumerate(zip(span(order[k + 1 :]), copies(j, k))):
                copy.wait_recv()
                add_rows(acc.at[j, base.index(m)], rbs[k].at[j, i])
            if k + 1 < nbits:
                for copy in copies(j, k + 1):
                    copy.start()
            elif s > 0:
                z_copy(j).start()

    own_vec.wait()

    def wait_vec(i, carry):
        vec_copy(i, False).wait_recv()
        vec_copy(i, True).wait_send()
        return carry

    lax.fori_loop(1, total, wait_vec, 0)
    vout_ref[...] = jnp.sum(vb[...], axis=0)
    for a in range(arrays):
        for j, (b, s, _) in enumerate(chunks):
            if b == a and s > 0:
                z_copy(j).wait_recv()
        for j, (b, s, _) in enumerate(chunks):
            if b == a and s == 0:
                result = acc[j, 0].astype(F32)
                for other in range(places - 1):
                    result = result + zb[a, other].astype(F32)
                out_ref[a] = result
    for j, (_, s, _) in enumerate(chunks):
        for k in range(nbits):
            for copy in copies(j, k):
                copy.wait_send()
        if s > 0:
            z_copy(j).wait_send()


def scatter_all(grads, vectors):
    arrays, places, count, rows, width = grads.shape
    nbits, chunks = scatter_plan(count, places, arrays)
    n = len(chunks)
    sem = pltpu.SemaphoreType.DMA
    return pl.pallas_call(
        functools.partial(scatter_kernel, count, places, arrays),
        out_shape=(
            jax.ShapeDtypeStruct((arrays, rows, width), F32),
            jax.ShapeDtypeStruct(vectors.shape[2:], F32),
        ),
        in_specs=[ANY, ANY],
        out_specs=(VMEM, VMEM),
        scratch_shapes=[pltpu.VMEM((n, count // 2, rows, width), BF)]
        + [pltpu.VMEM((n, count >> (k + 1), rows, width), BF) for k in range(nbits)]
        + [
            pltpu.VMEM((arrays, places - 1, rows, width), BF),
            pltpu.VMEM((count * places,) + vectors.shape[2:], F32),
            sem((n * (count - 1),)),
            sem((n * (count - 1),)),
            sem((arrays * (places - 1),)),
            sem((arrays * (places - 1),)),
            sem((count * places,)),
            sem((count * places,)),
            sem((1 + n * (count // 2),)),
        ],
        compiler_params=pltpu.CompilerParams(
            has_side_effects=True, vmem_limit_bytes=VMEM_LIMIT
        ),
        name="scatter_all",
    )(grads, vectors)


def turn_tiles(tiles, cosine, low, high):
    out = []
    for tile in tiles:
        ahead = pltpu.roll(tile, LANES - ROT // 2, 1)
        behind = pltpu.roll(tile, ROT // 2, 1)
        out.append(tile * cosine + ahead * low + behind * high)
    return out


def rotary_lanes(offsets):
    half = ROT // 2
    freq = 10000.0 ** (-(2.0 * jnp.arange(half, dtype=F32)) / ROT)
    angles = offsets.astype(F32)[:, None] * freq[None, :]
    cosine, sine = jnp.cos(angles), jnp.sin(angles)
    rows = offsets.shape[0]
    rest = jnp.zeros((rows, HD - ROT), F32)
    blank = jnp.zeros((rows, half), F32)
    one = jnp.concatenate([cosine, cosine, rest + 1.0], axis=1)
    low = jnp.concatenate([-sine, blank, rest], axis=1)
    high = jnp.concatenate([blank, sine, rest], axis=1)
    return tuple(jnp.concatenate([t, t], axis=1) for t in (one, low, high))


def project_kernel(wide, n1_ref, cot_ref, w_ref, b_ref, c_ref, lo_ref, hi_ref, x_ref):
    full = 3 * wide
    cut = full // LANES * LANES
    part = full - cut
    w = w_ref[0]
    forward = dot(n1_ref[...], w[:, : cut + LANES], 1, 0) + b_ref[0]
    backward = dot(cot_ref[...], w[:, cut:], 1, 0)
    turned = 2 * wide // LANES
    tiles = [forward[:, i * LANES : (i + 1) * LANES] for i in range(turned)]
    tiles = turn_tiles(tiles, c_ref[...], lo_ref[...], hi_ref[...])
    for i, tile in enumerate(tiles):
        x_ref[0, :, i * LANES : (i + 1) * LANES] = tile.astype(BF)
    x_ref[0, :, turned * LANES : cut] = forward[:, turned * LANES : cut].astype(BF)
    lane = lax.broadcasted_iota(jnp.int32, (forward.shape[0], LANES), 1)
    mixed = jnp.where(lane < part, forward[:, cut:], backward[:, :LANES])
    x_ref[0, :, cut : cut + LANES] = mixed.astype(BF)
    x_ref[0, :, cut + LANES :] = backward[:, LANES:].astype(BF)


def project(n1, cot, w, bias, tables, wide):
    places, model, width = w.shape
    rows = n1.shape[0]
    whole = pl.BlockSpec((rows, model), lambda z: (0, 0))
    table = pl.BlockSpec((rows, LANES), lambda z: (0, 0))
    return pl.pallas_call(
        functools.partial(project_kernel, wide),
        grid=(places,),
        out_shape=jax.ShapeDtypeStruct((places, rows, width), BF),
        in_specs=[
            whole,
            whole,
            pl.BlockSpec((1, model, width), lambda z: (z, 0, 0)),
            pl.BlockSpec((1, 1, bias.shape[2]), lambda z: (z, 0, 0)),
            table,
            table,
            table,
        ],
        out_specs=pl.BlockSpec((1, rows, width), lambda z: (z, 0, 0)),
        compiler_params=pltpu.CompilerParams(vmem_limit_bytes=VMEM_LIMIT),
        name="project",
    )(n1, cot, w, bias, *tables)


def attention_kernel(
    heads,
    block,
    y_ref,
    begin_ref,
    c_ref,
    lo_ref,
    hi_ref,
    r_ref,
    bias_ref,
    qh,
    kh,
    vh,
    oh,
    kt,
    vt,
    s_scr,
    dq,
    dk,
    dv,
):
    total = y_ref.shape[0]
    wide = heads * HD
    scale = HD**-0.5
    blocks = total // block

    def prepare(i, carry):
        at = pl.ds(pl.multiple_of(i * block, block), block)
        for h in range(heads):
            q = y_ref[at, h * HD : (h + 1) * HD].astype(F32) * scale
            k = y_ref[at, wide + h * HD : wide + (h + 1) * HD].astype(F32)
            v = y_ref[at, 2 * wide + h * HD : 2 * wide + (h + 1) * HD].astype(F32)
            qh[h, at, :] = q.astype(BF)
            kh[h, at, :] = k.astype(BF)
            vh[h, at, :] = v.astype(BF)
            oh[h, at, :] = y_ref[at, 3 * wide + h * HD : 3 * wide + (h + 1) * HD]
            kt[h, :, at] = k.T.astype(BF)
            vt[h, :, at] = v.T.astype(BF)
            dk[h, at, :] = jnp.zeros((block, HD), F32)
            dv[h, at, :] = jnp.zeros((block, HD), F32)
        return carry

    lax.fori_loop(0, blocks, prepare, 0)

    def row_block(i, carry):
        at = pl.ds(pl.multiple_of(i * block, block), block)
        begin = begin_ref[0:1, at]
        last = i * block + lax.broadcasted_iota(jnp.int32, (1, block), 1)
        queries = [qh[h, at, :] for h in range(heads)]
        grads = [oh[h, at, :] for h in range(heads)]

        def scores(j, peaks):
            keys = pl.ds(pl.multiple_of(j * block, block), block)
            place = j * block + lax.broadcasted_iota(jnp.int32, (block, block), 0)
            allowed = (place >= begin) & (place <= last)
            out = []
            for h in range(heads):
                s = dot(kh[h, keys, :], queries[h], 1, 1)
                s = jnp.where(allowed, s, NEGATIVE)
                s_scr[h, keys, :] = s
                out.append(jnp.maximum(peaks[h], jnp.max(s.reshape(block // 8, 8, block), axis=0)))
            return tuple(out)

        start = tuple(jnp.full((8, block), NEGATIVE, F32) for _ in range(heads))
        peaks = lax.fori_loop(0, i + 1, scores, start)
        peaks = [jnp.max(p, axis=0, keepdims=True) for p in peaks]

        def weigh(j, state):
            keys = pl.ds(pl.multiple_of(j * block, block), block)
            out = []
            for h in range(heads):
                mass, acc = state[h]
                p = jnp.exp(s_scr[h, keys, :] - peaks[h])
                s_scr[h, keys, :] = p
                mass = mass + jnp.sum(p.reshape(block // 8, 8, block), axis=0)
                acc = acc + dot(vt[h, :, keys], p.astype(BF), 1, 0)
                out.append((mass, acc))
            return tuple(out)

        start = tuple(
            (jnp.zeros((8, block), F32), jnp.zeros((HD, block), F32)) for _ in range(heads)
        )
        state = lax.fori_loop(0, i + 1, weigh, start)
        inverses, deltas = [], []
        for h in range(heads):
            mass = jnp.sum(state[h][0], axis=0, keepdims=True)
            inverse = 1.0 / mass
            attended = (state[h][1] * inverse).astype(BF).astype(F32)
            deltas.append(
                jnp.sum(attended * grads[h].astype(F32).T, axis=0, keepdims=True)
            )
            inverses.append(inverse)
            r_ref[at, 3 * wide + h * HD : 3 * wide + (h + 1) * HD] = attended.T.astype(BF)

        def back(j, acc):
            keys = pl.ds(pl.multiple_of(j * block, block), block)
            out = []
            for h in range(heads):
                p = s_scr[h, keys, :] * inverses[h]
                dv[h, keys, :] += dot(p.astype(BF), grads[h], 1, 0)
                g = dot(vh[h, keys, :], grads[h], 1, 1)
                ds = (p * (g - deltas[h])).astype(BF)
                dk[h, keys, :] += dot(ds, queries[h], 1, 0)
                out.append(acc[h] + dot(kt[h, :, keys], ds, 1, 0))
            return tuple(out)

        start = tuple(jnp.zeros((HD, block), F32) for _ in range(heads))
        acc = lax.fori_loop(0, i + 1, back, start)
        for h in range(heads):
            dq[h, at, :] = (acc[h] * scale).T
        return carry

    lax.fori_loop(0, blocks, row_block, 0)

    def finish(i, sums):
        at = pl.ds(pl.multiple_of(i * block, block), block)
        pieces = [d[h, at, :] for d in (dq, dk, dv) for h in range(heads)]
        out = []
        turned = 2 * wide // LANES
        for t in range(3 * wide // LANES + 1):
            if 2 * t + 1 < len(pieces):
                tile = jnp.concatenate(pieces[2 * t : 2 * t + 2], axis=1)
            else:
                tile = pieces[2 * t]
            if t < turned:
                tile = turn_tiles([tile], c_ref[at, :], -lo_ref[at, :], -hi_ref[at, :])[0]
            width = tile.shape[1]
            r_ref[at, t * LANES : t * LANES + width] = tile.astype(BF)
            out.append(sums[t] + jnp.sum(tile.reshape(block // 8, 8, width), axis=0))
        return tuple(out)

    start = []
    for t in range(3 * wide // LANES + 1):
        width = min(LANES, 3 * wide - t * LANES)
        start.append(jnp.zeros((8, width), F32))
    sums = lax.fori_loop(0, blocks, finish, tuple(start))
    for t, value in enumerate(sums):
        bias_ref[0:1, t * LANES : t * LANES + value.shape[1]] = jnp.sum(
            value, axis=0, keepdims=True
        )


def attention(y, begin, tables, heads):
    total, width = y.shape
    block = min(256, total)
    scratch = pltpu.VMEM
    return pl.pallas_call(
        functools.partial(attention_kernel, heads, block),
        out_shape=(
            jax.ShapeDtypeStruct((total, width), BF),
            jax.ShapeDtypeStruct((1, 3 * heads * HD), F32),
        ),
        in_specs=[VMEM] * 5,
        out_specs=(VMEM, VMEM),
        scratch_shapes=[scratch((heads, total, HD), BF)] * 4
        + [scratch((heads, HD, total), BF)] * 2
        + [scratch((heads, total, block), F32)]
        + [scratch((heads, total, HD), F32)] * 3,
        compiler_params=pltpu.CompilerParams(vmem_limit_bytes=VMEM_LIMIT),
        name="attention",
    )(y, begin, *tables)


def feed_kernel(
    n2_ref, n2t_ref, cot_ref, cott_ref, up_ref, down_ref, b_ref, out_ref, back_ref, gu_ref, gd_ref, gb_ref
):
    @pl.when(pl.program_id(0) == 0)
    def _():
        out_ref[...] = jnp.zeros_like(out_ref)
        back_ref[...] = jnp.zeros_like(back_ref)

    up, down = up_ref[0, 0], down_ref[0, 0]
    pre = dot(n2_ref[...], up, 1, 0) + b_ref[0]
    bell = 0.5 * (1.0 + lax.erf(pre * 0.7071067811865476))
    activ = (pre * bell).astype(BF)
    out_ref[...] += dot(activ, down, 1, 1)
    gd_ref[0] = dot(cott_ref[...], activ, 1, 0).astype(BF)
    slope = bell + pre * jnp.exp(-0.5 * pre * pre) * 0.3989422804014327
    grad = dot(cot_ref[...], down, 1, 0) * slope
    gb_ref[0] = jnp.sum(grad, axis=0, keepdims=True)
    grad = grad.astype(BF)
    gu_ref[0] = dot(n2t_ref[...], grad, 1, 0).astype(BF)
    back_ref[...] += dot(grad, up, 1, 1)


def feed(n2, cot, w, bias):
    places, model, width = w.shape[1:]
    rows = n2.shape[0]
    whole = pl.BlockSpec((rows, model), lambda z: (0, 0))
    turned = pl.BlockSpec((model, rows), lambda z: (0, 0))
    square = pl.BlockSpec((1, model, width), lambda z: (z, 0, 0))
    return pl.pallas_call(
        feed_kernel,
        grid=(places,),
        out_shape=(
            jax.ShapeDtypeStruct((rows, model), F32),
            jax.ShapeDtypeStruct((rows, model), F32),
            jax.ShapeDtypeStruct((places, model, width), BF),
            jax.ShapeDtypeStruct((places, model, width), BF),
            jax.ShapeDtypeStruct((places, 1, width), F32),
        ),
        in_specs=[
            whole,
            turned,
            whole,
            turned,
            pl.BlockSpec((1, 1, model, width), lambda z: (1, z, 0, 0)),
            pl.BlockSpec((1, 1, model, width), lambda z: (2, z, 0, 0)),
            pl.BlockSpec((1, 1, width), lambda z: (z, 0, 0)),
        ],
        out_specs=(
            whole,
            whole,
            square,
            square,
            pl.BlockSpec((1, 1, width), lambda z: (z, 0, 0)),
        ),
        compiler_params=pltpu.CompilerParams(vmem_limit_bytes=VMEM_LIMIT),
        name="feed",
    )(n2, n2.T, cot, cot.T, w, w, bias)


def return_kernel(wide, n1t_ref, cott_ref, z_ref, w_ref, out_ref, back_ref, g_ref):
    @pl.when(pl.program_id(0) == 0)
    def _():
        out_ref[...] = jnp.zeros_like(out_ref)
        back_ref[...] = jnp.zeros_like(back_ref)

    full = 3 * wide
    cut = full // LANES * LANES
    part = full - cut
    z, w = z_ref[0], w_ref[0]
    lane = lax.broadcasted_iota(jnp.int32, (z.shape[0], LANES), 1)
    middle = z[:, cut : cut + LANES]
    none = jnp.zeros_like(middle)
    ours = jnp.where(lane < part, middle, none)
    theirs = jnp.where(lane < part, none, middle)
    back_ref[...] += dot(
        jnp.concatenate([z[:, :cut], ours], axis=1), w[:, : cut + LANES], 1, 1
    )
    out_ref[...] += dot(
        jnp.concatenate([theirs, z[:, cut + LANES :]], axis=1), w[:, cut:], 1, 1
    )
    first = dot(n1t_ref[...], z[:, : cut + LANES], 1, 0)
    second = dot(cott_ref[...], z[:, cut:], 1, 0)
    lane = lax.broadcasted_iota(jnp.int32, (first.shape[0], LANES), 1)
    g_ref[0, :, :cut] = first[:, :cut].astype(BF)
    g_ref[0, :, cut : cut + LANES] = jnp.where(
        lane < part, first[:, cut:], second[:, :LANES]
    ).astype(BF)
    g_ref[0, :, cut + LANES :] = second[:, LANES:].astype(BF)


def returning(n1, cot, z, w, wide):
    places, rows, width = z.shape
    model = n1.shape[1]
    turned = pl.BlockSpec((model, rows), lambda z: (0, 0))
    whole = pl.BlockSpec((rows, model), lambda z: (0, 0))
    return pl.pallas_call(
        functools.partial(return_kernel, wide),
        grid=(places,),
        out_shape=(
            jax.ShapeDtypeStruct((rows, model), F32),
            jax.ShapeDtypeStruct((rows, model), F32),
            jax.ShapeDtypeStruct((places, model, width), BF),
        ),
        in_specs=[
            turned,
            turned,
            pl.BlockSpec((1, rows, width), lambda z: (z, 0, 0)),
            pl.BlockSpec((1, model, width), lambda z: (z, 0, 0)),
        ],
        out_specs=(whole, whole, pl.BlockSpec((1, model, width), lambda z: (z, 0, 0))),
        compiler_params=pltpu.CompilerParams(vmem_limit_bytes=VMEM_LIMIT),
        name="returning",
    )(n1.T, cot.T, z, w)


def norm_back(grad_out, normal, inverse, gain):
    scaled = grad_out * gain
    return inverse * (
        scaled
        - jnp.mean(scaled, axis=1, keepdims=True)
        - normal * jnp.mean(scaled * normal, axis=1, keepdims=True)
    )


def lanes(values, width=LANES):
    return jnp.pad(values, [(0, 0)] * (values.ndim - 1) + [(0, width - values.shape[-1])])


def shards(
    count,
    places,
    block_input,
    cotangent,
    segment_ids,
    token_offset,
    first_gain,
    first_shift,
    second_gain,
    second_shift,
    qkv_weight,
    qkv_bias,
    proj_weight,
    up_weight,
    up_bias,
    down_weight,
    out_bias,
):
    rows, model = block_input.shape
    depth = qkv_weight.shape[1]
    wide = qkv_weight.shape[2]
    heads = wide // HD
    ff = up_weight.shape[1]
    piece = first_gain.shape[0]
    total = segment_ids.shape[0]
    place = lax.axis_index("tensor")

    attn = jnp.concatenate([qkv_weight[0], qkv_weight[1], qkv_weight[2], proj_weight.T], axis=1)
    packed = jnp.stack([attn, up_weight, down_weight.T])
    vector = jnp.stack(
        [lanes(v) for v in (first_gain, first_shift, second_gain, second_shift, out_bias)]
        + [lanes(qkv_bias.astype(F32).reshape(-1)), lanes(up_bias.astype(F32))]
        + [jnp.zeros((LANES,), F32)]
    )
    weights, vectors = gather_all(packed, vector, count, places)
    weights = weights.reshape(3, places, model, ff)
    small = vectors[:, :, :5, :piece].transpose(2, 0, 1, 3).reshape(5, model)
    gain_one, shift_one, gain_two, shift_two, bias_out = (small[i] for i in range(5))
    bias_qkv = (
        vectors[:, :, 5, : 3 * wide // count]
        .reshape(count, places, 3, wide // count)
        .transpose(1, 2, 0, 3)
        .reshape(places, 1, 3 * wide)
    )
    cut = 3 * wide // LANES * LANES
    bias_qkv = lanes(bias_qkv, cut + LANES)
    bias_up = vectors[:, :, 6, : ff // count].transpose(1, 0, 2).reshape(places, 1, ff)

    center = block_input - jnp.mean(block_input, axis=1, keepdims=True)
    inverse = lax.rsqrt(jnp.mean(center * center, axis=1, keepdims=True) + EPSILON)
    normal = center * inverse
    n1 = (normal * gain_one + shift_one).astype(BF)
    n2 = (normal * gain_two + shift_two).astype(BF)
    cot = cotangent.astype(BF)

    tables = rotary_lanes(token_offset)
    mine = tuple(lax.dynamic_slice_in_dim(t, place * rows, rows, 0) for t in tables)
    x = project(n1, cot, weights[0], bias_qkv, mine, wide)
    y = exchange(x, places)
    begin = (jnp.arange(total, dtype=jnp.int32) - token_offset)[None, :]
    r, qkv_bias_part = attention(y.reshape(total, y.shape[2]), begin, tables, heads)
    z = exchange(r.reshape(places, rows, r.shape[1]), places)
    out_two, grad_two, up_grad, down_grad, up_bias_part = feed(n2, cot, weights, bias_up)
    out_one, grad_one, attn_grad = returning(n1, cot, z, weights[0], wide)

    block_output = block_input + (out_one + out_two) + bias_out
    input_grad = (
        cotangent
        + norm_back(grad_one, normal, inverse, gain_one)
        + norm_back(grad_two, normal, inverse, gain_two)
    )
    sums = jnp.stack(
        [
            jnp.sum(grad_one * normal, axis=0),
            jnp.sum(grad_one, axis=0),
            jnp.sum(grad_two * normal, axis=0),
            jnp.sum(grad_two, axis=0),
            jnp.sum(cotangent, axis=0),
        ]
    )
    sums = lanes(sums.reshape(5, count, places, piece).transpose(1, 2, 0, 3))
    qkv_sum = qkv_bias_part.reshape(3, count, wide // count).transpose(1, 0, 2)
    qkv_sum = lanes(qkv_sum.reshape(count, 1, 3 * wide // count))
    here = jnp.arange(places, dtype=jnp.int32)[None, :, None, None] == place
    qkv_sum = jnp.where(here, qkv_sum[:, None], 0.0)
    up_sum = lanes(up_bias_part.reshape(places, count, ff // count).transpose(1, 0, 2))[:, :, None]
    parts = jnp.concatenate([sums, qkv_sum, up_sum, jnp.zeros_like(up_sum)], axis=2)

    grads = jnp.stack([attn_grad, up_grad, down_grad]).reshape(3, places, count, depth, ff)
    done, vec = scatter_all(grads, parts)
    attn_done = done[0]
    qkv_weight_grad = jnp.stack([attn_done[:, i * wide : (i + 1) * wide] for i in range(3)])
    return (
        block_output,
        input_grad,
        vec[0, :piece],
        vec[1, :piece],
        vec[2, :piece],
        vec[3, :piece],
        qkv_weight_grad,
        vec[5, : 3 * wide // count].reshape(3, wide // count),
        attn_done[:, 3 * wide :].T,
        done[1],
        vec[6, : ff // count],
        done[2].T,
        vec[4, :piece],
    )


def solution(mesh):
    both = P(("dp", "tensor"))
    return jax.shard_map(
        functools.partial(shards, mesh.shape["dp"], mesh.shape["tensor"]),
        mesh=mesh,
        in_specs=(
            P(("dp", "tensor"), None),
            P(("dp", "tensor"), None),
            P("dp"),
            P("dp"),
            both,
            both,
            both,
            both,
            P(None, "dp", "tensor"),
            P(None, ("tensor", "dp")),
            P("tensor", "dp"),
            P("dp", "tensor"),
            P(("tensor", "dp")),
            P("tensor", "dp"),
            both,
        ),
        out_specs=(
            P(("dp", "tensor"), None),
            P(("dp", "tensor"), None),
            both,
            both,
            both,
            both,
            P(None, "dp", "tensor"),
            P(None, ("tensor", "dp")),
            P("tensor", "dp"),
            P("dp", "tensor"),
            P(("tensor", "dp")),
            P("tensor", "dp"),
            both,
        ),
        check_vma=False,
    )
```

```python
import functools

import jax
import jax.numpy as jnp
from jax import lax
from jax.experimental import pallas as pl
from jax.experimental.pallas import tpu as pltpu
from jax.sharding import PartitionSpec as P

HD = 64
ROT = 16
EPSILON = 1e-05
NEGATIVE = -1e30
LANES = 128
BF = jnp.bfloat16
F32 = jnp.float32
ANY = pl.BlockSpec(memory_space=pl.ANY)
VMEM = pl.BlockSpec(memory_space=pltpu.VMEM)
VMEM_LIMIT = 60 * 1024 * 1024


def dot(a, b, ca, cb):
    return lax.dot_general(a, b, (((ca,), (cb,)), ((), ())), preferred_element_type=F32)


def flip(index, mask):
    out = index
    bit = 0
    while (1 << bit) <= mask:
        if (mask >> bit) & 1:
            step = 1 << bit
            out = out + (1 - 2 * ((index // step) % 2)) * step
        bit += 1
    return out


def span(bits):
    masks = [0]
    for bit in bits:
        masks = masks + [m | (1 << bit) for m in masks]
    return masks


def remote(src, dst, send_sem, recv_sem, device):
    return pltpu.make_async_remote_copy(
        src_ref=src,
        dst_ref=dst,
        send_sem=send_sem,
        recv_sem=recv_sem,
        device_id=device,
        device_id_type=pl.DeviceIdType.MESH,
    )


def shift_order(count):
    return sorted(range(1, count), key=lambda s: (min(s, count - s), s))


def gather_plan(count, places, arrays):
    nbits = count.bit_length() - 1
    first = list(range(nbits - 1, -1, -1))
    second = [first[1], first[0]] + first[2:] if nbits >= 3 else first
    chunks = []
    for a in range(arrays):
        for s in [0] + shift_order(places):
            chunks.append((a, s, (first, second)[len(chunks) % 2]))
    return nbits, chunks


def gather_kernel(
    count, places, arrays, w_ref, vec_ref, g_ref, vout_ref, zs, zr, ds, dr, vs, vr, ls
):
    me, mz = lax.axis_index("dp"), lax.axis_index("tensor")
    total = count * places

    def vec_copy(i, sending):
        di, zi = i // places, i % places
        if sending:
            slot = (me, mz)
        else:
            slot = ((me + count - di) % count, (mz + places - zi) % places)
        return remote(
            vec_ref,
            vout_ref.at[slot[0], slot[1]],
            vs.at[i],
            vr.at[i],
            ((me + di) % count, (mz + zi) % places),
        )

    def send_vec(i, carry):
        vec_copy(i, True).start()
        return carry

    lax.fori_loop(1, total, send_vec, 0)

    nbits, chunks = gather_plan(count, places, arrays)
    own = [
        pltpu.make_async_copy(w_ref.at[a], g_ref.at[a, mz, me], ls.at[a]) for a in range(arrays)
    ]
    own_vec = pltpu.make_async_copy(vec_ref, vout_ref.at[me, mz], ls.at[arrays])

    def z_copy(a, s, sending):
        slot = mz if sending else (mz + places - s) % places
        n = a * (places - 1) + s - 1
        return remote(
            w_ref.at[a],
            g_ref.at[a, slot, me],
            zs.at[n],
            zr.at[n],
            (me, (mz + s) % places),
        )

    def d_copies(j, k, sending):
        a, s, order = chunks[j]
        place = (mz + places - s) % places
        bit = order[k]
        out = []
        for i, m in enumerate(span(order[:k])):
            slot = flip(me, m if sending else m | (1 << bit))
            src = w_ref.at[a] if s == 0 and m == 0 and sending else g_ref.at[a, place, slot]
            n = j * (count - 1) + (1 << k) - 1 + i
            out.append(
                remote(
                    src,
                    g_ref.at[a, place, slot],
                    ds.at[n],
                    dr.at[n],
                    (flip(me, 1 << bit), mz),
                )
            )
        return out

    for a in range(arrays):
        for s in shift_order(places):
            z_copy(a, s, True).start()
    for copy in own:
        copy.start()
    own_vec.start()
    for slot in range(len(chunks) + nbits):
        for k in range(nbits, -1, -1):
            j = slot - k
            if not 0 <= j < len(chunks):
                continue
            if k == 0:
                if chunks[j][1] > 0:
                    z_copy(chunks[j][0], chunks[j][1], False).wait_recv()
            else:
                for copy in d_copies(j, k - 1, False):
                    copy.wait_recv()
            if k < nbits:
                for copy in d_copies(j, k, True):
                    copy.start()
    for copy in own:
        copy.wait()
    own_vec.wait()

    def wait_vec(i, carry):
        vec_copy(i, False).wait_recv()
        vec_copy(i, True).wait_send()
        return carry

    lax.fori_loop(1, total, wait_vec, 0)
    for a in range(arrays):
        for s in range(1, places):
            z_copy(a, s, True).wait_send()
    for j in range(len(chunks)):
        for k in range(nbits):
            for copy in d_copies(j, k, True):
                copy.wait_send()


def gather_all(weights, vector, count, places):
    arrays, rows, width = weights.shape
    chunks = arrays * places
    sem = pltpu.SemaphoreType.DMA
    return pl.pallas_call(
        functools.partial(gather_kernel, count, places, arrays),
        out_shape=(
            jax.ShapeDtypeStruct((arrays, places, count, rows, width), weights.dtype),
            jax.ShapeDtypeStruct((count, places) + vector.shape, vector.dtype),
        ),
        in_specs=[VMEM, VMEM],
        out_specs=(ANY, ANY),
        scratch_shapes=[
            sem((arrays * (places - 1),)),
            sem((arrays * (places - 1),)),
            sem((chunks * (count - 1),)),
            sem((chunks * (count - 1),)),
            sem((count * places,)),
            sem((count * places,)),
            sem((arrays + 1,)),
        ],
        compiler_params=pltpu.CompilerParams(has_side_effects=True),
        name="gather_all",
    )(weights, vector)


def exchange_kernel(places, x_ref, y_ref, stage, ss, rs, ls):
    me, mz = lax.axis_index("dp"), lax.axis_index("tensor")

    def copy(s, sending):
        to = (mz + s) % places
        slot = mz if sending else (mz + places - s) % places
        return remote(x_ref.at[to], y_ref.at[slot], ss.at[s], rs.at[s], (me, to))

    for s in shift_order(places)[::-1]:
        copy(s, True).start()
    inward = pltpu.make_async_copy(x_ref.at[mz], stage, ls.at[0])
    inward.start()
    inward.wait()
    outward = pltpu.make_async_copy(stage, y_ref.at[mz], ls.at[1])
    outward.start()
    outward.wait()
    for s in range(1, places):
        copy(s, False).wait_recv()
    for s in range(1, places):
        copy(s, True).wait_send()


def exchange(x, places):
    sem = pltpu.SemaphoreType.DMA
    return pl.pallas_call(
        functools.partial(exchange_kernel, places),
        out_shape=jax.ShapeDtypeStruct(x.shape, x.dtype),
        in_specs=[ANY],
        out_specs=ANY,
        scratch_shapes=[
            pltpu.VMEM(x.shape[1:], x.dtype),
            sem((places,)),
            sem((places,)),
            sem((2,)),
        ],
        compiler_params=pltpu.CompilerParams(has_side_effects=True),
        name="exchange",
    )(x)


def scatter_plan(count, places, arrays):
    nbits = count.bit_length() - 1
    first = list(range(nbits))
    second = [first[0], first[2], first[1]] + first[3:] if nbits >= 3 else first
    chunks = []
    for a in range(arrays):
        for s in shift_order(places)[::-1] + [0]:
            chunks.append((a, s, (first, second)[len(chunks) % 2]))
    return nbits, chunks


def add_rows(acc_ref, other_ref):
    rows = acc_ref.shape[0]
    step = 32 if rows % 32 == 0 else rows

    def body(i, carry):
        at = pl.ds(i * step, step)
        acc_ref[at, :] = (acc_ref[at, :].astype(F32) + other_ref[at, :].astype(F32)).astype(BF)
        return carry

    lax.fori_loop(0, rows // step, body, 0)


def scatter_kernel(count, places, arrays, *refs):
    nbits, chunks = scatter_plan(count, places, arrays)
    grs, refs = refs[:arrays], refs[arrays:]
    vec_ref, out_ref, vout_ref, acc = refs[:4]
    rbs = refs[4 : 4 + nbits]
    zb, vb, ks, kr, zs, zr, vs, vr, ls = refs[4 + nbits :]
    me, mz = lax.axis_index("dp"), lax.axis_index("tensor")
    total = count * places

    def vec_copy(i, sending):
        to = ((me + i // places) % count, (mz + i % places) % places)
        return remote(vec_ref.at[to[0], to[1]], vb.at[i], vs.at[i], vr.at[i], to)

    def send_vec(i, carry):
        vec_copy(i, True).start()
        return carry

    lax.fori_loop(1, total, send_vec, 0)
    own_vec = pltpu.make_async_copy(vec_ref.at[me, mz], vb.at[0], ls.at[0])
    own_vec.start()

    def loads(j):
        a, s, order = chunks[j]
        place = (mz + s) % places
        out = []
        for i, m in enumerate(span(order[1:])):
            n = 1 + j * (count // 2) + i
            out.append(
                pltpu.make_async_copy(grs[a].at[place, flip(me, m)], acc.at[j, i], ls.at[n])
            )
        return out

    def copies(j, k):
        a, s, order = chunks[j]
        place = (mz + s) % places
        base = span(order[1:])
        out = []
        for i, m in enumerate(span(order[k + 1 :])):
            far = m | (1 << order[k])
            if k == 0:
                src = grs[a].at[place, flip(me, far)]
            else:
                src = acc.at[j, base.index(far)]
            n = j * (count - 1) + (count - (count >> k)) + i
            out.append(
                remote(
                    src, rbs[k].at[j, i], ks.at[n], kr.at[n], (flip(me, 1 << order[k]), mz)
                )
            )
        return out

    def z_copy(j):
        a, s, _ = chunks[j]
        n = a * (places - 1) + s - 1
        return remote(acc.at[j, 0], zb.at[a, s - 1], zs.at[n], zr.at[n], (me, (mz + s) % places))

    for j in range(len(chunks)):
        for copy in copies(j, 0):
            copy.start()
        for copy in loads(j):
            copy.start()
    for slot in range(len(chunks) + nbits - 1):
        for k in range(nbits - 1, -1, -1):
            j = slot - k
            if not 0 <= j < len(chunks):
                continue
            _, s, order = chunks[j]
            base = span(order[1:])
            if k == 0:
                for copy in loads(j):
                    copy.wait()
            for i, (m, copy) in enumerate(zip(span(order[k + 1 :]), copies(j, k))):
                copy.wait_recv()
                add_rows(acc.at[j, base.index(m)], rbs[k].at[j, i])
            if k + 1 < nbits:
                for copy in copies(j, k + 1):
                    copy.start()
            elif s > 0:
                z_copy(j).start()

    own_vec.wait()

    def wait_vec(i, carry):
        vec_copy(i, False).wait_recv()
        vec_copy(i, True).wait_send()
        return carry

    lax.fori_loop(1, total, wait_vec, 0)
    vout_ref[...] = jnp.sum(vb[...], axis=0)
    for a in range(arrays):
        for j, (b, s, _) in enumerate(chunks):
            if b == a and s > 0:
                z_copy(j).wait_recv()
        for j, (b, s, _) in enumerate(chunks):
            if b == a and s == 0:
                result = acc[j, 0].astype(F32)
                for other in range(places - 1):
                    result = result + zb[a, other].astype(F32)
                out_ref[a] = result
    for j, (_, s, _) in enumerate(chunks):
        for k in range(nbits):
            for copy in copies(j, k):
                copy.wait_send()
        if s > 0:
            z_copy(j).wait_send()


def scatter_all(grads, vectors):
    arrays = len(grads)
    places, count, rows, width = grads[0].shape
    nbits, chunks = scatter_plan(count, places, arrays)
    n = len(chunks)
    sem = pltpu.SemaphoreType.DMA
    return pl.pallas_call(
        functools.partial(scatter_kernel, count, places, arrays),
        out_shape=(
            jax.ShapeDtypeStruct((arrays, rows, width), F32),
            jax.ShapeDtypeStruct(vectors.shape[2:], F32),
        ),
        in_specs=[ANY] * (arrays + 1),
        out_specs=(VMEM, VMEM),
        scratch_shapes=[pltpu.VMEM((n, count // 2, rows, width), BF)]
        + [pltpu.VMEM((n, count >> (k + 1), rows, width), BF) for k in range(nbits)]
        + [
            pltpu.VMEM((arrays, places - 1, rows, width), BF),
            pltpu.VMEM((count * places,) + vectors.shape[2:], F32),
            sem((n * (count - 1),)),
            sem((n * (count - 1),)),
            sem((arrays * (places - 1),)),
            sem((arrays * (places - 1),)),
            sem((count * places,)),
            sem((count * places,)),
            sem((1 + n * (count // 2),)),
        ],
        compiler_params=pltpu.CompilerParams(
            has_side_effects=True, vmem_limit_bytes=VMEM_LIMIT
        ),
        name="scatter_all",
    )(*grads, vectors)


def turn_tiles(tiles, cosine, low, high):
    out = []
    for tile in tiles:
        ahead = pltpu.roll(tile, LANES - ROT // 2, 1)
        behind = pltpu.roll(tile, ROT // 2, 1)
        out.append(tile * cosine + ahead * low + behind * high)
    return out


def rotary_turns(offsets):
    half = ROT // 2
    freq = 10000.0 ** (-(2.0 * jnp.arange(half, dtype=F32)) / ROT)
    angles = offsets.astype(F32)[None, :] * freq[:, None]
    return jnp.concatenate([jnp.cos(angles), jnp.sin(angles)], axis=0)


def spread_turns(turns):
    half = ROT // 2
    lane = lax.broadcasted_iota(jnp.int32, (ROT, LANES), 1) % HD
    line = lax.broadcasted_iota(jnp.int32, (ROT, LANES), 0)
    picks = (
        jnp.where((lane < ROT) & (line == lane % half), 1.0, 0.0),
        jnp.where((lane < half) & (line == half + lane), -1.0, 0.0),
        jnp.where((lane >= half) & (lane < ROT) & (line == lane), 1.0, 0.0),
    )
    tables = [
        lax.dot_general(
            turns,
            pick,
            (((0,), (0,)), ((), ())),
            precision=lax.Precision.HIGHEST,
            preferred_element_type=F32,
        )
        for pick in picks
    ]
    column = lax.broadcasted_iota(jnp.int32, tables[0].shape, 1) % HD
    tables[0] = jnp.where(column < ROT, tables[0], 1.0)
    return tables


def project_kernel(wide, n1_ref, cot_ref, w_ref, b_ref, cs_ref, x_ref):
    full = 3 * wide
    cut = full // LANES * LANES
    part = full - cut
    w = w_ref[0]
    forward = dot(n1_ref[...], w[:, : cut + LANES], 1, 0) + b_ref[0]
    backward = dot(cot_ref[...], w[:, cut:], 1, 0)
    turned = 2 * wide // LANES
    tiles = [forward[:, i * LANES : (i + 1) * LANES] for i in range(turned)]
    tiles = turn_tiles(tiles, *spread_turns(cs_ref[...]))
    for i, tile in enumerate(tiles):
        x_ref[0, :, i * LANES : (i + 1) * LANES] = tile.astype(BF)
    x_ref[0, :, turned * LANES : cut] = forward[:, turned * LANES : cut].astype(BF)
    lane = lax.broadcasted_iota(jnp.int32, (forward.shape[0], LANES), 1)
    mixed = jnp.where(lane < part, forward[:, cut:], backward[:, :LANES])
    x_ref[0, :, cut : cut + LANES] = mixed.astype(BF)
    x_ref[0, :, cut + LANES :] = backward[:, LANES:].astype(BF)


def project(n1, cot, w, bias, turns, wide):
    places, model, width = w.shape
    rows = n1.shape[0]
    whole = pl.BlockSpec((rows, model), lambda z: (0, 0))
    return pl.pallas_call(
        functools.partial(project_kernel, wide),
        grid=(places,),
        out_shape=jax.ShapeDtypeStruct((places, rows, width), BF),
        in_specs=[
            whole,
            whole,
            pl.BlockSpec((1, model, width), lambda z: (z, 0, 0)),
            pl.BlockSpec((1, 1, bias.shape[2]), lambda z: (z, 0, 0)),
            pl.BlockSpec((ROT, rows), lambda z: (0, 0)),
        ],
        out_specs=pl.BlockSpec((1, rows, width), lambda z: (z, 0, 0)),
        compiler_params=pltpu.CompilerParams(vmem_limit_bytes=VMEM_LIMIT),
        name="project",
    )(n1, cot, w, bias, turns)


def attention_kernel(
    heads,
    block,
    y_ref,
    begin_ref,
    cs_ref,
    r_ref,
    bias_ref,
    qh,
    kh,
    vh,
    oh,
    kt,
    vt,
    s_scr,
    dq,
    dk,
    dv,
):
    total = y_ref.shape[0]
    wide = heads * HD
    scale = HD**-0.5
    blocks = total // block

    def prepare(i, carry):
        at = pl.ds(pl.multiple_of(i * block, block), block)
        for h in range(heads):
            q = y_ref[at, h * HD : (h + 1) * HD].astype(F32) * scale
            k = y_ref[at, wide + h * HD : wide + (h + 1) * HD].astype(F32)
            v = y_ref[at, 2 * wide + h * HD : 2 * wide + (h + 1) * HD].astype(F32)
            qh[h, at, :] = q.astype(BF)
            kh[h, at, :] = k.astype(BF)
            vh[h, at, :] = v.astype(BF)
            oh[h, at, :] = y_ref[at, 3 * wide + h * HD : 3 * wide + (h + 1) * HD]
            kt[h, :, at] = k.T.astype(BF)
            vt[h, :, at] = v.T.astype(BF)
            dk[h, at, :] = jnp.zeros((block, HD), F32)
            dv[h, at, :] = jnp.zeros((block, HD), F32)
        return carry

    lax.fori_loop(0, blocks, prepare, 0)

    def row_block(i, carry):
        at = pl.ds(pl.multiple_of(i * block, block), block)
        begin = begin_ref[0:1, at]
        last = i * block + lax.broadcasted_iota(jnp.int32, (1, block), 1)
        queries = [qh[h, at, :] for h in range(heads)]
        grads = [oh[h, at, :] for h in range(heads)]

        def scores(j, peaks):
            keys = pl.ds(pl.multiple_of(j * block, block), block)
            place = j * block + lax.broadcasted_iota(jnp.int32, (block, block), 0)
            allowed = (place >= begin) & (place <= last)
            out = []
            for h in range(heads):
                s = dot(kh[h, keys, :], queries[h], 1, 1)
                s = jnp.where(allowed, s, NEGATIVE)
                s_scr[h, keys, :] = s
                out.append(jnp.maximum(peaks[h], jnp.max(s.reshape(block // 8, 8, block), axis=0)))
            return tuple(out)

        start = tuple(jnp.full((8, block), NEGATIVE, F32) for _ in range(heads))
        peaks = lax.fori_loop(0, i + 1, scores, start)
        peaks = [jnp.max(p, axis=0, keepdims=True) for p in peaks]

        def weigh(j, state):
            keys = pl.ds(pl.multiple_of(j * block, block), block)
            out = []
            for h in range(heads):
                mass, acc = state[h]
                p = jnp.exp(s_scr[h, keys, :] - peaks[h])
                s_scr[h, keys, :] = p
                mass = mass + jnp.sum(p.reshape(block // 8, 8, block), axis=0)
                acc = acc + dot(vt[h, :, keys], p.astype(BF), 1, 0)
                out.append((mass, acc))
            return tuple(out)

        start = tuple(
            (jnp.zeros((8, block), F32), jnp.zeros((HD, block), F32)) for _ in range(heads)
        )
        state = lax.fori_loop(0, i + 1, weigh, start)
        inverses, deltas = [], []
        for h in range(heads):
            mass = jnp.sum(state[h][0], axis=0, keepdims=True)
            inverse = 1.0 / mass
            attended = (state[h][1] * inverse).astype(BF).astype(F32)
            deltas.append(
                jnp.sum(attended * grads[h].astype(F32).T, axis=0, keepdims=True)
            )
            inverses.append(inverse)
            r_ref[at, 3 * wide + h * HD : 3 * wide + (h + 1) * HD] = attended.T.astype(BF)

        def back(j, acc):
            keys = pl.ds(pl.multiple_of(j * block, block), block)
            out = []
            for h in range(heads):
                p = s_scr[h, keys, :] * inverses[h]
                dv[h, keys, :] += dot(p.astype(BF), grads[h], 1, 0)
                g = dot(vh[h, keys, :], grads[h], 1, 1)
                ds = (p * (g - deltas[h])).astype(BF)
                dk[h, keys, :] += dot(ds, queries[h], 1, 0)
                out.append(acc[h] + dot(kt[h, :, keys], ds, 1, 0))
            return tuple(out)

        start = tuple(jnp.zeros((HD, block), F32) for _ in range(heads))
        acc = lax.fori_loop(0, i + 1, back, start)
        for h in range(heads):
            dq[h, at, :] = (acc[h] * scale).T
        return carry

    lax.fori_loop(0, blocks, row_block, 0)

    def finish(i, sums):
        at = pl.ds(pl.multiple_of(i * block, block), block)
        pieces = [d[h, at, :] for d in (dq, dk, dv) for h in range(heads)]
        cosine, low, high = spread_turns(cs_ref[:, at])
        out = []
        turned = 2 * wide // LANES
        for t in range(3 * wide // LANES + 1):
            if 2 * t + 1 < len(pieces):
                tile = jnp.concatenate(pieces[2 * t : 2 * t + 2], axis=1)
            else:
                tile = pieces[2 * t]
            if t < turned:
                tile = turn_tiles([tile], cosine, -low, -high)[0]
            width = tile.shape[1]
            r_ref[at, t * LANES : t * LANES + width] = tile.astype(BF)
            out.append(sums[t] + jnp.sum(tile.reshape(block // 8, 8, width), axis=0))
        return tuple(out)

    start = []
    for t in range(3 * wide // LANES + 1):
        width = min(LANES, 3 * wide - t * LANES)
        start.append(jnp.zeros((8, width), F32))
    sums = lax.fori_loop(0, blocks, finish, tuple(start))
    for t, value in enumerate(sums):
        bias_ref[0:1, t * LANES : t * LANES + value.shape[1]] = jnp.sum(
            value, axis=0, keepdims=True
        )


def attention(y, begin, turns, heads):
    total, width = y.shape
    block = min(256, total)
    scratch = pltpu.VMEM
    return pl.pallas_call(
        functools.partial(attention_kernel, heads, block),
        out_shape=(
            jax.ShapeDtypeStruct((total, width), BF),
            jax.ShapeDtypeStruct((1, 3 * heads * HD), F32),
        ),
        in_specs=[VMEM] * 3,
        out_specs=(VMEM, VMEM),
        scratch_shapes=[scratch((heads, total, HD), BF)] * 4
        + [scratch((heads, HD, total), BF)] * 2
        + [scratch((heads, total, block), F32)]
        + [scratch((heads, total, HD), F32)] * 3,
        compiler_params=pltpu.CompilerParams(vmem_limit_bytes=VMEM_LIMIT),
        name="attention",
    )(y, begin, turns)


def feed_kernel(
    n2_ref, n2t_ref, cot_ref, cott_ref, up_ref, down_ref, b_ref, out_ref, back_ref, gu_ref, gd_ref, gb_ref
):
    @pl.when(pl.program_id(0) == 0)
    def _():
        out_ref[...] = jnp.zeros_like(out_ref)
        back_ref[...] = jnp.zeros_like(back_ref)

    up, down = up_ref[0, 0], down_ref[0, 0]
    pre = dot(n2_ref[...], up, 1, 0) + b_ref[0]
    bell = 0.5 * (1.0 + lax.erf(pre * 0.7071067811865476))
    activ = (pre * bell).astype(BF)
    out_ref[...] += dot(activ, down, 1, 1)
    gd_ref[0] = dot(cott_ref[...], activ, 1, 0).astype(BF)
    slope = bell + pre * jnp.exp(-0.5 * pre * pre) * 0.3989422804014327
    grad = dot(cot_ref[...], down, 1, 0) * slope
    gb_ref[0] = jnp.sum(grad, axis=0, keepdims=True)
    grad = grad.astype(BF)
    gu_ref[0] = dot(n2t_ref[...], grad, 1, 0).astype(BF)
    back_ref[...] += dot(grad, up, 1, 1)


def feed(n2, cot, w, bias):
    places, model, width = w.shape[1:]
    rows = n2.shape[0]
    whole = pl.BlockSpec((rows, model), lambda z: (0, 0))
    turned = pl.BlockSpec((model, rows), lambda z: (0, 0))
    square = pl.BlockSpec((1, model, width), lambda z: (z, 0, 0))
    return pl.pallas_call(
        feed_kernel,
        grid=(places,),
        out_shape=(
            jax.ShapeDtypeStruct((rows, model), F32),
            jax.ShapeDtypeStruct((rows, model), F32),
            jax.ShapeDtypeStruct((places, model, width), BF),
            jax.ShapeDtypeStruct((places, model, width), BF),
            jax.ShapeDtypeStruct((places, 1, width), F32),
        ),
        in_specs=[
            whole,
            turned,
            whole,
            turned,
            pl.BlockSpec((1, 1, model, width), lambda z: (1, z, 0, 0)),
            pl.BlockSpec((1, 1, model, width), lambda z: (2, z, 0, 0)),
            pl.BlockSpec((1, 1, width), lambda z: (z, 0, 0)),
        ],
        out_specs=(
            whole,
            whole,
            square,
            square,
            pl.BlockSpec((1, 1, width), lambda z: (z, 0, 0)),
        ),
        compiler_params=pltpu.CompilerParams(vmem_limit_bytes=VMEM_LIMIT),
        name="feed",
    )(n2, n2.T, cot, cot.T, w, w, bias)


def return_kernel(wide, n1t_ref, cott_ref, z_ref, w_ref, out_ref, back_ref, g_ref):
    @pl.when(pl.program_id(0) == 0)
    def _():
        out_ref[...] = jnp.zeros_like(out_ref)
        back_ref[...] = jnp.zeros_like(back_ref)

    full = 3 * wide
    cut = full // LANES * LANES
    part = full - cut
    z, w = z_ref[0], w_ref[0]
    lane = lax.broadcasted_iota(jnp.int32, (z.shape[0], LANES), 1)
    middle = z[:, cut : cut + LANES]
    none = jnp.zeros_like(middle)
    ours = jnp.where(lane < part, middle, none)
    theirs = jnp.where(lane < part, none, middle)
    back_ref[...] += dot(
        jnp.concatenate([z[:, :cut], ours], axis=1), w[:, : cut + LANES], 1, 1
    )
    out_ref[...] += dot(
        jnp.concatenate([theirs, z[:, cut + LANES :]], axis=1), w[:, cut:], 1, 1
    )
    first = dot(n1t_ref[...], z[:, : cut + LANES], 1, 0)
    second = dot(cott_ref[...], z[:, cut:], 1, 0)
    lane = lax.broadcasted_iota(jnp.int32, (first.shape[0], LANES), 1)
    g_ref[0, :, :cut] = first[:, :cut].astype(BF)
    g_ref[0, :, cut : cut + LANES] = jnp.where(
        lane < part, first[:, cut:], second[:, :LANES]
    ).astype(BF)
    g_ref[0, :, cut + LANES :] = second[:, LANES:].astype(BF)


def returning(n1, cot, z, w, wide):
    places, rows, width = z.shape
    model = n1.shape[1]
    turned = pl.BlockSpec((model, rows), lambda z: (0, 0))
    whole = pl.BlockSpec((rows, model), lambda z: (0, 0))
    return pl.pallas_call(
        functools.partial(return_kernel, wide),
        grid=(places,),
        out_shape=(
            jax.ShapeDtypeStruct((rows, model), F32),
            jax.ShapeDtypeStruct((rows, model), F32),
            jax.ShapeDtypeStruct((places, model, width), BF),
        ),
        in_specs=[
            turned,
            turned,
            pl.BlockSpec((1, rows, width), lambda z: (z, 0, 0)),
            pl.BlockSpec((1, model, width), lambda z: (z, 0, 0)),
        ],
        out_specs=(whole, whole, pl.BlockSpec((1, model, width), lambda z: (z, 0, 0))),
        compiler_params=pltpu.CompilerParams(vmem_limit_bytes=VMEM_LIMIT),
        name="returning",
    )(n1.T, cot.T, z, w)


def select_rows(values, pick, keep):
    spread = lax.dot_general(
        values,
        pick,
        (((1,), (0,)), ((), ())),
        precision=lax.Precision.HIGHEST,
        preferred_element_type=F32,
    )
    return jnp.where(keep, spread, 0.0)


def front_kernel(
    count,
    places,
    wide,
    piece,
    x_ref,
    cot_ref,
    w_ref,
    vec_ref,
    cs_ref,
    y_ref,
    p_ref,
    small_ref,
    out_ref,
    back_ref,
    gu_ref,
    gd_ref,
    gb_ref,
    g_ref,
    x_buf,
    n1_ref,
    n2_ref,
    cb_ref,
    n2t_ref,
    cbt_ref,
    table_ref,
    vb_ref,
    bq_ref,
    bu_ref,
    gu_buf,
    gd_buf,
    zs,
    zr,
    ds,
    dr,
    vs,
    vr,
    xs,
    xr,
    ls,
):
    me, mz = lax.axis_index("dp"), lax.axis_index("tensor")
    total = count * places
    rows, model = x_ref.shape
    ff = w_ref.shape[2]
    full = 3 * wide
    cut = full // LANES * LANES
    part = full - cut
    nbits = count.bit_length() - 1
    first = list(range(nbits - 1, -1, -1))
    second = [first[1], first[0]] + first[2:] if nbits >= 3 else first
    order_s = [0] + shift_order(places)
    head_chunks = [(0, s, (first, second)[i % 2]) for i, s in enumerate(order_s)]
    feed_chunks = [
        (a, s, (first, second)[(i + a + 1) % 2]) for i, s in enumerate(order_s) for a in (1, 2)
    ]
    chunks = head_chunks + feed_chunks

    def vec_copy(i, sending):
        di, zi = i // places, i % places
        if sending:
            slot = me * places + mz
        else:
            slot = ((me + count - di) % count) * places + (mz + places - zi) % places
        return remote(
            vec_ref,
            vb_ref.at[slot],
            vs.at[i],
            vr.at[i],
            ((me + di) % count, (mz + zi) % places),
        )

    def z_copy(a, s, sending):
        slot = mz if sending else (mz + places - s) % places
        n = a * (places - 1) + s - 1
        return remote(
            w_ref.at[a], g_ref.at[a, slot, me], zs.at[n], zr.at[n], (me, (mz + s) % places)
        )

    def d_copies(j, k, sending):
        a, s, order = chunks[j]
        place = (mz + places - s) % places
        bit = order[k]
        out = []
        for i, m in enumerate(span(order[:k])):
            slot = flip(me, m if sending else m | (1 << bit))
            src = w_ref.at[a] if s == 0 and m == 0 and sending else g_ref.at[a, place, slot]
            n = j * (count - 1) + (1 << k) - 1 + i
            out.append(
                remote(
                    src,
                    g_ref.at[a, place, slot],
                    ds.at[n],
                    dr.at[n],
                    (flip(me, 1 << bit), mz),
                )
            )
        return out

    def step(j, k):
        a, s, _ = chunks[j]
        if k == 0:
            if s > 0:
                z_copy(a, s, False).wait_recv()
        else:
            for copy in d_copies(j, k - 1, False):
                copy.wait_recv()
        if k < nbits:
            for copy in d_copies(j, k, True):
                copy.start()

    def slot_steps(slot, low, high):
        for k in range(nbits, -1, -1):
            j = low + slot - k
            if low <= j < high and slot - k >= 0:
                step(j, k)

    def x_copy(s, sending):
        to = (mz + s) % places
        slot = mz if sending else (mz + places - s) % places
        return remote(x_buf.at[to], y_ref.at[slot], xs.at[s], xr.at[s], (me, to))

    own = [
        pltpu.make_async_copy(w_ref.at[a], g_ref.at[a, mz, me], ls.at[a]) for a in range(3)
    ]
    own_vec = pltpu.make_async_copy(vec_ref, vb_ref.at[me * places + mz], ls.at[3])

    def send_vec(i, carry):
        vec_copy(i, True).start()
        return carry

    lax.fori_loop(1, total, send_vec, 0)
    own_vec.start()
    step(0, 0)
    for s in shift_order(places):
        z_copy(0, s, True).start()
    for copy in own:
        copy.start()

    mine = cs_ref[:, pl.ds(pl.multiple_of(mz * rows, rows), rows)]
    for i, table in enumerate(spread_turns(mine)):
        table_ref[i] = table

    def wait_vec(i, carry):
        vec_copy(i, False).wait_recv()
        return carry

    own_vec.wait()
    lax.fori_loop(1, total, wait_vec, 0)
    values = vb_ref[...].reshape(total * 8, LANES)
    sub = lax.broadcasted_iota(jnp.int32, (total * 8, 1), 0)
    who, what = sub // 8, sub % 8
    which = lax.broadcasted_iota(jnp.int32, (LANES, 1), 0)

    def pick_of(at):
        return jnp.where(which == at, 1.0, 0.0)

    at = lax.broadcasted_iota(jnp.int32, (1, model), 1)
    kept = select_rows(values, pick_of(at % piece), who == at // piece)
    small_ref[...] = jnp.sum(kept.reshape(total, 8, model), axis=0)
    each = wide // count
    at = lax.broadcasted_iota(jnp.int32, (1, cut + LANES), 1)
    inner = at % wide
    kept = select_rows(
        values,
        pick_of((at // wide) * each + inner % each),
        (what == 5) & (at < full) & (who // places == inner // each),
    )
    for z in range(places):
        bq_ref[z : z + 1, :] = jnp.sum(
            jnp.where(who % places == z, kept, 0.0), axis=0, keepdims=True
        )
    each = ff // count
    at = lax.broadcasted_iota(jnp.int32, (1, ff), 1)
    kept = select_rows(
        values, pick_of(at % each), (what == 6) & (who // places == at // each)
    )
    for z in range(places):
        bu_ref[z : z + 1, :] = jnp.sum(
            jnp.where(who % places == z, kept, 0.0), axis=0, keepdims=True
        )

    block = rows // 4

    def norm(i):
        here = slice(i * block, (i + 1) * block)
        values = x_ref[here, :]
        center = values - jnp.mean(values, axis=1, keepdims=True)
        inverse = lax.rsqrt(jnp.mean(center * center, axis=1, keepdims=True) + EPSILON)
        normal = center * inverse
        n1_ref[here, :] = (normal * small_ref[0:1, :] + small_ref[1:2, :]).astype(BF)
        second_norm = normal * small_ref[2:3, :] + small_ref[3:4, :]
        n2_ref[here, :] = second_norm.astype(BF)
        n2t_ref[:, here] = second_norm.astype(BF).astype(F32).T.astype(BF)
        cot = cot_ref[here, :]
        cb_ref[here, :] = cot.astype(BF)
        cbt_ref[:, here] = cot.T.astype(BF)

    heads_end = len(head_chunks)
    for slot in range(1, heads_end + nbits):
        if slot == heads_end:
            for s in shift_order(places):
                for a in (1, 2):
                    z_copy(a, s, True).start()
        slot_steps(slot, 0, heads_end)
        if slot <= 4:
            norm(slot - 1)
    own[0].wait()
    save = pltpu.make_async_copy(g_ref.at[0], p_ref, ls.at[4])
    save.start()

    end = len(chunks)
    to_order = shift_order(places)[::-1] + [0]
    keep_own = pltpu.make_async_copy(x_buf.at[mz], y_ref.at[mz], ls.at[5])
    for i, s in enumerate(to_order):
        slot_steps(i, heads_end, end)
        to = (mz + s) % places
        w = g_ref[0, to].reshape(model, ff)
        forward = dot(n1_ref[...], w[:, : cut + LANES], 1, 0) + bq_ref[pl.ds(to, 1), :]
        backward = dot(cb_ref[...], w[:, cut:], 1, 0)
        turned = 2 * wide // LANES
        tiles = [forward[:, t * LANES : (t + 1) * LANES] for t in range(turned)]
        tiles = turn_tiles(tiles, table_ref[0], table_ref[1], table_ref[2])
        for t, tile in enumerate(tiles):
            x_buf[to, :, t * LANES : (t + 1) * LANES] = tile.astype(BF)
        x_buf[to, :, turned * LANES : cut] = forward[:, turned * LANES : cut].astype(BF)
        column = lax.broadcasted_iota(jnp.int32, (rows, LANES), 1)
        mixed = jnp.where(column < part, forward[:, cut:], backward[:, :LANES])
        x_buf[to, :, cut : cut + LANES] = mixed.astype(BF)
        x_buf[to, :, cut + LANES :] = backward[:, LANES:].astype(BF)
        if s > 0:
            x_copy(s, True).start()
        else:
            keep_own.start()

    out_ref[...] = jnp.zeros_like(out_ref)
    back_ref[...] = jnp.zeros_like(back_ref)
    own[1].wait()
    own[2].wait()
    width = ff // 2
    puts = []
    slot = len(to_order)
    last = len(feed_chunks) + nbits
    for i, s in enumerate(order_s):
        place = (mz + places - s) % places
        ready = 2 * i + 1 + nbits
        while slot <= ready:
            slot_steps(slot, heads_end, end)
            slot += 1
        for h in range(2):
            cols = slice(h * width, (h + 1) * width)
            up = g_ref[1, place, :, :, cols].reshape(model, width)
            down = g_ref[2, place, :, :, cols].reshape(model, width)
            pre = dot(n2_ref[...], up, 1, 0) + bu_ref[pl.ds(place, 1), cols]
            bell = 0.5 * (1.0 + lax.erf(pre * 0.7071067811865476))
            activ = (pre * bell).astype(BF)
            out_ref[...] += dot(activ, down, 1, 1)
            gd_buf[i, :, cols] = dot(cbt_ref[...], activ, 1, 0).astype(BF)
            slope = bell + pre * jnp.exp(-0.5 * pre * pre) * 0.3989422804014327
            grad = dot(cb_ref[...], down, 1, 0) * slope
            gb_ref[pl.ds(place, 1), cols] = jnp.sum(grad, axis=0, keepdims=True)
            grad = grad.astype(BF)
            gu_buf[i, :, cols] = dot(n2t_ref[...], grad, 1, 0).astype(BF)
            back_ref[...] += dot(grad, up, 1, 1)
            if h == 0 and slot < last:
                slot_steps(slot, heads_end, end)
                slot += 1
        for a, (buf, ref) in enumerate(((gu_buf, gu_ref), (gd_buf, gd_ref))):
            puts.append(pltpu.make_async_copy(buf.at[i], ref.at[place], ls.at[6 + 2 * i + a]))
            puts[-1].start()

    save.wait()
    keep_own.wait()
    for copy in puts:
        copy.wait()
    for s in range(1, places):
        x_copy(s, False).wait_recv()
    for s in range(1, places):
        x_copy(s, True).wait_send()

    def wait_sent(i, carry):
        vec_copy(i, True).wait_send()
        return carry

    lax.fori_loop(1, total, wait_sent, 0)
    for a in range(3):
        for s in range(1, places):
            z_copy(a, s, True).wait_send()
    for j in range(len(chunks)):
        for k in range(nbits):
            for copy in d_copies(j, k, True):
                copy.wait_send()


def front(block_input, cotangent, weights, vector, turns, count, places, wide, piece):
    rows, model = block_input.shape
    depth, ff = weights.shape[1:]
    total = count * places
    sem = pltpu.SemaphoreType.DMA
    shape = jax.ShapeDtypeStruct
    cut = 3 * wide // LANES * LANES
    return pl.pallas_call(
        functools.partial(front_kernel, count, places, wide, piece),
        out_shape=(
            shape((places, rows, ff), BF),
            shape((places, count, depth, ff), BF),
            shape((8, model), F32),
            shape((rows, model), F32),
            shape((rows, model), F32),
            shape((places, model, ff), BF),
            shape((places, model, ff), BF),
            shape((places, ff), F32),
        ),
        in_specs=[VMEM] * 5,
        out_specs=(ANY, ANY, VMEM, VMEM, VMEM, ANY, ANY, VMEM),
        scratch_shapes=[
            pltpu.VMEM((3, places, count, depth, ff), BF),
            pltpu.VMEM((places, rows, ff), BF),
            pltpu.VMEM((rows, model), BF),
            pltpu.VMEM((rows, model), BF),
            pltpu.VMEM((rows, model), BF),
            pltpu.VMEM((model, rows), BF),
            pltpu.VMEM((model, rows), BF),
            pltpu.VMEM((3, rows, LANES), F32),
            pltpu.VMEM((total, 8, LANES), F32),
            pltpu.VMEM((places, cut + LANES), F32),
            pltpu.VMEM((places, ff), F32),
            pltpu.VMEM((places, model, ff), BF),
            pltpu.VMEM((places, model, ff), BF),
            sem((3 * (places - 1),)),
            sem((3 * (places - 1),)),
            sem((3 * places * (count - 1),)),
            sem((3 * places * (count - 1),)),
            sem((total,)),
            sem((total,)),
            sem((places,)),
            sem((places,)),
            sem((6 + 2 * places,)),
        ],
        compiler_params=pltpu.CompilerParams(
            has_side_effects=True, vmem_limit_bytes=VMEM_LIMIT
        ),
        name="front",
    )(block_input, cotangent, weights, vector, turns)


def norm_back(grad_out, normal, inverse, gain):
    scaled = grad_out * gain
    return inverse * (
        scaled
        - jnp.mean(scaled, axis=1, keepdims=True)
        - normal * jnp.mean(scaled * normal, axis=1, keepdims=True)
    )


def lanes(values, width=LANES):
    return jnp.pad(values, [(0, 0)] * (values.ndim - 1) + [(0, width - values.shape[-1])])


def shards(
    count,
    places,
    block_input,
    cotangent,
    segment_ids,
    token_offset,
    first_gain,
    first_shift,
    second_gain,
    second_shift,
    qkv_weight,
    qkv_bias,
    proj_weight,
    up_weight,
    up_bias,
    down_weight,
    out_bias,
):
    rows, model = block_input.shape
    depth = qkv_weight.shape[1]
    wide = qkv_weight.shape[2]
    heads = wide // HD
    ff = up_weight.shape[1]
    piece = first_gain.shape[0]
    total = segment_ids.shape[0]
    place = lax.axis_index("tensor")

    attn = jnp.concatenate([qkv_weight[0], qkv_weight[1], qkv_weight[2], proj_weight.T], axis=1)
    packed = jnp.stack([attn, up_weight, down_weight.T])
    vector = jnp.stack(
        [lanes(v) for v in (first_gain, first_shift, second_gain, second_shift, out_bias)]
        + [lanes(qkv_bias.astype(F32).reshape(-1)), lanes(up_bias.astype(F32))]
        + [jnp.zeros((LANES,), F32)]
    )
    turns = rotary_turns(token_offset)
    begin = (jnp.arange(total, dtype=jnp.int32) - token_offset)[None, :]
    center = block_input - jnp.mean(block_input, axis=1, keepdims=True)
    inverse = lax.rsqrt(jnp.mean(center * center, axis=1, keepdims=True) + EPSILON)
    normal = center * inverse
    cot = cotangent.astype(BF)
    if depth % 16 == 0:
        y, attn_weights, small, out_two, grad_two, up_grad, down_grad, up_bias_part = front(
            block_input, cotangent, packed, vector, turns, count, places, wide, piece
        )
        attn_weights = attn_weights.reshape(places, model, ff)
        gain_one, shift_one, gain_two, shift_two, bias_out = (small[i] for i in range(5))
        n1 = (normal * gain_one + shift_one).astype(BF)
    else:
        weights, vectors = gather_all(packed, vector, count, places)
        weights = weights.reshape(3, places, model, ff)
        attn_weights = weights[0]
        small = vectors[:, :, :5, :piece].transpose(2, 0, 1, 3).reshape(5, model)
        gain_one, shift_one, gain_two, shift_two, bias_out = (small[i] for i in range(5))
        bias_qkv = (
            vectors[:, :, 5, : 3 * wide // count]
            .reshape(count, places, 3, wide // count)
            .transpose(1, 2, 0, 3)
            .reshape(places, 1, 3 * wide)
        )
        cut = 3 * wide // LANES * LANES
        bias_qkv = lanes(bias_qkv, cut + LANES)
        bias_up = vectors[:, :, 6, : ff // count].transpose(1, 0, 2).reshape(places, 1, ff)
        n1 = (normal * gain_one + shift_one).astype(BF)
        n2 = (normal * gain_two + shift_two).astype(BF)
        mine = lax.dynamic_slice_in_dim(turns, place * rows, rows, 1)
        y = exchange(project(n1, cot, attn_weights, bias_qkv, mine, wide), places)
        out_two, grad_two, up_grad, down_grad, up_bias_part = feed(n2, cot, weights, bias_up)
    r, qkv_bias_part = attention(y.reshape(total, y.shape[2]), begin, turns, heads)
    z = exchange(r.reshape(places, rows, r.shape[1]), places)
    out_one, grad_one, attn_grad = returning(n1, cot, z, attn_weights, wide)

    block_output = block_input + (out_one + out_two) + bias_out
    input_grad = (
        cotangent
        + norm_back(grad_one, normal, inverse, gain_one)
        + norm_back(grad_two, normal, inverse, gain_two)
    )
    sums = jnp.stack(
        [
            jnp.sum(grad_one * normal, axis=0),
            jnp.sum(grad_one, axis=0),
            jnp.sum(grad_two * normal, axis=0),
            jnp.sum(grad_two, axis=0),
            jnp.sum(cotangent, axis=0),
        ]
    )
    sums = lanes(sums.reshape(5, count, places, piece).transpose(1, 2, 0, 3))
    qkv_sum = qkv_bias_part.reshape(3, count, wide // count).transpose(1, 0, 2)
    qkv_sum = lanes(qkv_sum.reshape(count, 1, 3 * wide // count))
    here = jnp.arange(places, dtype=jnp.int32)[None, :, None, None] == place
    qkv_sum = jnp.where(here, qkv_sum[:, None], 0.0)
    up_sum = lanes(up_bias_part.reshape(places, count, ff // count).transpose(1, 0, 2))[:, :, None]
    parts = jnp.concatenate([sums, qkv_sum, up_sum, jnp.zeros_like(up_sum)], axis=2)

    grads = [g.reshape(places, count, depth, ff) for g in (attn_grad, up_grad, down_grad)]
    done, vec = scatter_all(grads, parts)
    attn_done = done[0]
    qkv_weight_grad = jnp.stack([attn_done[:, i * wide : (i + 1) * wide] for i in range(3)])
    return (
        block_output,
        input_grad,
        vec[0, :piece],
        vec[1, :piece],
        vec[2, :piece],
        vec[3, :piece],
        qkv_weight_grad,
        vec[5, : 3 * wide // count].reshape(3, wide // count),
        attn_done[:, 3 * wide :].T,
        done[1],
        vec[6, : ff // count],
        done[2].T,
        vec[4, :piece],
    )


def solution(mesh):
    both = P(("dp", "tensor"))
    return jax.shard_map(
        functools.partial(shards, mesh.shape["dp"], mesh.shape["tensor"]),
        mesh=mesh,
        in_specs=(
            P(("dp", "tensor"), None),
            P(("dp", "tensor"), None),
            P("dp"),
            P("dp"),
            both,
            both,
            both,
            both,
            P(None, "dp", "tensor"),
            P(None, ("tensor", "dp")),
            P("tensor", "dp"),
            P("dp", "tensor"),
            P(("tensor", "dp")),
            P("tensor", "dp"),
            both,
        ),
        out_specs=(
            P(("dp", "tensor"), None),
            P(("dp", "tensor"), None),
            both,
            both,
            both,
            both,
            P(None, "dp", "tensor"),
            P(None, ("tensor", "dp")),
            P("tensor", "dp"),
            P("dp", "tensor"),
            P(("tensor", "dp")),
            P("tensor", "dp"),
            both,
        ),
        check_vma=False,
    )
```

```python
import functools

import jax
import jax.numpy as jnp
from jax import lax
from jax.experimental import pallas as pl
from jax.experimental.pallas import tpu as pltpu
from jax.sharding import PartitionSpec as P

HD = 64
ROT = 16
EPSILON = 1e-05
NEGATIVE = -1e30
LANES = 128
GROUP = 4 * HD
BF = jnp.bfloat16
F32 = jnp.float32
ANY = pl.BlockSpec(memory_space=pl.ANY)
VMEM = pl.BlockSpec(memory_space=pltpu.VMEM)
VMEM_LIMIT = 60 * 1024 * 1024


def dot(a, b, ca, cb):
    return lax.dot_general(a, b, (((ca,), (cb,)), ((), ())), preferred_element_type=F32)


def flip(index, mask):
    out = index
    bit = 0
    while (1 << bit) <= mask:
        if (mask >> bit) & 1:
            step = 1 << bit
            out = out + (1 - 2 * ((index // step) % 2)) * step
        bit += 1
    return out


def span(bits):
    masks = [0]
    for bit in bits:
        masks = masks + [m | (1 << bit) for m in masks]
    return masks


def remote(src, dst, send_sem, recv_sem, device):
    return pltpu.make_async_remote_copy(
        src_ref=src,
        dst_ref=dst,
        send_sem=send_sem,
        recv_sem=recv_sem,
        device_id=device,
        device_id_type=pl.DeviceIdType.MESH,
    )


def turn_tiles(tiles, cosine, low, high):
    out = []
    for tile in tiles:
        ahead = pltpu.roll(tile, LANES - ROT // 2, 1)
        behind = pltpu.roll(tile, ROT // 2, 1)
        out.append(tile * cosine + ahead * low + behind * high)
    return out


def rotary_turns(offsets):
    half = ROT // 2
    freq = 10000.0 ** (-(2.0 * jnp.arange(half, dtype=F32)) / ROT)
    angles = offsets.astype(F32)[None, :] * freq[:, None]
    return jnp.concatenate([jnp.cos(angles), jnp.sin(angles)], axis=0)


def spread_turns(turns):
    half = ROT // 2
    lane = lax.broadcasted_iota(jnp.int32, (ROT, LANES), 1) % HD
    line = lax.broadcasted_iota(jnp.int32, (ROT, LANES), 0)
    picks = (
        jnp.where((lane < ROT) & (line == lane % half), 1.0, 0.0),
        jnp.where((lane < half) & (line == half + lane), -1.0, 0.0),
        jnp.where((lane >= half) & (lane < ROT) & (line == lane), 1.0, 0.0),
    )
    tables = [
        lax.dot_general(
            turns,
            pick,
            (((0,), (0,)), ((), ())),
            precision=lax.Precision.HIGHEST,
            preferred_element_type=F32,
        )
        for pick in picks
    ]
    column = lax.broadcasted_iota(jnp.int32, tables[0].shape, 1) % HD
    tables[0] = jnp.where(column < ROT, tables[0], 1.0)
    return tables


def select_rows(values, pick, keep):
    spread = lax.dot_general(
        values,
        pick,
        (((1,), (0,)), ((), ())),
        precision=lax.Precision.HIGHEST,
        preferred_element_type=F32,
    )
    return jnp.where(keep, spread, 0.0)


def front_kernel(
    count,
    places,
    wide,
    piece,
    x_ref,
    cot_ref,
    w_ref,
    vec_ref,
    cs_ref,
    y_ref,
    p_ref,
    small_ref,
    out_ref,
    back_ref,
    gu_ref,
    gd_ref,
    gb_ref,
    g_ref,
    x_buf,
    n1_ref,
    n2_ref,
    cb_ref,
    n2t_ref,
    cbt_ref,
    table_ref,
    vb_ref,
    bq_ref,
    bu_ref,
    gu_buf,
    gd_buf,
    zs,
    zr,
    ds,
    dr,
    vs,
    vr,
    xs,
    xr,
    ls,
):
    me, mz = lax.axis_index("dp"), lax.axis_index("tensor")
    total = count * places
    rows, model = x_ref.shape
    ff = w_ref.shape[2]
    nbits = count.bit_length() - 1
    first = list(range(nbits - 1, -1, -1))
    second = [first[1], first[0]] + first[2:] if nbits >= 3 else first
    head_chunks = [(0, s, (first, second)[s % 2]) for s in range(places)]
    feed_chunks = [(a, s, (first, second)[a - 1]) for s in range(places) for a in (1, 2)]
    chunks = head_chunks + feed_chunks

    def vec_copy(i, sending):
        di, zi = i // places, i % places
        if sending:
            slot = me * places + mz
        else:
            slot = ((me + count - di) % count) * places + (mz + places - zi) % places
        return remote(
            vec_ref,
            vb_ref.at[slot],
            vs.at[i],
            vr.at[i],
            ((me + di) % count, (mz + zi) % places),
        )

    def z_copy(a, s, sending):
        slot = mz if sending else (mz + places - s) % places
        n = a * (places - 1) + s - 1
        return remote(
            w_ref.at[a], g_ref.at[a, slot, me], zs.at[n], zr.at[n], (me, (mz + s) % places)
        )

    def d_copies(j, k, sending):
        a, s, order = chunks[j]
        place = (mz + places - s) % places
        bit = order[k]
        out = []
        for i, m in enumerate(span(order[:k])):
            slot = flip(me, m if sending else m | (1 << bit))
            src = w_ref.at[a] if s == 0 and m == 0 and sending else g_ref.at[a, place, slot]
            n = j * (count - 1) + (1 << k) - 1 + i
            out.append(
                remote(
                    src,
                    g_ref.at[a, place, slot],
                    ds.at[n],
                    dr.at[n],
                    (flip(me, 1 << bit), mz),
                )
            )
        return out

    def step(j, k):
        a, s, _ = chunks[j]
        if k == 0:
            if s > 0:
                z_copy(a, s, False).wait_recv()
        else:
            for copy in d_copies(j, k - 1, False):
                copy.wait_recv()
        if k < nbits:
            for copy in d_copies(j, k, True):
                copy.start()

    def slot_steps(slot, low, high, lag, skip=()):
        for k in range(nbits, -1, -1):
            pair = slot - lag * k
            for j in (low + 2 * pair, low + 2 * pair + 1):
                if pair >= 0 and j < high and (j, k) not in skip:
                    step(j, k)

    def x_copy(h, s, sending):
        to = (mz + s) % places
        slot = mz if sending else (mz + places - s) % places
        n = h * places + s
        return remote(x_buf.at[to, h], y_ref.at[h, slot], xs.at[n], xr.at[n], (me, to))

    def keep_own(h):
        return pltpu.make_async_copy(x_buf.at[mz, h], y_ref.at[h, mz], ls.at[5 + h])

    own = [
        pltpu.make_async_copy(w_ref.at[a], g_ref.at[a, mz, me], ls.at[a]) for a in range(3)
    ]
    own_vec = pltpu.make_async_copy(vec_ref, vb_ref.at[me * places + mz], ls.at[3])

    def send_vec(i, carry):
        vec_copy(i, True).start()
        return carry

    lax.fori_loop(1, total, send_vec, 0)
    own_vec.start()
    heads_end = len(head_chunks)
    end = len(chunks)
    early = [(0, 0), (heads_end, 0), (heads_end + 1, 0)]
    for j, k in early:
        step(j, k)
    for a in range(3):
        for s in range(1, places):
            z_copy(a, s, True).start()
    for copy in own:
        copy.start()

    mine = cs_ref[:, pl.ds(pl.multiple_of(mz * rows, rows), rows)]
    for i, table in enumerate(spread_turns(mine)):
        table_ref[i] = table

    def wait_vec(i, carry):
        vec_copy(i, False).wait_recv()
        return carry

    own_vec.wait()
    lax.fori_loop(1, total, wait_vec, 0)
    values = vb_ref[...].reshape(total * 8, LANES)
    sub = lax.broadcasted_iota(jnp.int32, (total * 8, 1), 0)
    who, what = sub // 8, sub % 8
    which = lax.broadcasted_iota(jnp.int32, (LANES, 1), 0)

    def pick_of(at):
        return jnp.where(which == at, 1.0, 0.0)

    at = lax.broadcasted_iota(jnp.int32, (1, model), 1)
    kept = select_rows(values, pick_of(at % piece), who == at // piece)
    small_ref[...] = jnp.sum(kept.reshape(total, 8, model), axis=0)
    each = wide // count
    at = lax.broadcasted_iota(jnp.int32, (1, ff), 1)
    kind = at % GROUP // HD
    inner = at // GROUP * HD + at % HD
    kept = select_rows(
        values,
        pick_of(kind * each + inner % each),
        (what == 5) & (kind < 3) & (who // places == inner // each),
    )
    for z in range(places):
        bq_ref[z : z + 1, :] = jnp.sum(
            jnp.where(who % places == z, kept, 0.0), axis=0, keepdims=True
        )
    each = ff // count
    at = lax.broadcasted_iota(jnp.int32, (1, ff), 1)
    kept = select_rows(
        values, pick_of(at % each), (what == 6) & (who // places == at // each)
    )
    for z in range(places):
        bu_ref[z : z + 1, :] = jnp.sum(
            jnp.where(who % places == z, kept, 0.0), axis=0, keepdims=True
        )

    block = rows // 4

    def norm(i):
        here = slice(i * block, (i + 1) * block)
        values = x_ref[here, :]
        center = values - jnp.mean(values, axis=1, keepdims=True)
        inverse = lax.rsqrt(jnp.mean(center * center, axis=1, keepdims=True) + EPSILON)
        normal = center * inverse
        n1_ref[here, :] = (normal * small_ref[0:1, :] + small_ref[1:2, :]).astype(BF)
        second_norm = normal * small_ref[2:3, :] + small_ref[3:4, :]
        n2_ref[here, :] = second_norm.astype(BF)
        n2t_ref[:, here] = second_norm.astype(BF).astype(F32).T.astype(BF)
        cot = cot_ref[here, :]
        cb_ref[here, :] = cot.astype(BF)
        cbt_ref[:, here] = cot.T.astype(BF)

    slot_count = (heads_end + 1) // 2 + nbits
    for slot in range(slot_count):
        slot_steps(slot, 0, heads_end, 1, early)
        if slot < 4:
            norm(slot)
    for i in range(slot_count, 4):
        norm(i)
    own[0].wait()
    save = pltpu.make_async_copy(g_ref.at[0], p_ref, ls.at[4])
    save.start()

    lag = 2
    heads = ff // GROUP

    def project(i, carry):
        for slot in range(places):

            @pl.when(i == slot)
            def _():
                slot_steps(slot, heads_end, end, lag, early)

        to = (mz + 1 + i) % places
        w = g_ref[0, to].reshape(model, ff)
        forward = dot(n1_ref[...], w, 1, 0) + bq_ref[pl.ds(to, 1), :]
        column = lax.broadcasted_iota(jnp.int32, (rows, LANES), 1)
        for h in range(heads):
            tile = forward[:, h * GROUP : h * GROUP + LANES]
            tile = turn_tiles([tile], table_ref[0], table_ref[1], table_ref[2])[0]
            x_buf[to, h, :, :LANES] = tile.astype(BF)
            late = slice(h * GROUP + LANES, (h + 1) * GROUP)
            backward = dot(cb_ref[...], w[:, late], 1, 0)
            tile = jnp.where(column < HD, forward[:, late], backward)
            x_buf[to, h, :, LANES:] = tile.astype(BF)

        @pl.when(i < places - 1)
        def _():
            for h in range(heads):
                x_copy(h, 1 + i, True).start()

        @pl.when(i == places - 1)
        def _():
            for h in range(heads):
                keep_own(h).start()

        return carry

    lax.fori_loop(0, places, project, 0)

    out_ref[...] = jnp.zeros_like(out_ref)
    back_ref[...] = jnp.zeros_like(back_ref)
    own[1].wait()
    own[2].wait()
    width = ff // 2

    def puts(i):
        place = (mz + places - i) % places
        return [
            pltpu.make_async_copy(
                buf.at[i], ref.at[place], ls.at[5 + heads + 2 * i + a]
            )
            for a, (buf, ref) in enumerate(((gu_buf, gu_ref), (gd_buf, gd_ref)))
        ]

    def feed(f, carry):
        slot = places
        for i in range(places):
            until = i + lag * nbits

            @pl.when(f == 2 * i)
            def _(slot=slot, until=until):
                for t in range(slot, until + 1):
                    slot_steps(t, heads_end, end, lag, early)

            slot = max(slot, until + 1)
        i, h = f // 2, f % 2
        place = (mz + places - i) % places
        cols = pl.ds(pl.multiple_of(h * width, width), width)
        up = g_ref[1, place, :, :, cols].reshape(model, width)
        down = g_ref[2, place, :, :, cols].reshape(model, width)
        pre = dot(n2_ref[...], up, 1, 0) + bu_ref[pl.ds(place, 1), cols]
        bell = 0.5 * (1.0 + lax.erf(pre * 0.7071067811865476))
        activ = (pre * bell).astype(BF)
        out_ref[...] += dot(activ, down, 1, 1)
        gd_buf[i, :, cols] = dot(cbt_ref[...], activ, 1, 0).astype(BF)
        slope = bell + pre * jnp.exp(-0.5 * pre * pre) * 0.3989422804014327
        grad = dot(cb_ref[...], down, 1, 0) * slope
        gb_ref[pl.ds(place, 1), cols] = jnp.sum(grad, axis=0, keepdims=True)
        grad = grad.astype(BF)
        gu_buf[i, :, cols] = dot(n2t_ref[...], grad, 1, 0).astype(BF)
        back_ref[...] += dot(grad, up, 1, 1)

        @pl.when(h == 1)
        def _():
            for copy in puts(i):
                copy.start()

        return carry

    lax.fori_loop(0, 2 * places, feed, 0)

    save.wait()
    for i in range(places):
        for copy in puts(i):
            copy.wait()
    for h in range(heads):
        keep_own(h).wait()
        for s in range(1, places):
            x_copy(h, s, False).wait_recv()
        for s in range(1, places):
            x_copy(h, s, True).wait_send()

    def wait_sent(i, carry):
        vec_copy(i, True).wait_send()
        return carry

    lax.fori_loop(1, total, wait_sent, 0)
    for a in range(3):
        for s in range(1, places):
            z_copy(a, s, True).wait_send()
    for j in range(len(chunks)):
        for k in range(nbits):
            for copy in d_copies(j, k, True):
                copy.wait_send()


def front(block_input, cotangent, weights, vector, turns, count, places, wide, piece):
    rows, model = block_input.shape
    depth, ff = weights.shape[1:]
    total = count * places
    heads = ff // GROUP
    sem = pltpu.SemaphoreType.DMA
    shape = jax.ShapeDtypeStruct
    return pl.pallas_call(
        functools.partial(front_kernel, count, places, wide, piece),
        out_shape=(
            shape((heads, places, rows, GROUP), BF),
            shape((places, count, depth, ff), BF),
            shape((8, model), F32),
            shape((rows, model), F32),
            shape((rows, model), F32),
            shape((places, model, ff), BF),
            shape((places, model, ff), BF),
            shape((places, ff), F32),
        ),
        in_specs=[VMEM] * 5,
        out_specs=(ANY, ANY, VMEM, VMEM, VMEM, ANY, ANY, VMEM),
        scratch_shapes=[
            pltpu.VMEM((3, places, count, depth, ff), BF),
            pltpu.VMEM((places, heads, rows, GROUP), BF),
            pltpu.VMEM((rows, model), BF),
            pltpu.VMEM((rows, model), BF),
            pltpu.VMEM((rows, model), BF),
            pltpu.VMEM((model, rows), BF),
            pltpu.VMEM((model, rows), BF),
            pltpu.VMEM((3, rows, LANES), F32),
            pltpu.VMEM((total, 8, LANES), F32),
            pltpu.VMEM((places, ff), F32),
            pltpu.VMEM((places, ff), F32),
            pltpu.VMEM((places, model, ff), BF),
            pltpu.VMEM((places, model, ff), BF),
            sem((3 * (places - 1),)),
            sem((3 * (places - 1),)),
            sem((3 * places * (count - 1),)),
            sem((3 * places * (count - 1),)),
            sem((total,)),
            sem((total,)),
            sem((heads * places,)),
            sem((heads * places,)),
            sem((5 + heads + 2 * places,)),
        ],
        compiler_params=pltpu.CompilerParams(
            has_side_effects=True, vmem_limit_bytes=VMEM_LIMIT
        ),
        name="front",
    )(block_input, cotangent, weights, vector, turns)


class Scatter:
    def __init__(self, count, places, chunks, sources, acc, landing, sems, local):
        self.me, self.mz = lax.axis_index("dp"), lax.axis_index("tensor")
        self.count, self.places, self.chunks, self.sources = count, places, chunks, sources
        self.acc, self.landing, self.sems, self.local = acc, landing, sems, local
        self.nbits = count.bit_length() - 1

    @staticmethod
    def orders(count):
        nbits = count.bit_length() - 1
        first = list(range(nbits))
        return first, ([first[0], first[2], first[1]] + first[3:] if nbits >= 3 else first)

    def copies(self, j, k):
        a, s, order = self.chunks[j]
        to = (flip(self.me, 1 << order[k]), self.mz)
        half = self.count >> (k + 1)
        base = j * (half_of(self.count) + self.nbits - 1)
        send, recv = self.sems
        if k > 0:
            n = base + half_of(self.count) + k - 1
            src = self.acc.at[j, half : 2 * half]
            return [remote(src, self.landing[k].at[j], send.at[n], recv.at[n], to)]
        place = (self.mz + s) % self.places
        out = []
        for i, m in enumerate(span(order[1:][::-1])):
            slot = flip(self.me, m | (1 << order[0]))
            out.append(
                remote(
                    self.sources[a].at[place, slot],
                    self.landing[0].at[j, i],
                    send.at[base + i],
                    recv.at[base + i],
                    to,
                )
            )
        return out

    def loads(self, j):
        a, s, order = self.chunks[j]
        place = (self.mz + s) % self.places
        return [
            pltpu.make_async_copy(
                self.sources[a].at[place, flip(self.me, m)],
                self.acc.at[j, i],
                self.local.at[j * half_of(self.count) + i],
            )
            for i, m in enumerate(span(order[1:][::-1]))
        ]

    def start(self, j):
        for copy in self.copies(j, 0) + self.loads(j):
            copy.start()

    def stage(self, j, k, final=None):
        if k == 0:
            for copy in self.loads(j):
                copy.wait()
        for copy in self.copies(j, k):
            copy.wait_recv()
        half = self.count >> (k + 1)
        rows = self.acc.shape[2]
        step = 32 if rows % 32 == 0 else rows
        parts = rows // step
        target = self.acc.at[j] if final is None else final

        def body(i, carry):
            shard, at = i // parts, pl.ds(pl.multiple_of(i % parts * step, step), step)
            mine = self.acc[j, shard, at, :].astype(F32)
            other = self.landing[k][j, shard, at, :].astype(F32)
            target[shard, at, :] = (mine + other).astype(BF)
            return carry

        lax.fori_loop(0, half * parts, body, 0)
        if k + 1 < self.nbits:
            for copy in self.copies(j, k + 1):
                copy.start()

    def drain(self):
        for j in range(len(self.chunks)):
            for k in range(self.nbits):
                for copy in self.copies(j, k):
                    copy.wait_send()

    @staticmethod
    def scratch(count, chunks, rows, width):
        nbits = count.bit_length() - 1
        sem = pltpu.SemaphoreType.DMA
        copies = chunks * (half_of(count) + nbits - 1)
        return (
            [pltpu.VMEM((chunks, half_of(count), rows, width), BF)]
            + [pltpu.VMEM((chunks, count >> (k + 1), rows, width), BF) for k in range(nbits)]
            + [sem((copies,)), sem((copies,)), sem((chunks * half_of(count),))]
        )


def half_of(count):
    return count // 2


def middle_kernel(count, places, heads, wq, wk, *refs):
    y_ref, begin_ref, cs_ref, gu_ref, gd_ref, z_ref, bias_ref, red_ref = refs[:8]
    r_buf, qh, kh, vh, oh, kt, vt, s_scr, dq, dk, dv, at_scr, table_ref = refs[8:21]
    ss, rs, ls, acc = refs[21:25]
    nbits = count.bit_length() - 1
    landing = refs[25 : 25 + nbits]
    send, recv, local = refs[25 + nbits :]
    me, mz = lax.axis_index("dp"), lax.axis_index("tensor")
    total = y_ref.shape[1]
    rows = total // places
    scale = HD**-0.5
    nq = total // wq
    ratio = wq // wk

    chunks = []
    for s in list(range(1, places)) + [0]:
        for a in range(2):
            chunks.append((a, s, Scatter.orders(count)[a]))
    scatter = Scatter(
        count, places, chunks, (gu_ref, gd_ref), acc, landing, (send, recv), local
    )
    events = {}
    last_step = heads * nq
    for k in range(nbits):
        for pair in range(len(chunks) // 2):
            when = (2 + pair // 2, 5 + pair)[k] if k < 2 else 9 + pair + 4 * (k - 2)
            events.setdefault(min(when, last_step), []).append((pair, k))

    def run_events(step):
        for pair, k in events.get(step, []):
            for j in (2 * pair, 2 * pair + 1):
                a, s, _ = chunks[j]
                final = red_ref.at[a, pl.ds(s, 1)] if k == nbits - 1 else None
                scatter.stage(j, k, final)

    for j in range(len(chunks)):
        scatter.start(j)

    def tables(i, carry):
        at = pl.ds(pl.multiple_of(i * wk, wk), wk)
        cosine, low, high = spread_turns(cs_ref[:, at])
        table_ref[0, at, :] = cosine
        table_ref[1, at, :] = -low
        table_ref[2, at, :] = -high
        return carry

    lax.fori_loop(0, total // wk, tables, 0)

    def back_copy(h, s, sending):
        to = (mz + s) % places
        slot = mz if sending else (mz + places - s) % places
        n = h * places + s
        return remote(r_buf.at[h, to], z_ref.at[slot, h], ss.at[n], rs.at[n], (me, to))

    def keep_own(h):
        return pltpu.make_async_copy(r_buf.at[h, mz], z_ref.at[mz, h], ls.at[h])

    def flat(t, carry):
        h, i = t // nq, t % nq
        for step in sorted(events):
            if step < last_step:

                @pl.when(t == step)
                def _(step=step):
                    run_events(step)

        @pl.when(i == 0)
        def _():
            def prepare(b, carry):
                at = pl.ds(pl.multiple_of(b * wk, wk), wk)
                both = y_ref[h, at, :LANES].astype(F32)
                q, k = both[:, :HD] * scale, both[:, HD:]
                both = y_ref[h, at, LANES:].astype(F32)
                v, o = both[:, :HD], both[:, HD:]
                qh[at, :] = q.astype(BF)
                kh[at, :] = k.astype(BF)
                vh[at, :] = v.astype(BF)
                oh[at, :] = o.astype(BF)
                kt[:, at] = k.T.astype(BF)
                vt[:, at] = v.T.astype(BF)
                dk[at, :] = jnp.zeros((wk, HD), F32)
                dv[at, :] = jnp.zeros((wk, HD), F32)
                return carry

            lax.fori_loop(0, total // wk, prepare, 0)

        at = pl.ds(pl.multiple_of(i * wq, wq), wq)
        begin = begin_ref[0:1, at]
        last = i * wq + lax.broadcasted_iota(jnp.int32, (1, wq), 1)
        query, grad = qh[at, :], oh[at, :]
        trips = (i + 1) * ratio

        def scores(j, peak):
            keys = pl.ds(pl.multiple_of(j * wk, wk), wk)
            place = j * wk + lax.broadcasted_iota(jnp.int32, (wk, wq), 0)
            s = dot(kh[keys, :], query, 1, 1)
            s = jnp.where((place >= begin) & (place <= last), s, NEGATIVE)
            s_scr[keys, :] = s
            return jnp.maximum(peak, jnp.max(s.reshape(wk // 8, 8, wq), axis=0))

        peak = lax.fori_loop(0, trips, scores, jnp.full((8, wq), NEGATIVE, F32))
        peak = jnp.max(peak, axis=0, keepdims=True)

        def weigh(j, state):
            mass, out = state
            keys = pl.ds(pl.multiple_of(j * wk, wk), wk)
            p = jnp.exp(s_scr[keys, :] - peak)
            s_scr[keys, :] = p
            mass = mass + jnp.sum(p.reshape(wk // 8, 8, wq), axis=0)
            return mass, out + dot(vt[:, keys], p.astype(BF), 1, 0)

        mass, out = lax.fori_loop(
            0, trips, weigh, (jnp.zeros((8, wq), F32), jnp.zeros((HD, wq), F32))
        )
        inverse = 1.0 / jnp.sum(mass, axis=0, keepdims=True)
        attended = (out * inverse).astype(BF).astype(F32)
        delta = jnp.sum(attended * grad.astype(F32).T, axis=0, keepdims=True)
        at_scr[at, :] = attended.T

        def back(j, out):
            keys = pl.ds(pl.multiple_of(j * wk, wk), wk)
            p = s_scr[keys, :] * inverse
            dv[keys, :] += dot(p.astype(BF), grad, 1, 0)
            g = dot(vh[keys, :], grad, 1, 1)
            ds = (p * (g - delta)).astype(BF)
            dk[keys, :] += dot(ds, query, 1, 0)
            return out + dot(kt[:, keys], ds, 1, 0)

        out = lax.fori_loop(0, trips, back, jnp.zeros((HD, wq), F32))
        dq[at, :] = (out * scale).T

        @pl.when(i == nq - 1)
        def _():
            per = rows // wk

            def finish(b, sums):
                at = pl.ds(pl.multiple_of(b * wk, wk), wk)
                inside = pl.ds(pl.multiple_of(b % per * wk, wk), wk)
                tile = jnp.concatenate([dq[at, :], dk[at, :]], axis=1)
                tile = turn_tiles(
                    [tile], table_ref[0, at, :], table_ref[1, at, :], table_ref[2, at, :]
                )[0]
                r_buf[h, b // per, inside, :LANES] = tile.astype(BF)
                other = jnp.concatenate([dv[at, :], at_scr[at, :]], axis=1)
                r_buf[h, b // per, inside, LANES:] = other.astype(BF)
                return tuple(
                    total + jnp.sum(x.reshape(wk // 8, 8, LANES), axis=0)
                    for total, x in zip(sums, (tile, other))
                )

            zero = jnp.zeros((8, LANES), F32)
            sums = lax.fori_loop(0, total // wk, finish, (zero, zero))
            for c, value in enumerate(sums):
                bias_ref[h, :, c * LANES : (c + 1) * LANES] = value
            for s in range(1, places):
                back_copy(h, s, True).start()
            keep_own(h).start()

        return carry

    lax.fori_loop(0, last_step, flat, 0)
    run_events(last_step)
    for h in range(heads):
        keep_own(h).wait()
        for s in range(1, places):
            back_copy(h, s, False).wait_recv()
        for s in range(1, places):
            back_copy(h, s, True).wait_send()
    scatter.drain()


def middle(y, begin, turns, up_grad, down_grad):
    heads, total, group = y.shape
    places, count, depth, ff = up_grad.shape
    wq, wk = min(512, total), min(256, total)
    vmem = pltpu.VMEM
    sem = pltpu.SemaphoreType.DMA
    shape = jax.ShapeDtypeStruct
    return pl.pallas_call(
        functools.partial(middle_kernel, count, places, heads, wq, wk),
        out_shape=(
            shape((places, heads, total // places, group), BF),
            shape((heads, 8, group), F32),
            shape((2, places, depth, ff), BF),
        ),
        in_specs=[VMEM, VMEM, VMEM, ANY, ANY],
        out_specs=(ANY, VMEM, VMEM),
        scratch_shapes=[vmem((heads, places, total // places, group), BF)]
        + [vmem((total, HD), BF)] * 4
        + [vmem((HD, total), BF)] * 2
        + [vmem((total, wq), F32)]
        + [vmem((total, HD), F32)] * 4
        + [vmem((3, total, LANES), F32)]
        + [sem((heads * places,)), sem((heads * places,)), sem((heads,))]
        + Scatter.scratch(count, 2 * places, depth, ff),
        compiler_params=pltpu.CompilerParams(
            has_side_effects=True, vmem_limit_bytes=VMEM_LIMIT
        ),
        name="middle",
    )(y, begin, turns, up_grad, down_grad)


def return_kernel(n1t_ref, cb_ref, z_ref, w_ref, out_ref, back_ref, g_ref):
    @pl.when(pl.program_id(0) == 0)
    def _():
        out_ref[...] = jnp.zeros_like(out_ref)
        back_ref[...] = jnp.zeros_like(back_ref)

    heads = z_ref.shape[1]
    rows = z_ref.shape[2]
    model = w_ref.shape[1]
    left = lax.broadcasted_iota(jnp.int32, (rows, LANES), 1) < HD
    wide_left = lax.broadcasted_iota(jnp.int32, (model, LANES), 1) < HD
    out, back = out_ref[...], back_ref[...]
    for h in range(heads):
        z = z_ref[0, h]
        w = w_ref[0, :, h * GROUP : (h + 1) * GROUP]
        late = z[:, LANES:]
        none = jnp.zeros_like(late)
        ours = jnp.concatenate([z[:, :LANES], jnp.where(left, late, none)], axis=1)
        back = back + dot(ours, w, 1, 1)
        out = out + dot(jnp.where(left, none, late), w[:, LANES:], 1, 1)
        first = dot(n1t_ref[...], z, 1, 0)
        second = dot(cb_ref[...], late, 1, 0)
        g_ref[0, :, h * GROUP : h * GROUP + LANES] = first[:, :LANES].astype(BF)
        g_ref[0, :, h * GROUP + LANES : (h + 1) * GROUP] = jnp.where(
            wide_left, first[:, LANES:], second
        ).astype(BF)
    out_ref[...] = out
    back_ref[...] = back


def returning(n1, cot, z, w):
    places, heads, rows, group = z.shape
    model, width = w.shape[1:]
    turned = pl.BlockSpec((model, rows), lambda z: (0, 0))
    whole = pl.BlockSpec((rows, model), lambda z: (0, 0))
    square = pl.BlockSpec((1, model, width), lambda z: (z, 0, 0))
    return pl.pallas_call(
        return_kernel,
        grid=(places,),
        out_shape=(
            jax.ShapeDtypeStruct((rows, model), F32),
            jax.ShapeDtypeStruct((rows, model), F32),
            jax.ShapeDtypeStruct((places, model, width), BF),
        ),
        in_specs=[
            turned,
            turned,
            pl.BlockSpec((1, heads, rows, group), lambda z: (z, 0, 0, 0)),
            square,
        ],
        out_specs=(whole, whole, square),
        compiler_params=pltpu.CompilerParams(vmem_limit_bytes=VMEM_LIMIT),
        name="returning",
    )(n1.T, cot.T, z, w)


def last_kernel(count, places, *refs):
    g_ref, red_ref, vec_ref, out_ref, vout_ref, zb, vb, zs, zr, vs, vr, ls, acc = refs[:13]
    nbits = count.bit_length() - 1
    landing = refs[13 : 13 + nbits]
    send, recv, local = refs[13 + nbits :]
    me, mz = lax.axis_index("dp"), lax.axis_index("tensor")
    total = count * places

    def vec_copy(i, sending):
        to = ((me + i // places) % count, (mz + i % places) % places)
        return remote(vec_ref.at[to[0], to[1]], vb.at[i], vs.at[i], vr.at[i], to)

    def send_vec(i, carry):
        vec_copy(i, True).start()
        return carry

    chunks = []
    for i, s in enumerate(list(range(1, places)) + [0]):
        chunks.append((0, s, Scatter.orders(count)[i % 2]))
    scatter = Scatter(count, places, chunks, (g_ref,), acc, landing, (send, recv), local)
    for j in range(len(chunks)):
        scatter.start(j)

    def z_copy(a, s):
        n = a * (places - 1) + s - 1
        if a == 0:
            src = acc.at[s - 1, 0]
        else:
            src = red_ref.at[a - 1, s]
        return remote(src, zb.at[a, s - 1], zs.at[n], zr.at[n], (me, (mz + s) % places))

    for a in (1, 2):
        for s in range(1, places):
            z_copy(a, s).start()
    lax.fori_loop(1, total, send_vec, 0)
    own_vec = pltpu.make_async_copy(vec_ref.at[me, mz], vb.at[0], ls.at[0])
    own_vec.start()
    for slot in range((len(chunks) + 1) // 2 + nbits - 1):
        for k in range(nbits - 1, -1, -1):
            pair = slot - k
            for j in (2 * pair, 2 * pair + 1):
                if 0 <= pair and j < len(chunks):
                    scatter.stage(j, k)
                    if k == nbits - 1 and chunks[j][1] > 0:
                        z_copy(0, chunks[j][1]).start()
    own_vec.wait()

    def wait_vec(i, carry):
        vec_copy(i, False).wait_recv()
        vec_copy(i, True).wait_send()
        return carry

    lax.fori_loop(1, total, wait_vec, 0)
    vout_ref[...] = jnp.sum(vb[...], axis=0)
    for a in (1, 2, 0):
        for s in range(1, places):
            z_copy(a, s).wait_recv()
        own = acc[places - 1, 0] if a == 0 else red_ref[a - 1, 0]
        result = own.astype(F32)
        for s in range(1, places):
            result = result + zb[a, s - 1].astype(F32)
        out_ref[a] = result
    scatter.drain()
    for a in range(3):
        for s in range(1, places):
            z_copy(a, s).wait_send()


def scatter_last(grad, partly, vectors):
    places, count, rows, width = grad.shape
    total = count * places
    sem = pltpu.SemaphoreType.DMA
    return pl.pallas_call(
        functools.partial(last_kernel, count, places),
        out_shape=(
            jax.ShapeDtypeStruct((3, rows, width), F32),
            jax.ShapeDtypeStruct(vectors.shape[2:], F32),
        ),
        in_specs=[ANY, VMEM, ANY],
        out_specs=(VMEM, VMEM),
        scratch_shapes=[
            pltpu.VMEM((3, places - 1, rows, width), BF),
            pltpu.VMEM((total,) + vectors.shape[2:], F32),
            sem((3 * (places - 1),)),
            sem((3 * (places - 1),)),
            sem((total,)),
            sem((total,)),
            sem((1,)),
        ]
        + Scatter.scratch(count, places, rows, width),
        compiler_params=pltpu.CompilerParams(
            has_side_effects=True, vmem_limit_bytes=VMEM_LIMIT
        ),
        name="scatter_last",
    )(grad, partly, vectors)


def norm_back(grad_out, normal, inverse, gain):
    scaled = grad_out * gain
    return inverse * (
        scaled
        - jnp.mean(scaled, axis=1, keepdims=True)
        - normal * jnp.mean(scaled * normal, axis=1, keepdims=True)
    )


def lanes(values, width=LANES):
    return jnp.pad(values, [(0, 0)] * (values.ndim - 1) + [(0, width - values.shape[-1])])


def shards(
    count,
    places,
    block_input,
    cotangent,
    segment_ids,
    token_offset,
    first_gain,
    first_shift,
    second_gain,
    second_shift,
    qkv_weight,
    qkv_bias,
    proj_weight,
    up_weight,
    up_bias,
    down_weight,
    out_bias,
):
    rows, model = block_input.shape
    depth = qkv_weight.shape[1]
    wide = qkv_weight.shape[2]
    heads = wide // HD
    ff = up_weight.shape[1]
    piece = first_gain.shape[0]
    total = segment_ids.shape[0]
    place = lax.axis_index("tensor")

    attn = jnp.stack([qkv_weight[0], qkv_weight[1], qkv_weight[2], proj_weight.T])
    attn = attn.reshape(4, depth, heads, HD).transpose(1, 2, 0, 3).reshape(depth, 4 * wide)
    packed = jnp.stack([attn, up_weight, down_weight.T])
    vector = jnp.stack(
        [lanes(v) for v in (first_gain, first_shift, second_gain, second_shift, out_bias)]
        + [lanes(qkv_bias.astype(F32).reshape(-1)), lanes(up_bias.astype(F32))]
        + [jnp.zeros((LANES,), F32)]
    )
    turns = rotary_turns(token_offset)
    begin = (jnp.arange(total, dtype=jnp.int32) - token_offset)[None, :]
    y, attn_weights, small, out_two, grad_two, up_grad, down_grad, up_bias_part = front(
        block_input, cotangent, packed, vector, turns, count, places, wide, piece
    )
    attn_weights = attn_weights.reshape(places, model, ff)
    gain_one, shift_one, gain_two, shift_two, bias_out = (small[i] for i in range(5))
    z, qkv_bias_part, partly = middle(
        y.reshape(heads, total, GROUP),
        begin,
        turns,
        up_grad.reshape(places, count, depth, ff),
        down_grad.reshape(places, count, depth, ff),
    )
    center = block_input - jnp.mean(block_input, axis=1, keepdims=True)
    inverse = lax.rsqrt(jnp.mean(center * center, axis=1, keepdims=True) + EPSILON)
    normal = center * inverse
    n1 = (normal * gain_one + shift_one).astype(BF)
    out_one, grad_one, attn_grad = returning(n1, cotangent.astype(BF), z, attn_weights)

    block_output = block_input + (out_one + out_two) + bias_out
    input_grad = (
        cotangent
        + norm_back(grad_one, normal, inverse, gain_one)
        + norm_back(grad_two, normal, inverse, gain_two)
    )
    sums = jnp.stack(
        [
            jnp.sum(grad_one * normal, axis=0),
            jnp.sum(grad_one, axis=0),
            jnp.sum(grad_two * normal, axis=0),
            jnp.sum(grad_two, axis=0),
            jnp.sum(cotangent, axis=0),
        ]
    )
    sums = lanes(sums.reshape(5, count, places, piece).transpose(1, 2, 0, 3))
    qkv_sum = jnp.sum(qkv_bias_part, axis=1).reshape(heads, 4, HD)[:, :3].transpose(1, 0, 2)
    qkv_sum = qkv_sum.reshape(3, count, wide // count).transpose(1, 0, 2)
    qkv_sum = lanes(qkv_sum.reshape(count, 1, 3 * wide // count))
    here = jnp.arange(places, dtype=jnp.int32)[None, :, None, None] == place
    qkv_sum = jnp.where(here, qkv_sum[:, None], 0.0)
    up_sum = lanes(up_bias_part.reshape(places, count, ff // count).transpose(1, 0, 2))[:, :, None]
    parts = jnp.concatenate([sums, qkv_sum, up_sum, jnp.zeros_like(up_sum)], axis=2)

    done, vec = scatter_last(attn_grad.reshape(places, count, depth, ff), partly, parts)
    attn_done = done[0].reshape(depth, heads, 4, HD).transpose(2, 0, 1, 3).reshape(4, depth, wide)
    return (
        block_output,
        input_grad,
        vec[0, :piece],
        vec[1, :piece],
        vec[2, :piece],
        vec[3, :piece],
        attn_done[:3],
        vec[5, : 3 * wide // count].reshape(3, wide // count),
        attn_done[3].T,
        done[1],
        vec[6, : ff // count],
        done[2].T,
        vec[4, :piece],
    )


def solution(mesh):
    both = P(("dp", "tensor"))
    return jax.shard_map(
        functools.partial(shards, mesh.shape["dp"], mesh.shape["tensor"]),
        mesh=mesh,
        in_specs=(
            P(("dp", "tensor"), None),
            P(("dp", "tensor"), None),
            P("dp"),
            P("dp"),
            both,
            both,
            both,
            both,
            P(None, "dp", "tensor"),
            P(None, ("tensor", "dp")),
            P("tensor", "dp"),
            P("dp", "tensor"),
            P(("tensor", "dp")),
            P("tensor", "dp"),
            both,
        ),
        out_specs=(
            P(("dp", "tensor"), None),
            P(("dp", "tensor"), None),
            both,
            both,
            both,
            both,
            P(None, "dp", "tensor"),
            P(None, ("tensor", "dp")),
            P("tensor", "dp"),
            P("dp", "tensor"),
            P(("tensor", "dp")),
            P("tensor", "dp"),
            both,
        ),
        check_vma=False,
    )
```

```python
import functools

import jax
import jax.numpy as jnp
from jax import lax
from jax.experimental import pallas as pl
from jax.experimental.pallas import tpu as pltpu
from jax.sharding import PartitionSpec as P

HD = 64
ROT = 16
EPSILON = 1e-05
NEGATIVE = -1e30
LANES = 128
GROUP = 4 * HD
BF = jnp.bfloat16
F32 = jnp.float32
ANY = pl.BlockSpec(memory_space=pl.ANY)
VMEM = pl.BlockSpec(memory_space=pltpu.VMEM)
VMEM_LIMIT = 60 * 1024 * 1024


def dot(a, b, ca, cb):
    return lax.dot_general(a, b, (((ca,), (cb,)), ((), ())), preferred_element_type=F32)


def flip(index, mask):
    out = index
    bit = 0
    while (1 << bit) <= mask:
        if (mask >> bit) & 1:
            step = 1 << bit
            out = out + (1 - 2 * ((index // step) % 2)) * step
        bit += 1
    return out


def span(bits):
    masks = [0]
    for bit in bits:
        masks = masks + [m | (1 << bit) for m in masks]
    return masks


def same(index, value, count):
    return 1 - ((index + count - value) % count + count - 1) // count


def nearest(place, turn, count):
    out = 0
    for p in range(count):
        order = sorted(range(count), key=lambda q: (abs(q - p), q < count - 1 - p))
        out = out + same(place, p, count) * order[turn]
    return out


def remote(src, dst, send_sem, recv_sem, device):
    return pltpu.make_async_remote_copy(
        src_ref=src,
        dst_ref=dst,
        send_sem=send_sem,
        recv_sem=recv_sem,
        device_id=device,
        device_id_type=pl.DeviceIdType.MESH,
    )


def turn_tiles(tiles, cosine, low, high):
    out = []
    for tile in tiles:
        ahead = pltpu.roll(tile, LANES - ROT // 2, 1)
        behind = pltpu.roll(tile, ROT // 2, 1)
        out.append(tile * cosine + ahead * low + behind * high)
    return out


def rotary_turns(offsets):
    half = ROT // 2
    freq = 10000.0 ** (-(2.0 * jnp.arange(half, dtype=F32)) / ROT)
    angles = offsets.astype(F32)[None, :] * freq[:, None]
    return jnp.concatenate([jnp.cos(angles), jnp.sin(angles)], axis=0)


def spread_turns(turns):
    half = ROT // 2
    lane = lax.broadcasted_iota(jnp.int32, (ROT, LANES), 1) % HD
    line = lax.broadcasted_iota(jnp.int32, (ROT, LANES), 0)
    picks = (
        jnp.where((lane < ROT) & (line == lane % half), 1.0, 0.0),
        jnp.where((lane < half) & (line == half + lane), -1.0, 0.0),
        jnp.where((lane >= half) & (lane < ROT) & (line == lane), 1.0, 0.0),
    )
    tables = [
        lax.dot_general(
            turns,
            pick,
            (((0,), (0,)), ((), ())),
            precision=lax.Precision.HIGHEST,
            preferred_element_type=F32,
        )
        for pick in picks
    ]
    column = lax.broadcasted_iota(jnp.int32, tables[0].shape, 1) % HD
    tables[0] = jnp.where(column < ROT, tables[0], 1.0)
    return tables


def select_rows(values, pick, keep):
    spread = lax.dot_general(
        values,
        pick,
        (((1,), (0,)), ((), ())),
        precision=lax.Precision.HIGHEST,
        preferred_element_type=F32,
    )
    return jnp.where(keep, spread, 0.0)


def front_kernel(
    count,
    places,
    wide,
    piece,
    x_ref,
    cot_ref,
    w_ref,
    vec_ref,
    cs_ref,
    y_ref,
    p_ref,
    small_ref,
    two_ref,
    grad_ref,
    gu_ref,
    gd_ref,
    gb_ref,
    out_ref,
    back_ref,
    g_ref,
    x_buf,
    n1_ref,
    n2_ref,
    cb_ref,
    n2t_ref,
    cbt_ref,
    table_ref,
    vb_ref,
    bq_ref,
    bu_ref,
    gu_buf,
    gd_buf,
    zs,
    zr,
    ds,
    dr,
    vs,
    vr,
    xs,
    xr,
    ls,
):
    me, mz = lax.axis_index("dp"), lax.axis_index("tensor")
    total = count * places
    rows, model = x_ref.shape
    ff = w_ref.shape[2]
    nbits = count.bit_length() - 1
    first = list(range(nbits - 1, -1, -1))
    second = [first[1], first[0]] + first[2:] if nbits >= 3 else first
    turns = list(range(places))
    pairs = [
        tuple((0, t, (first, second)[t % 2]) for t in turns[n : n + 2])
        for n in range(0, places, 2)
    ]
    head_pairs = len(pairs)
    pairs += [((1, t, first), (2, t, second)) for t in turns]
    chunks = [chunk for pair in pairs for chunk in pair]
    numbers, n = [], 0
    for pair in pairs:
        numbers.append(list(range(n, n + len(pair))))
        n += len(pair)

    def source(t):
        return nearest(mz, t, places)

    def source_at(i):
        return sum(same(i, t, places) * source(t) for t in turns)

    def vec_copy(i, sending):
        di, zi = i // places, i % places
        if sending:
            slot = me * places + mz
        else:
            slot = ((me + count - di) % count) * places + (mz + places - zi) % places
        return remote(
            vec_ref,
            vb_ref.at[slot],
            vs.at[i],
            vr.at[i],
            ((me + di) % count, (mz + zi) % places),
        )

    def z_copy(a, p, up, own=False):
        src = w_ref.at[a] if own else g_ref.at[a, p, me]
        return remote(
            src,
            g_ref.at[a, p, me],
            zs.at[(a * places + p) * 2 + (0 if up else 1)],
            zr.at[a * places + p],
            (me, mz + 1 if up else mz - 1),
        )

    def pass_on(a, p, own=False):
        @pl.when((p <= mz) & (mz < places - 1))
        def _():
            z_copy(a, p, True, own).start()

        @pl.when((p >= mz) & (mz > 0))
        def _():
            z_copy(a, p, False, own).start()

    def d_copies(j, k, sending):
        a, t, order = chunks[j]
        place = source(t)
        bit = order[k]
        out = []
        for i, m in enumerate(span(order[:k])):
            slot = flip(me, m if sending else m | (1 << bit))
            src = w_ref.at[a] if t == 0 and m == 0 and sending else g_ref.at[a, place, slot]
            n = j * (count - 1) + (1 << k) - 1 + i
            out.append(
                remote(
                    src,
                    g_ref.at[a, place, slot],
                    ds.at[n],
                    dr.at[n],
                    (flip(me, 1 << bit), mz),
                )
            )
        return out

    def step(j, k):
        a, t, _ = chunks[j]
        if k == 0:
            if t > 0:
                p = source(t)
                z_copy(a, p, True).wait_recv()
                pass_on(a, p)
        else:
            for copy in d_copies(j, k - 1, False):
                copy.wait_recv()
        if k < nbits:
            for copy in d_copies(j, k, True):
                copy.start()

    def pair_step(pair, k):
        for j in numbers[pair]:
            if k > 0 or chunks[j][1] > 0:
                step(j, k)

    def x_copy(h, p, sending):
        slot = mz if sending else p
        return remote(
            x_buf.at[p, h],
            y_ref.at[h, slot],
            xs.at[h * places + p],
            xr.at[h * places + slot],
            (me, p),
        )

    def keep_own(h):
        return pltpu.make_async_copy(x_buf.at[mz, h], y_ref.at[h, mz], ls.at[5 + h])

    schedule = []
    for pair in range(len(pairs)):
        head = pair < head_pairs
        for k in range(nbits + 1):
            at = 3 * k + 2 * pair if head else 3 * k + 2 * pair + 2
            schedule.append((at, -k, pair))
    schedule = [(pair, -k) for _, k, pair in sorted(schedule)]
    head_done = max(i for i, (p, k) in enumerate(schedule) if p < head_pairs and k == nbits) + 1
    feed_done = [schedule.index((head_pairs + t, nbits)) + 1 for t in turns]

    def run(low, high):
        for pair, k in schedule[low:high]:
            pair_step(pair, k)

    own = [
        pltpu.make_async_copy(w_ref.at[a], g_ref.at[a, mz, me], ls.at[a]) for a in range(3)
    ]
    own_vec = pltpu.make_async_copy(vec_ref, vb_ref.at[me * places + mz], ls.at[3])

    def send_vec(i, carry):
        vec_copy(i, True).start()
        return carry

    lax.fori_loop(1, total, send_vec, 0)
    own_vec.start()
    for j in [n for n, chunk in enumerate(chunks) if chunk[1] == 0]:
        step(j, 0)
    for a in range(3):
        pass_on(a, mz, True)
    for copy in own:
        copy.start()

    mine = cs_ref[:, pl.ds(pl.multiple_of(mz * rows, rows), rows)]
    for i, table in enumerate(spread_turns(mine)):
        table_ref[i] = table

    run(0, 2)

    def wait_vec(i, carry):
        vec_copy(i, False).wait_recv()
        return carry

    own_vec.wait()
    lax.fori_loop(1, total, wait_vec, 0)
    values = vb_ref[...].reshape(total * 8, LANES)
    sub = lax.broadcasted_iota(jnp.int32, (total * 8, 1), 0)
    who, what = sub // 8, sub % 8
    which = lax.broadcasted_iota(jnp.int32, (LANES, 1), 0)

    def pick_of(at):
        return jnp.where(which == at, 1.0, 0.0)

    at = lax.broadcasted_iota(jnp.int32, (1, model), 1)
    kept = select_rows(values, pick_of(at % piece), who == at // piece)
    small_ref[...] = jnp.sum(kept.reshape(total, 8, model), axis=0)
    each = wide // count
    at = lax.broadcasted_iota(jnp.int32, (1, ff), 1)
    kind = at % GROUP // HD
    inner = at // GROUP * HD + at % HD
    kept = select_rows(
        values,
        pick_of(kind * each + inner % each),
        (what == 5) & (kind < 3) & (who // places == inner // each),
    )
    for z in range(places):
        bq_ref[z : z + 1, :] = jnp.sum(
            jnp.where(who % places == z, kept, 0.0), axis=0, keepdims=True
        )
    each = ff // count
    at = lax.broadcasted_iota(jnp.int32, (1, ff), 1)
    kept = select_rows(
        values, pick_of(at % each), (what == 6) & (who // places == at // each)
    )
    for z in range(places):
        bu_ref[z : z + 1, :] = jnp.sum(
            jnp.where(who % places == z, kept, 0.0), axis=0, keepdims=True
        )

    block = rows // 4

    def norm(i):
        here = slice(i * block, (i + 1) * block)
        values = x_ref[here, :]
        center = values - jnp.mean(values, axis=1, keepdims=True)
        inverse = lax.rsqrt(jnp.mean(center * center, axis=1, keepdims=True) + EPSILON)
        normal = center * inverse
        n1_ref[here, :] = (normal * small_ref[0:1, :] + small_ref[1:2, :]).astype(BF)
        second_norm = normal * small_ref[2:3, :] + small_ref[3:4, :]
        n2_ref[here, :] = second_norm.astype(BF)
        n2t_ref[:, here] = second_norm.astype(BF).astype(F32).T.astype(BF)
        cot = cot_ref[here, :]
        cb_ref[here, :] = cot.astype(BF)
        cbt_ref[:, here] = cot.T.astype(BF)

    cuts = [2 + (head_done - 2) * i // 5 for i in range(6)]
    for i in range(5):
        run(cuts[i], cuts[i + 1])
        if i < 4:
            norm(i)
    own[0].wait()
    save = pltpu.make_async_copy(g_ref.at[0], p_ref, ls.at[4])
    save.start()

    heads = ff // GROUP
    before_feed = max(feed_done[0], head_done)
    cuts = [head_done + (before_feed - head_done) * i // places for i in range(places + 1)]

    def project(i, carry):
        for n in range(places):

            @pl.when(i == n)
            def _(n=n):
                run(cuts[n], cuts[n + 1])

        to = source_at((i + 1) % places)
        w = g_ref[0, to].reshape(model, ff)
        forward = dot(n1_ref[...], w, 1, 0) + bq_ref[pl.ds(to, 1), :]
        column = lax.broadcasted_iota(jnp.int32, (rows, LANES), 1)
        for h in range(heads):
            tile = forward[:, h * GROUP : h * GROUP + LANES]
            tile = turn_tiles([tile], table_ref[0], table_ref[1], table_ref[2])[0]
            x_buf[to, h, :, :LANES] = tile.astype(BF)
            late = slice(h * GROUP + LANES, (h + 1) * GROUP)
            backward = dot(cb_ref[...], w[:, late], 1, 0)
            tile = jnp.where(column < HD, forward[:, late], backward)
            x_buf[to, h, :, LANES:] = tile.astype(BF)

        @pl.when(i < places - 1)
        def _():
            for h in range(heads):
                x_copy(h, to, True).start()

        @pl.when(i == places - 1)
        def _():
            for h in range(heads):
                keep_own(h).start()

        return carry

    lax.fori_loop(0, places, project, 0)

    out_ref[...] = jnp.zeros_like(out_ref)
    back_ref[...] = jnp.zeros_like(back_ref)
    own[1].wait()
    own[2].wait()
    width = ff // 2

    def puts(i):
        place = source_at(i)
        return [
            pltpu.make_async_copy(
                buf.at[i], ref.at[place], ls.at[5 + heads + 2 * i + a]
            )
            for a, (buf, ref) in enumerate(((gu_buf, gu_ref), (gd_buf, gd_ref)))
        ]

    def feed(f, carry):
        low = before_feed
        for t in turns:
            high = max(low, feed_done[t])

            @pl.when(f == 2 * t)
            def _(low=low, high=high):
                run(low, high)

            low = high
        i, h = f // 2, f % 2
        place = source_at(i)
        cols = pl.ds(pl.multiple_of(h * width, width), width)
        up = g_ref[1, place, :, :, cols].reshape(model, width)
        down = g_ref[2, place, :, :, cols].reshape(model, width)
        pre = dot(n2_ref[...], up, 1, 0) + bu_ref[pl.ds(place, 1), cols]
        bell = 0.5 * (1.0 + lax.erf(pre * 0.7071067811865476))
        activ = (pre * bell).astype(BF)
        out_ref[...] += dot(activ, down, 1, 1)
        gd_buf[i, :, cols] = dot(cbt_ref[...], activ, 1, 0).astype(BF)
        slope = bell + pre * jnp.exp(-0.5 * pre * pre) * 0.3989422804014327
        grad = dot(cb_ref[...], down, 1, 0) * slope
        gb_ref[pl.ds(place, 1), cols] = jnp.sum(grad, axis=0, keepdims=True)
        grad = grad.astype(BF)
        gu_buf[i, :, cols] = dot(n2t_ref[...], grad, 1, 0).astype(BF)
        back_ref[...] += dot(grad, up, 1, 1)

        @pl.when(h == 1)
        def _():
            for copy in puts(i):
                copy.start()

        return carry

    lax.fori_loop(0, 2 * places, feed, 0)

    saves = [
        pltpu.make_async_copy(buf, ref, ls.at[5 + heads + 2 * places + i])
        for i, (buf, ref) in enumerate(((out_ref, two_ref), (back_ref, grad_ref)))
    ]
    for copy in saves:
        copy.start()
    for copy in [save] + saves:
        copy.wait()
    for i in range(places):
        for copy in puts(i):
            copy.wait()
    for h in range(heads):
        keep_own(h).wait()
        for p in range(places):

            @pl.when(p != mz)
            def _(h=h, p=p):
                x_copy(h, p, False).wait_recv()
                x_copy(h, p, True).wait_send()


    def wait_sent(i, carry):
        vec_copy(i, True).wait_send()
        return carry

    lax.fori_loop(1, total, wait_sent, 0)
    for a in range(3):
        for p in range(places):

            @pl.when((p <= mz) & (mz < places - 1))
            def _(a=a, p=p):
                z_copy(a, p, True).wait_send()

            @pl.when((p >= mz) & (mz > 0))
            def _(a=a, p=p):
                z_copy(a, p, False).wait_send()

    for j in range(len(chunks)):
        for k in range(nbits):
            for copy in d_copies(j, k, True):
                copy.wait_send()


def front(block_input, cotangent, weights, vector, turns, count, places, wide, piece):
    rows, model = block_input.shape
    depth, ff = weights.shape[1:]
    total = count * places
    heads = ff // GROUP
    sem = pltpu.SemaphoreType.DMA
    shape = jax.ShapeDtypeStruct
    return pl.pallas_call(
        functools.partial(front_kernel, count, places, wide, piece),
        out_shape=(
            shape((heads, places, rows, GROUP), BF),
            shape((places, count, depth, ff), BF),
            shape((8, model), F32),
            shape((rows, model), F32),
            shape((rows, model), F32),
            shape((places, model, ff), BF),
            shape((places, model, ff), BF),
            shape((places, ff), F32),
        ),
        in_specs=[VMEM] * 5,
        out_specs=(ANY, ANY, VMEM, ANY, ANY, ANY, ANY, VMEM),
        scratch_shapes=[
            pltpu.VMEM((rows, model), F32),
            pltpu.VMEM((rows, model), F32),
            pltpu.VMEM((3, places, count, depth, ff), BF),
            pltpu.VMEM((places, heads, rows, GROUP), BF),
            pltpu.VMEM((rows, model), BF),
            pltpu.VMEM((rows, model), BF),
            pltpu.VMEM((rows, model), BF),
            pltpu.VMEM((model, rows), BF),
            pltpu.VMEM((model, rows), BF),
            pltpu.VMEM((3, rows, LANES), F32),
            pltpu.VMEM((total, 8, LANES), F32),
            pltpu.VMEM((places, ff), F32),
            pltpu.VMEM((places, ff), F32),
            pltpu.VMEM((places, model, ff), BF),
            pltpu.VMEM((places, model, ff), BF),
            sem((6 * places,)),
            sem((3 * places,)),
            sem((3 * places * (count - 1),)),
            sem((3 * places * (count - 1),)),
            sem((total,)),
            sem((total,)),
            sem((heads * places,)),
            sem((heads * places,)),
            sem((7 + heads + 2 * places,)),
        ],
        compiler_params=pltpu.CompilerParams(
            has_side_effects=True, vmem_limit_bytes=VMEM_LIMIT
        ),
        name="front",
    )(block_input, cotangent, weights, vector, turns)


class Scatter:
    def __init__(self, count, places, chunks, sources, acc, landing, sems, local):
        self.me, self.mz = lax.axis_index("dp"), lax.axis_index("tensor")
        self.count, self.places, self.chunks, self.sources = count, places, chunks, sources
        self.acc, self.landing, self.sems, self.local = acc, landing, sems, local
        self.nbits = count.bit_length() - 1

    @staticmethod
    def orders(count):
        nbits = count.bit_length() - 1
        first = list(range(nbits))
        return first, ([first[0], first[2], first[1]] + first[3:] if nbits >= 3 else first)

    def copies(self, j, k):
        a, s, order = self.chunks[j]
        to = (flip(self.me, 1 << order[k]), self.mz)
        half = self.count >> (k + 1)
        base = j * (half_of(self.count) + self.nbits - 1)
        send, recv = self.sems
        if k > 0:
            n = base + half_of(self.count) + k - 1
            src = self.acc.at[j, half : 2 * half]
            return [remote(src, self.landing[k].at[j], send.at[n], recv.at[n], to)]
        place = (self.mz + s) % self.places
        out = []
        for i, m in enumerate(span(order[1:][::-1])):
            slot = flip(self.me, m | (1 << order[0]))
            out.append(
                remote(
                    self.sources[a].at[place, slot],
                    self.landing[0].at[j, i],
                    send.at[base + i],
                    recv.at[base + i],
                    to,
                )
            )
        return out

    def loads(self, j):
        a, s, order = self.chunks[j]
        place = (self.mz + s) % self.places
        return [
            pltpu.make_async_copy(
                self.sources[a].at[place, flip(self.me, m)],
                self.acc.at[j, i],
                self.local.at[j * half_of(self.count) + i],
            )
            for i, m in enumerate(span(order[1:][::-1]))
        ]

    def start(self, j):
        for copy in self.copies(j, 0) + self.loads(j):
            copy.start()

    def stage(self, j, k, final=None):
        if k == 0:
            for copy in self.loads(j):
                copy.wait()
        for copy in self.copies(j, k):
            copy.wait_recv()
        half = self.count >> (k + 1)
        rows = self.acc.shape[2]
        step = 32 if rows % 32 == 0 else rows
        parts = rows // step
        target = self.acc.at[j] if final is None else final

        def body(i, carry):
            shard, at = i // parts, pl.ds(pl.multiple_of(i % parts * step, step), step)
            mine = self.acc[j, shard, at, :].astype(F32)
            other = self.landing[k][j, shard, at, :].astype(F32)
            target[shard, at, :] = (mine + other).astype(BF)
            return carry

        lax.fori_loop(0, half * parts, body, 0)
        if k + 1 < self.nbits:
            for copy in self.copies(j, k + 1):
                copy.start()

    def drain(self):
        for j in range(len(self.chunks)):
            for k in range(self.nbits):
                for copy in self.copies(j, k):
                    copy.wait_send()

    @staticmethod
    def scratch(count, chunks, rows, width):
        nbits = count.bit_length() - 1
        sem = pltpu.SemaphoreType.DMA
        copies = chunks * (half_of(count) + nbits - 1)
        return (
            [pltpu.VMEM((chunks, half_of(count), rows, width), BF)]
            + [pltpu.VMEM((chunks, count >> (k + 1), rows, width), BF) for k in range(nbits)]
            + [sem((copies,)), sem((copies,)), sem((chunks * half_of(count),))]
        )


def half_of(count):
    return count // 2


def middle_kernel(count, places, heads, wq, wk, *refs):
    y_ref, begin_ref, cs_ref, gu_ref, gd_ref, z_ref, bias_ref, red_ref = refs[:8]
    r_buf, qh, kh, vh, oh, kt, vt, s_scr, dq, dk, dv, at_scr, table_ref = refs[8:21]
    ss, rs, ls, acc = refs[21:25]
    nbits = count.bit_length() - 1
    landing = refs[25 : 25 + nbits]
    send, recv, local = refs[25 + nbits :]
    me, mz = lax.axis_index("dp"), lax.axis_index("tensor")
    total = y_ref.shape[1]
    rows = total // places
    scale = HD**-0.5
    nq = total // wq

    chunks = []
    for s in list(range(1, places)) + [0]:
        for a in range(2):
            chunks.append((a, s, Scatter.orders(count)[a]))
    scatter = Scatter(
        count, places, chunks, (gu_ref, gd_ref), acc, landing, (send, recv), local
    )
    events = {}
    last_step = heads * nq
    for k in range(nbits):
        for pair in range(len(chunks) // 2):
            when = (2 + pair // 2, 5 + pair)[k] if k < 2 else 9 + pair + 4 * (k - 2)
            events.setdefault(min(when * nq // 4, last_step), []).append((pair, k))

    def run_events(step):
        for pair, k in events.get(step, []):
            for j in (2 * pair, 2 * pair + 1):
                a, s, _ = chunks[j]
                final = red_ref.at[a, pl.ds(s, 1)] if k == nbits - 1 else None
                scatter.stage(j, k, final)

    for j in range(len(chunks)):
        scatter.start(j)

    def tables(i, carry):
        at = pl.ds(pl.multiple_of(i * wk, wk), wk)
        cosine, low, high = spread_turns(cs_ref[:, at])
        table_ref[0, at, :] = cosine
        table_ref[1, at, :] = -low
        table_ref[2, at, :] = -high
        return carry

    lax.fori_loop(0, total // wk, tables, 0)

    def back_copy(h, s, sending):
        to = (mz + s) % places
        slot = mz if sending else (mz + places - s) % places
        n = h * places + s
        return remote(r_buf.at[h, to], z_ref.at[slot, h], ss.at[n], rs.at[n], (me, to))

    def keep_own(h):
        return pltpu.make_async_copy(r_buf.at[h, mz], z_ref.at[mz, h], ls.at[h])

    def flat(t, carry):
        h, i = t // nq, t % nq
        for step in sorted(events):
            if step < last_step:

                @pl.when(t == step)
                def _(step=step):
                    run_events(step)

        @pl.when(i == 0)
        def _():
            def prepare(b, carry):
                at = pl.ds(pl.multiple_of(b * wk, wk), wk)
                both = y_ref[h, at, :LANES].astype(F32)
                q, k = both[:, :HD] * scale, both[:, HD:]
                both = y_ref[h, at, LANES:].astype(F32)
                v, o = both[:, :HD], both[:, HD:]
                qh[at, :] = q.astype(BF)
                kh[at, :] = k.astype(BF)
                vh[at, :] = v.astype(BF)
                oh[at, :] = o.astype(BF)
                kt[:, at] = k.T.astype(BF)
                vt[:, at] = v.T.astype(BF)
                dk[at, :] = jnp.zeros((wk, HD), F32)
                dv[at, :] = jnp.zeros((wk, HD), F32)
                return carry

            lax.fori_loop(0, total // wk, prepare, 0)

        at = pl.ds(pl.multiple_of(i * wq, wq), wq)
        begin = begin_ref[0:1, at]
        last = i * wq + lax.broadcasted_iota(jnp.int32, (1, wq), 1)
        query, grad = qh[at, :], oh[at, :]
        trips = ((i + 1) * wq + wk - 1) // wk

        def scores(j, peak):
            keys = pl.ds(pl.multiple_of(j * wk, wk), wk)
            place = j * wk + lax.broadcasted_iota(jnp.int32, (wk, wq), 0)
            s = dot(kh[keys, :], query, 1, 1)
            s = jnp.where((place >= begin) & (place <= last), s, NEGATIVE)
            s_scr[keys, :] = s
            return jnp.maximum(peak, jnp.max(s.reshape(wk // 8, 8, wq), axis=0))

        peak = lax.fori_loop(0, trips, scores, jnp.full((8, wq), NEGATIVE, F32))
        peak = jnp.max(peak, axis=0, keepdims=True)

        def weigh(j, state):
            mass, out = state
            keys = pl.ds(pl.multiple_of(j * wk, wk), wk)
            p = jnp.exp(s_scr[keys, :] - peak)
            s_scr[keys, :] = p
            mass = mass + jnp.sum(p.reshape(wk // 8, 8, wq), axis=0)
            return mass, out + dot(vt[:, keys], p.astype(BF), 1, 0)

        mass, out = lax.fori_loop(
            0, trips, weigh, (jnp.zeros((8, wq), F32), jnp.zeros((HD, wq), F32))
        )
        inverse = 1.0 / jnp.sum(mass, axis=0, keepdims=True)
        attended = (out * inverse).astype(BF).astype(F32)
        delta = jnp.sum(attended * grad.astype(F32).T, axis=0, keepdims=True)
        at_scr[at, :] = attended.T

        def back(j, out):
            keys = pl.ds(pl.multiple_of(j * wk, wk), wk)
            p = s_scr[keys, :] * inverse
            dv[keys, :] += dot(p.astype(BF), grad, 1, 0)
            g = dot(vh[keys, :], grad, 1, 1)
            ds = (p * (g - delta)).astype(BF)
            dk[keys, :] += dot(ds, query, 1, 0)
            return out + dot(kt[:, keys], ds, 1, 0)

        out = lax.fori_loop(0, trips, back, jnp.zeros((HD, wq), F32))
        dq[at, :] = (out * scale).T

        @pl.when(i == nq - 1)
        def _():
            per = rows // wk

            def finish(b, sums):
                at = pl.ds(pl.multiple_of(b * wk, wk), wk)
                inside = pl.ds(pl.multiple_of(b % per * wk, wk), wk)
                tile = jnp.concatenate([dq[at, :], dk[at, :]], axis=1)
                tile = turn_tiles(
                    [tile], table_ref[0, at, :], table_ref[1, at, :], table_ref[2, at, :]
                )[0]
                r_buf[h, b // per, inside, :LANES] = tile.astype(BF)
                other = jnp.concatenate([dv[at, :], at_scr[at, :]], axis=1)
                r_buf[h, b // per, inside, LANES:] = other.astype(BF)
                return tuple(
                    total + jnp.sum(x.reshape(wk // 8, 8, LANES), axis=0)
                    for total, x in zip(sums, (tile, other))
                )

            zero = jnp.zeros((8, LANES), F32)
            sums = lax.fori_loop(0, total // wk, finish, (zero, zero))
            for c, value in enumerate(sums):
                bias_ref[h, :, c * LANES : (c + 1) * LANES] = value
            for s in range(1, places):
                back_copy(h, s, True).start()
            keep_own(h).start()

        return carry

    lax.fori_loop(0, last_step, flat, 0)
    run_events(last_step)
    for h in range(heads):
        keep_own(h).wait()
        for s in range(1, places):
            back_copy(h, s, False).wait_recv()
        for s in range(1, places):
            back_copy(h, s, True).wait_send()
    scatter.drain()


def middle(y, begin, turns, up_grad, down_grad):
    heads, total, group = y.shape
    places, count, depth, ff = up_grad.shape
    wq, wk = min(512, total), min(512, total)
    vmem = pltpu.VMEM
    sem = pltpu.SemaphoreType.DMA
    shape = jax.ShapeDtypeStruct
    return pl.pallas_call(
        functools.partial(middle_kernel, count, places, heads, wq, wk),
        out_shape=(
            shape((places, heads, total // places, group), BF),
            shape((heads, 8, group), F32),
            shape((2, places, depth, ff), BF),
        ),
        in_specs=[VMEM, VMEM, VMEM, ANY, ANY],
        out_specs=(ANY, VMEM, VMEM),
        scratch_shapes=[vmem((heads, places, total // places, group), BF)]
        + [vmem((total, HD), BF)] * 4
        + [vmem((HD, total), BF)] * 2
        + [vmem((total, wq), F32)]
        + [vmem((total, HD), F32)] * 4
        + [vmem((3, total, LANES), F32)]
        + [sem((heads * places,)), sem((heads * places,)), sem((heads,))]
        + Scatter.scratch(count, 2 * places, depth, ff),
        compiler_params=pltpu.CompilerParams(
            has_side_effects=True, vmem_limit_bytes=VMEM_LIMIT
        ),
        name="middle",
    )(y, begin, turns, up_grad, down_grad)


def place_rows(values, pick, keep):
    return lax.dot_general(
        jnp.where(keep, values, 0.0),
        pick,
        (((1,), (0,)), ((), ())),
        precision=lax.Precision.HIGHEST,
        preferred_element_type=F32,
    )


def tail_kernel(count, places, wide, piece, *refs):
    x_hbm, cot_hbm, z_hbm, w_hbm, two_hbm, grad_hbm, small_ref, red_ref, qb_ref, gb_ref = refs[:10]
    y_ref, dx_ref, gq_ref, gp_ref, gu_ref, gd_ref, vout_ref = refs[10:17]
    x_ref, cot_ref, z_ref, w_ref, two_ref, grad_ref = refs[17:23]
    normal_ref, inverse_ref, n1t_ref, cbt_ref, out_ref, back_ref, g_ref = refs[23:30]
    sums_ref, vec_ref, zb, vb, zs, zr, vs, vr, ls, acc = refs[30:40]
    nbits = count.bit_length() - 1
    landing = refs[40 : 40 + nbits]
    send, recv, local = refs[40 + nbits :]
    me, mz = lax.axis_index("dp"), lax.axis_index("tensor")
    total = count * places
    rows, model = x_ref.shape
    heads = z_ref.shape[1]
    depth, ff = acc.shape[2:]

    chunks = [
        (0, s, Scatter.orders(count)[i % 2])
        for i, s in enumerate(list(range(1, places)) + [0])
    ]
    scatter = Scatter(count, places, chunks, (g_ref,), acc, landing, (send, recv), local)

    def z_copy(a, s):
        n = a * (places - 1) + s - 1
        src = acc.at[s - 1, 0] if a == 0 else red_ref.at[a - 1, s]
        return remote(src, zb.at[a, s - 1], zs.at[n], zr.at[n], (me, (mz + s) % places))

    def vec_copy(i, sending):
        to = ((me + i // places) % count, (mz + i % places) % places)
        return remote(
            vec_ref.at[to[0] * places + to[1]], vb.at[i], vs.at[i], vr.at[i], to
        )

    def fetch(i):
        at = (mz + 1 + i) % places
        return [
            pltpu.make_async_copy(z_hbm.at[at], z_ref.at[at], ls.at[4 + 2 * i]),
            pltpu.make_async_copy(w_hbm.at[at], w_ref.at[at], ls.at[5 + 2 * i]),
        ]

    inputs = [
        pltpu.make_async_copy(src, dst, ls.at[i])
        for i, (src, dst) in enumerate(
            ((x_hbm, x_ref), (cot_hbm, cot_ref), (two_hbm, two_ref), (grad_hbm, grad_ref))
        )
    ]
    for copy in inputs[:2]:
        copy.start()
    for i in range(places):
        for copy in fetch(i):
            copy.start()
    for copy in inputs[2:]:
        copy.start()
    for s in range(1, places):
        for a in (1, 2):
            z_copy(a, s).start()

    blocks = 4
    block = rows // blocks
    for copy in inputs[:2]:
        copy.wait()
    for i in range(blocks):
        here = slice(i * block, (i + 1) * block)
        values = x_ref[here, :]
        center = values - jnp.mean(values, axis=1, keepdims=True)
        inverse = lax.rsqrt(jnp.mean(center * center, axis=1, keepdims=True) + EPSILON)
        normal = center * inverse
        normal_ref[here, :] = normal
        inverse_ref[here, :] = jnp.broadcast_to(inverse, (block, LANES))
        mixed = normal * small_ref[0:1, :] + small_ref[1:2, :]
        n1t_ref[:, here] = mixed.T.astype(BF)
        cbt_ref[:, here] = cot_ref[here, :].T.astype(BF)
    out_ref[...] = jnp.zeros_like(out_ref)
    back_ref[...] = jnp.zeros_like(back_ref)

    def steps(slot):
        for k in range(nbits - 1, -1, -1):
            pair = slot - k
            for j in (2 * pair, 2 * pair + 1):
                if 0 <= pair and j < len(chunks):
                    scatter.stage(j, k)
                    if k == nbits - 1 and chunks[j][1] > 0:
                        z_copy(0, chunks[j][1]).start()

    left = lax.broadcasted_iota(jnp.int32, (rows, LANES), 1) < HD
    wide_left = lax.broadcasted_iota(jnp.int32, (model, LANES), 1) < HD

    def source(i, carry):
        at = (mz + 1 + i) % places
        for n in range(places):

            @pl.when(i == n)
            def _():
                for copy in fetch(n):
                    copy.wait()

        def head(h, carry):
            z = z_ref[at, h]
            start = pl.multiple_of(h * GROUP, GROUP)
            w = w_ref[at, :, :, pl.ds(start, GROUP)].reshape(model, GROUP)
            late = z[:, LANES:]
            none = jnp.zeros_like(late)
            ours = jnp.concatenate([z[:, :LANES], jnp.where(left, late, none)], axis=1)
            back_ref[...] += dot(ours, w, 1, 1)
            out_ref[...] += dot(jnp.where(left, none, late), w[:, LANES:], 1, 1)
            first = dot(n1t_ref[...], z, 1, 0)
            second = dot(cbt_ref[...], late, 1, 0)
            g_ref[at, :, :, pl.ds(start, LANES)] = (
                first[:, :LANES].astype(BF).reshape(count, depth, LANES)
            )
            second = jnp.where(wide_left, first[:, LANES:], second)
            g_ref[at, :, :, pl.ds(start + LANES, LANES)] = second.astype(BF).reshape(
                count, depth, LANES
            )
            return carry

        lax.fori_loop(0, heads, head, 0)
        for n in range(places):

            @pl.when(i == n)
            def _():
                scatter.start(n)
                if n % 2 == 0 and n > 0:
                    steps(n // 2 - 1)

        return carry

    lax.fori_loop(0, places, source, 0)
    slot = max((places - 1) // 2, 0)
    last = (len(chunks) + 1) // 2 + nbits - 1

    for copy in inputs[2:]:
        copy.wait()
    sums = [jnp.zeros((8, model), F32) for _ in range(5)]

    def norm_rows_back(grad, gain, normal, inverse):
        scaled = grad * gain
        first = jnp.mean(scaled, axis=1, keepdims=True)
        second = jnp.mean(scaled * normal, axis=1, keepdims=True)
        return inverse * (scaled - first - normal * second)

    def fold(values):
        return jnp.sum(values.reshape(block // 8, 8, model), axis=0)

    for i in range(blocks):
        here = slice(i * block, (i + 1) * block)
        normal, inverse = normal_ref[here, :], inverse_ref[here, 0:1]
        cot, one, two = cot_ref[here, :], back_ref[here, :], grad_ref[here, :]
        y_ref[here, :] = (
            x_ref[here, :] + (out_ref[here, :] + two_ref[here, :]) + small_ref[4:5, :]
        )
        dx_ref[here, :] = (
            cot
            + norm_rows_back(one, small_ref[0:1, :], normal, inverse)
            + norm_rows_back(two, small_ref[2:3, :], normal, inverse)
        )
        for r, values in enumerate((one * normal, one, two * normal, two, cot)):
            sums[r] = sums[r] + fold(values)
        if slot < last:
            steps(slot)
            slot += 1
    sums_ref[...] = jnp.zeros_like(sums_ref)
    for r in range(5):
        sums_ref[r : r + 1, :] = jnp.sum(sums[r], axis=0, keepdims=True)

    lane = lax.broadcasted_iota(jnp.int32, (1, ff), 1)
    line = lax.broadcasted_iota(jnp.int32, (ff, 1), 0)
    out_lane = lax.broadcasted_iota(jnp.int32, (1, LANES), 1)
    sub = lax.broadcasted_iota(jnp.int32, (total * 8, 1), 0)
    who, what = sub // 8, sub % 8
    spread = jnp.broadcast_to(sums_ref[...][None], (total, 8, model)).reshape(total * 8, model)
    parts = place_rows(
        spread,
        jnp.where(line % piece == out_lane, 1.0, 0.0),
        (what < 5) & (who == lane // piece),
    )
    each = wide // count
    kind, inner = lane % GROUP // HD, lane // GROUP * HD + lane % HD
    kind_line, inner_line = line % GROUP // HD, line // GROUP * HD + line % HD
    qkv = jnp.concatenate(
        [jnp.sum(qb_ref[h], axis=0, keepdims=True) for h in range(heads)], axis=1
    )
    parts += place_rows(
        jnp.broadcast_to(qkv, (total * 8, ff)),
        jnp.where(kind_line * each + inner_line % each == out_lane, 1.0, 0.0),
        (what == 5) & (kind < 3) & (who == inner // each * places + mz),
    )
    each = ff // count
    up = jnp.zeros((total * 8, ff), F32)
    for z in range(places):
        up = jnp.where(who % places == z, gb_ref[z : z + 1, :], up)
    parts += place_rows(
        up,
        jnp.where(line % each == out_lane, 1.0, 0.0),
        (what == 6) & (who // places == lane // each),
    )
    vec_ref[...] = parts.reshape(total, 8, LANES)

    def send_vec(i, carry):
        vec_copy(i, True).start()
        return carry

    lax.fori_loop(1, total, send_vec, 0)
    own_vec = pltpu.make_async_copy(vec_ref.at[me * places + mz], vb.at[0], ls.at[4 + 2 * places])
    own_vec.start()
    while slot < last:
        steps(slot)
        slot += 1

    own_vec.wait()

    def wait_vec(i, carry):
        vec_copy(i, False).wait_recv()
        vec_copy(i, True).wait_send()
        return carry

    lax.fori_loop(1, total, wait_vec, 0)
    vout_ref[...] = jnp.sum(vb[...], axis=0)
    for a in (1, 2, 0):
        for s in range(1, places):
            z_copy(a, s).wait_recv()
        own = acc[places - 1, 0] if a == 0 else red_ref[a - 1, 0]
        result = own.astype(F32)
        for s in range(1, places):
            result = result + zb[a, s - 1].astype(F32)
        if a == 1:
            gu_ref[...] = result
        elif a == 2:
            gd_ref[...] = result.T
        else:
            for h in range(heads):
                for c, ref in enumerate((gq_ref.at[0], gq_ref.at[1], gq_ref.at[2])):
                    ref[:, h * HD : (h + 1) * HD] = result[
                        :, h * GROUP + c * HD : h * GROUP + (c + 1) * HD
                    ]
                gp_ref[h * HD : (h + 1) * HD, :] = result[
                    :, h * GROUP + 3 * HD : (h + 1) * GROUP
                ].T
    scatter.drain()
    for a in range(3):
        for s in range(1, places):
            z_copy(a, s).wait_send()


def tail(x, cot, z, w, two, grad, small, partly, qkv_sums, up_sums, wide, piece):
    places, heads, rows, group = z.shape
    count, depth, ff = w.shape[1:]
    model = x.shape[1]
    total = count * places
    sem = pltpu.SemaphoreType.DMA
    shape = jax.ShapeDtypeStruct
    vmem = pltpu.VMEM
    return pl.pallas_call(
        functools.partial(tail_kernel, count, places, wide, piece),
        out_shape=(
            shape((rows, model), F32),
            shape((rows, model), F32),
            shape((3, depth, wide), F32),
            shape((wide, depth), F32),
            shape((depth, ff), F32),
            shape((ff, depth), F32),
            shape((8, LANES), F32),
        ),
        in_specs=[ANY] * 6 + [VMEM] * 4,
        out_specs=(VMEM,) * 7,
        scratch_shapes=[
            vmem((rows, model), F32),
            vmem((rows, model), F32),
            vmem((places, heads, rows, group), BF),
            vmem((places, count, depth, ff), BF),
            vmem((rows, model), F32),
            vmem((rows, model), F32),
            vmem((rows, model), F32),
            vmem((rows, LANES), F32),
            vmem((model, rows), BF),
            vmem((model, rows), BF),
            vmem((rows, model), F32),
            vmem((rows, model), F32),
            vmem((places, count, depth, ff), BF),
            vmem((8, model), F32),
            vmem((total, 8, LANES), F32),
            vmem((3, places - 1, depth, ff), BF),
            vmem((total, 8, LANES), F32),
            sem((3 * (places - 1),)),
            sem((3 * (places - 1),)),
            sem((total,)),
            sem((total,)),
            sem((5 + 2 * places,)),
        ]
        + Scatter.scratch(count, places, depth, ff),
        compiler_params=pltpu.CompilerParams(
            has_side_effects=True, vmem_limit_bytes=VMEM_LIMIT
        ),
        name="tail",
    )(x, cot, z, w, two, grad, small, partly, qkv_sums, up_sums)


def lanes(values, width=LANES):
    return jnp.pad(values, [(0, 0)] * (values.ndim - 1) + [(0, width - values.shape[-1])])


def shards(
    count,
    places,
    block_input,
    cotangent,
    segment_ids,
    token_offset,
    first_gain,
    first_shift,
    second_gain,
    second_shift,
    qkv_weight,
    qkv_bias,
    proj_weight,
    up_weight,
    up_bias,
    down_weight,
    out_bias,
):
    rows, model = block_input.shape
    depth = qkv_weight.shape[1]
    wide = qkv_weight.shape[2]
    heads = wide // HD
    ff = up_weight.shape[1]
    piece = first_gain.shape[0]
    total = segment_ids.shape[0]

    attn = jnp.stack([qkv_weight[0], qkv_weight[1], qkv_weight[2], proj_weight.T])
    attn = attn.reshape(4, depth, heads, HD).transpose(1, 2, 0, 3).reshape(depth, 4 * wide)
    packed = jnp.stack([attn, up_weight, down_weight.T])
    vector = jnp.stack(
        [lanes(v) for v in (first_gain, first_shift, second_gain, second_shift, out_bias)]
        + [lanes(qkv_bias.astype(F32).reshape(-1)), lanes(up_bias.astype(F32))]
        + [jnp.zeros((LANES,), F32)]
    )
    turns = rotary_turns(token_offset)
    begin = (jnp.arange(total, dtype=jnp.int32) - token_offset)[None, :]
    y, attn_weights, small, out_two, grad_two, up_grad, down_grad, up_bias_part = front(
        block_input, cotangent, packed, vector, turns, count, places, wide, piece
    )
    z, qkv_bias_part, partly = middle(
        y.reshape(heads, total, GROUP),
        begin,
        turns,
        up_grad.reshape(places, count, depth, ff),
        down_grad.reshape(places, count, depth, ff),
    )
    block_output, input_grad, gq, gp, gu, gd, vec = tail(
        block_input,
        cotangent,
        z,
        attn_weights,
        out_two,
        grad_two,
        small,
        partly,
        qkv_bias_part,
        up_bias_part,
        wide,
        piece,
    )
    return (
        block_output,
        input_grad,
        vec[0, :piece],
        vec[1, :piece],
        vec[2, :piece],
        vec[3, :piece],
        gq,
        vec[5, : 3 * wide // count].reshape(3, wide // count),
        gp,
        gu,
        vec[6, : ff // count],
        gd,
        vec[4, :piece],
    )


def solution(mesh):
    both = P(("dp", "tensor"))
    return jax.shard_map(
        functools.partial(shards, mesh.shape["dp"], mesh.shape["tensor"]),
        mesh=mesh,
        in_specs=(
            P(("dp", "tensor"), None),
            P(("dp", "tensor"), None),
            P("dp"),
            P("dp"),
            both,
            both,
            both,
            both,
            P(None, "dp", "tensor"),
            P(None, ("tensor", "dp")),
            P("tensor", "dp"),
            P("dp", "tensor"),
            P(("tensor", "dp")),
            P("tensor", "dp"),
            both,
        ),
        out_specs=(
            P(("dp", "tensor"), None),
            P(("dp", "tensor"), None),
            both,
            both,
            both,
            both,
            P(None, "dp", "tensor"),
            P(None, ("tensor", "dp")),
            P("tensor", "dp"),
            P("dp", "tensor"),
            P(("tensor", "dp")),
            P("tensor", "dp"),
            both,
        ),
        check_vma=False,
    )
```

```python
import functools

import jax
import jax.numpy as jnp
from jax import lax
from jax.experimental import pallas as pl
from jax.experimental.pallas import tpu as pltpu
from jax.sharding import PartitionSpec as P

HD = 64
ROT = 16
EPSILON = 1e-05
NEGATIVE = -1e30
LANES = 128
GROUP = 4 * HD
BF = jnp.bfloat16
F32 = jnp.float32
ANY = pl.BlockSpec(memory_space=pl.ANY)
VMEM = pl.BlockSpec(memory_space=pltpu.VMEM)
VMEM_LIMIT = 60 * 1024 * 1024


def dot(a, b, ca, cb):
    return lax.dot_general(a, b, (((ca,), (cb,)), ((), ())), preferred_element_type=F32)


def flip(index, mask):
    out = index
    bit = 0
    while (1 << bit) <= mask:
        if (mask >> bit) & 1:
            step = 1 << bit
            out = out + (1 - 2 * ((index // step) % 2)) * step
        bit += 1
    return out


def span(bits):
    masks = [0]
    for bit in bits:
        masks = masks + [m | (1 << bit) for m in masks]
    return masks


def same(index, value, count):
    return 1 - ((index + count - value) % count + count - 1) // count


def nearest(place, turn, count):
    out = 0
    for p in range(count):
        order = sorted(range(count), key=lambda q: (abs(q - p), q < count - 1 - p))
        out = out + same(place, p, count) * order[turn]
    return out


def remote(src, dst, send_sem, recv_sem, device):
    return pltpu.make_async_remote_copy(
        src_ref=src,
        dst_ref=dst,
        send_sem=send_sem,
        recv_sem=recv_sem,
        device_id=device,
        device_id_type=pl.DeviceIdType.MESH,
    )


def turn_tiles(tiles, cosine, low, high):
    out = []
    for tile in tiles:
        ahead = pltpu.roll(tile, LANES - ROT // 2, 1)
        behind = pltpu.roll(tile, ROT // 2, 1)
        out.append(tile * cosine + ahead * low + behind * high)
    return out


def rotary_turns(offsets):
    half = ROT // 2
    freq = 10000.0 ** (-(2.0 * jnp.arange(half, dtype=F32)) / ROT)
    angles = offsets.astype(F32)[None, :] * freq[:, None]
    return jnp.concatenate([jnp.cos(angles), jnp.sin(angles)], axis=0)


def spread_turns(turns):
    half = ROT // 2
    lane = lax.broadcasted_iota(jnp.int32, (ROT, LANES), 1) % HD
    line = lax.broadcasted_iota(jnp.int32, (ROT, LANES), 0)
    picks = (
        jnp.where((lane < ROT) & (line == lane % half), 1.0, 0.0),
        jnp.where((lane < half) & (line == half + lane), -1.0, 0.0),
        jnp.where((lane >= half) & (lane < ROT) & (line == lane), 1.0, 0.0),
    )
    tables = [
        lax.dot_general(
            turns,
            pick,
            (((0,), (0,)), ((), ())),
            precision=lax.Precision.HIGHEST,
            preferred_element_type=F32,
        )
        for pick in picks
    ]
    column = lax.broadcasted_iota(jnp.int32, tables[0].shape, 1) % HD
    tables[0] = jnp.where(column < ROT, tables[0], 1.0)
    return tables


def select_rows(values, pick, keep):
    spread = lax.dot_general(
        values,
        pick,
        (((1,), (0,)), ((), ())),
        precision=lax.Precision.HIGHEST,
        preferred_element_type=F32,
    )
    return jnp.where(keep, spread, 0.0)


def front_kernel(
    count,
    places,
    wide,
    piece,
    x_ref,
    cot_ref,
    w_ref,
    vec_ref,
    cs_ref,
    y_ref,
    p_ref,
    small_ref,
    two_ref,
    grad_ref,
    gu_ref,
    gd_ref,
    gb_ref,
    out_ref,
    back_ref,
    g_ref,
    x_buf,
    n1_ref,
    n2_ref,
    cb_ref,
    n2t_ref,
    cbt_ref,
    table_ref,
    vb_ref,
    bq_ref,
    bu_ref,
    gu_buf,
    gd_buf,
    zs,
    zr,
    ds,
    dr,
    vs,
    vr,
    xs,
    xr,
    ls,
):
    me, mz = lax.axis_index("dp"), lax.axis_index("tensor")
    total = count * places
    rows, model = x_ref.shape
    ff = w_ref.shape[2]
    nbits = count.bit_length() - 1
    first = list(range(nbits - 1, -1, -1))
    second = [first[1], first[0]] + first[2:] if nbits >= 3 else first
    turns = list(range(places))
    pairs = [
        tuple((0, t, (first, second)[t % 2]) for t in turns[n : n + 2])
        for n in range(0, places, 2)
    ]
    head_pairs = len(pairs)
    pairs += [((1, t, first), (2, t, second)) for t in turns]
    chunks = [chunk for pair in pairs for chunk in pair]
    numbers, n = [], 0
    for pair in pairs:
        numbers.append(list(range(n, n + len(pair))))
        n += len(pair)

    def source(t):
        return nearest(mz, t, places)

    def source_at(i):
        return sum(same(i, t, places) * source(t) for t in turns)

    def vec_z(s, sending):
        to = (mz + s) % places
        slot = mz if sending else (mz + places - s) % places
        n = nbits + s
        return remote(vec_ref, vb_ref.at[me, slot], vs.at[n], vr.at[n], (me, to))

    def vec_d(b, sending):
        size = 1 << b
        holder = me if sending else flip(me, size)
        held = pl.ds(holder // size * size, size)
        return remote(
            vb_ref.at[held], vb_ref.at[held], vs.at[b], vr.at[b], (flip(me, size), mz)
        )

    def z_copy(a, p, up, own=False):
        src = w_ref.at[a] if own else g_ref.at[a, p, me]
        return remote(
            src,
            g_ref.at[a, p, me],
            zs.at[(a * places + p) * 2 + (0 if up else 1)],
            zr.at[a * places + p],
            (me, mz + 1 if up else mz - 1),
        )

    def pass_on(a, p, own=False):
        @pl.when((p <= mz) & (mz < places - 1))
        def _():
            z_copy(a, p, True, own).start()

        @pl.when((p >= mz) & (mz > 0))
        def _():
            z_copy(a, p, False, own).start()

    def d_copies(j, k, sending):
        a, t, order = chunks[j]
        place = source(t)
        bit = order[k]
        out = []
        for i, m in enumerate(span(order[:k])):
            slot = flip(me, m if sending else m | (1 << bit))
            src = w_ref.at[a] if t == 0 and m == 0 and sending else g_ref.at[a, place, slot]
            n = j * (count - 1) + (1 << k) - 1 + i
            out.append(
                remote(
                    src,
                    g_ref.at[a, place, slot],
                    ds.at[n],
                    dr.at[n],
                    (flip(me, 1 << bit), mz),
                )
            )
        return out

    def step(j, k):
        a, t, _ = chunks[j]
        if k == 0:
            if t > 0:
                p = source(t)
                z_copy(a, p, True).wait_recv()
                pass_on(a, p)
        else:
            for copy in d_copies(j, k - 1, False):
                copy.wait_recv()
        if k < nbits:
            for copy in d_copies(j, k, True):
                copy.start()

    def pair_step(pair, k):
        for j in numbers[pair]:
            if k > 0 or chunks[j][1] > 0:
                step(j, k)

    def x_copy(h, p, sending):
        slot = mz if sending else p
        return remote(
            x_buf.at[p, h],
            y_ref.at[h, slot],
            xs.at[h * places + p],
            xr.at[h * places + slot],
            (me, p),
        )

    def keep_own(h):
        return pltpu.make_async_copy(x_buf.at[mz, h], y_ref.at[h, mz], ls.at[5 + h])

    schedule = []
    for pair in range(len(pairs)):
        head = pair < head_pairs
        for k in range(nbits + 1):
            at = 3 * k + 2 * pair if head else 3 * k + 2 * pair + 2
            schedule.append((at, -k, pair))
    schedule = [(pair, -k) for _, k, pair in sorted(schedule)]
    head_done = max(i for i, (p, k) in enumerate(schedule) if p < head_pairs and k == nbits) + 1
    feed_done = [schedule.index((head_pairs + t, nbits)) + 1 for t in turns]

    def run(low, high):
        for pair, k in schedule[low:high]:
            pair_step(pair, k)

    own = [
        pltpu.make_async_copy(w_ref.at[a], g_ref.at[a, mz, me], ls.at[a]) for a in range(3)
    ]
    own_vec = pltpu.make_async_copy(vec_ref, vb_ref.at[me, mz], ls.at[3])

    for s in range(1, places):
        vec_z(s, True).start()
    own_vec.start()
    own_steps = [n for n, chunk in enumerate(chunks) if chunk[1] == 0]
    step(own_steps[0], 0)
    pass_on(0, mz, True)
    for copy in own:
        copy.start()

    mine = cs_ref[:, pl.ds(pl.multiple_of(mz * rows, rows), rows)]
    for i, table in enumerate(spread_turns(mine)):
        table_ref[i] = table

    own_vec.wait()
    for s in range(1, places):
        vec_z(s, False).wait_recv()
    for b in range(nbits):
        vec_d(b, True).start()
        if b == nbits - 1:
            for j in own_steps[1:]:
                step(j, 0)
            run(0, 2)
            for a in (1, 2):
                pass_on(a, mz, True)
        vec_d(b, False).wait_recv()
    values = vb_ref[...].reshape(total * 8, LANES)
    sub = lax.broadcasted_iota(jnp.int32, (total * 8, 1), 0)
    who, what = sub // 8, sub % 8
    which = lax.broadcasted_iota(jnp.int32, (LANES, 1), 0)

    def pick_of(at):
        return jnp.where(which == at, 1.0, 0.0)

    at = lax.broadcasted_iota(jnp.int32, (1, model), 1)
    kept = select_rows(values, pick_of(at % piece), who == at // piece)
    small_ref[...] = jnp.sum(kept.reshape(total, 8, model), axis=0)
    each = wide // count
    at = lax.broadcasted_iota(jnp.int32, (1, ff), 1)
    kind = at % GROUP // HD
    inner = at // GROUP * HD + at % HD
    kept = select_rows(
        values,
        pick_of(kind * each + inner % each),
        (what == 5) & (kind < 3) & (who // places == inner // each),
    )
    for z in range(places):
        bq_ref[z : z + 1, :] = jnp.sum(
            jnp.where(who % places == z, kept, 0.0), axis=0, keepdims=True
        )
    each = ff // count
    at = lax.broadcasted_iota(jnp.int32, (1, ff), 1)
    kept = select_rows(
        values, pick_of(at % each), (what == 6) & (who // places == at // each)
    )
    for z in range(places):
        bu_ref[z : z + 1, :] = jnp.sum(
            jnp.where(who % places == z, kept, 0.0), axis=0, keepdims=True
        )

    block = rows // 4

    def norm(i):
        here = slice(i * block, (i + 1) * block)
        values = x_ref[here, :]
        center = values - jnp.mean(values, axis=1, keepdims=True)
        inverse = lax.rsqrt(jnp.mean(center * center, axis=1, keepdims=True) + EPSILON)
        normal = center * inverse
        n1_ref[here, :] = (normal * small_ref[0:1, :] + small_ref[1:2, :]).astype(BF)
        second_norm = normal * small_ref[2:3, :] + small_ref[3:4, :]
        n2_ref[here, :] = second_norm.astype(BF)
        n2t_ref[:, here] = second_norm.astype(BF).astype(F32).T.astype(BF)
        cot = cot_ref[here, :]
        cb_ref[here, :] = cot.astype(BF)
        cbt_ref[:, here] = cot.T.astype(BF)

    cuts = [2 + (head_done - 2) * i // 5 for i in range(6)]
    for i in range(5):
        run(cuts[i], cuts[i + 1])
        if i < 4:
            norm(i)
    own[0].wait()
    save = pltpu.make_async_copy(g_ref.at[0], p_ref, ls.at[4])
    save.start()

    heads = ff // GROUP
    before_feed = max(feed_done[0], head_done)
    cuts = [head_done + (before_feed - head_done) * i // places for i in range(places + 1)]

    def project(i, carry):
        for n in range(places):

            @pl.when(i == n)
            def _(n=n):
                run(cuts[n], cuts[n + 1])

        to = source_at((i + 1) % places)
        w = g_ref[0, to].reshape(model, ff)
        forward = dot(n1_ref[...], w, 1, 0) + bq_ref[pl.ds(to, 1), :]
        column = lax.broadcasted_iota(jnp.int32, (rows, LANES), 1)
        for h in range(heads):
            tile = forward[:, h * GROUP : h * GROUP + LANES]
            tile = turn_tiles([tile], table_ref[0], table_ref[1], table_ref[2])[0]
            x_buf[to, h, :, :LANES] = tile.astype(BF)
            late = slice(h * GROUP + LANES, (h + 1) * GROUP)
            backward = dot(cb_ref[...], w[:, late], 1, 0)
            tile = jnp.where(column < HD, forward[:, late], backward)
            x_buf[to, h, :, LANES:] = tile.astype(BF)

        @pl.when(i < places - 1)
        def _():
            for h in range(heads):
                x_copy(h, to, True).start()

        @pl.when(i == places - 1)
        def _():
            for h in range(heads):
                keep_own(h).start()

        return carry

    lax.fori_loop(0, places, project, 0)

    out_ref[...] = jnp.zeros_like(out_ref)
    back_ref[...] = jnp.zeros_like(back_ref)
    own[1].wait()
    own[2].wait()
    width = ff // 2

    def puts(i):
        place = source_at(i)
        return [
            pltpu.make_async_copy(
                buf.at[i], ref.at[place], ls.at[5 + heads + 2 * i + a]
            )
            for a, (buf, ref) in enumerate(((gu_buf, gu_ref), (gd_buf, gd_ref)))
        ]

    def feed(f, carry):
        low = before_feed
        for t in turns:
            high = max(low, feed_done[t])

            @pl.when(f == 2 * t)
            def _(low=low, high=high):
                run(low, high)

            low = high
        i, h = f // 2, f % 2
        place = source_at(i)
        cols = pl.ds(pl.multiple_of(h * width, width), width)
        up = g_ref[1, place, :, :, cols].reshape(model, width)
        down = g_ref[2, place, :, :, cols].reshape(model, width)
        pre = dot(n2_ref[...], up, 1, 0) + bu_ref[pl.ds(place, 1), cols]
        bell = 0.5 * (1.0 + lax.erf(pre * 0.7071067811865476))
        activ = (pre * bell).astype(BF)
        out_ref[...] += dot(activ, down, 1, 1)
        gd_buf[i, :, cols] = dot(cbt_ref[...], activ, 1, 0).astype(BF)
        slope = bell + pre * jnp.exp(-0.5 * pre * pre) * 0.3989422804014327
        grad = dot(cb_ref[...], down, 1, 0) * slope
        gb_ref[pl.ds(place, 1), cols] = jnp.sum(grad, axis=0, keepdims=True)
        grad = grad.astype(BF)
        gu_buf[i, :, cols] = dot(n2t_ref[...], grad, 1, 0).astype(BF)
        back_ref[...] += dot(grad, up, 1, 1)

        @pl.when(h == 1)
        def _():
            for copy in puts(i):
                copy.start()

        return carry

    lax.fori_loop(0, 2 * places, feed, 0)

    saves = [
        pltpu.make_async_copy(buf, ref, ls.at[5 + heads + 2 * places + i])
        for i, (buf, ref) in enumerate(((out_ref, two_ref), (back_ref, grad_ref)))
    ]
    for copy in saves:
        copy.start()
    for copy in [save] + saves:
        copy.wait()
    for i in range(places):
        for copy in puts(i):
            copy.wait()
    for h in range(heads):
        keep_own(h).wait()
        for p in range(places):

            @pl.when(p != mz)
            def _(h=h, p=p):
                x_copy(h, p, False).wait_recv()
                x_copy(h, p, True).wait_send()


    for s in range(1, places):
        vec_z(s, True).wait_send()
    for b in range(nbits):
        vec_d(b, True).wait_send()
    for a in range(3):
        for p in range(places):

            @pl.when((p <= mz) & (mz < places - 1))
            def _(a=a, p=p):
                z_copy(a, p, True).wait_send()

            @pl.when((p >= mz) & (mz > 0))
            def _(a=a, p=p):
                z_copy(a, p, False).wait_send()

    for j in range(len(chunks)):
        for k in range(nbits):
            for copy in d_copies(j, k, True):
                copy.wait_send()


def front(block_input, cotangent, weights, vector, turns, count, places, wide, piece):
    rows, model = block_input.shape
    depth, ff = weights.shape[1:]
    heads = ff // GROUP
    sem = pltpu.SemaphoreType.DMA
    shape = jax.ShapeDtypeStruct
    return pl.pallas_call(
        functools.partial(front_kernel, count, places, wide, piece),
        out_shape=(
            shape((heads, places, rows, GROUP), BF),
            shape((places, count, depth, ff), BF),
            shape((8, model), F32),
            shape((rows, model), F32),
            shape((rows, model), F32),
            shape((places, model, ff), BF),
            shape((places, model, ff), BF),
            shape((places, ff), F32),
        ),
        in_specs=[VMEM] * 5,
        out_specs=(ANY, ANY, VMEM, ANY, ANY, ANY, ANY, VMEM),
        scratch_shapes=[
            pltpu.VMEM((rows, model), F32),
            pltpu.VMEM((rows, model), F32),
            pltpu.VMEM((3, places, count, depth, ff), BF),
            pltpu.VMEM((places, heads, rows, GROUP), BF),
            pltpu.VMEM((rows, model), BF),
            pltpu.VMEM((rows, model), BF),
            pltpu.VMEM((rows, model), BF),
            pltpu.VMEM((model, rows), BF),
            pltpu.VMEM((model, rows), BF),
            pltpu.VMEM((3, rows, LANES), F32),
            pltpu.VMEM((count, places, 8, LANES), F32),
            pltpu.VMEM((places, ff), F32),
            pltpu.VMEM((places, ff), F32),
            pltpu.VMEM((places, model, ff), BF),
            pltpu.VMEM((places, model, ff), BF),
            sem((6 * places,)),
            sem((3 * places,)),
            sem((3 * places * (count - 1),)),
            sem((3 * places * (count - 1),)),
            sem((count.bit_length() + places,)),
            sem((count.bit_length() + places,)),
            sem((heads * places,)),
            sem((heads * places,)),
            sem((7 + heads + 2 * places,)),
        ],
        compiler_params=pltpu.CompilerParams(
            has_side_effects=True, vmem_limit_bytes=VMEM_LIMIT
        ),
        name="front",
    )(block_input, cotangent, weights, vector, turns)


class Scatter:
    def __init__(self, count, places, chunks, sources, acc, landing, sems, local):
        self.me, self.mz = lax.axis_index("dp"), lax.axis_index("tensor")
        self.count, self.places, self.chunks, self.sources = count, places, chunks, sources
        self.acc, self.landing, self.sems, self.local = acc, landing, sems, local
        self.nbits = count.bit_length() - 1

    @staticmethod
    def orders(count):
        nbits = count.bit_length() - 1
        first = list(range(nbits))
        return first, ([first[0], first[2], first[1]] + first[3:] if nbits >= 3 else first)

    def copies(self, j, k):
        a, s, order = self.chunks[j]
        to = (flip(self.me, 1 << order[k]), self.mz)
        half = self.count >> (k + 1)
        base = j * (half_of(self.count) + self.nbits - 1)
        send, recv = self.sems
        if k > 0:
            n = base + half_of(self.count) + k - 1
            src = self.acc.at[j, half : 2 * half]
            return [remote(src, self.landing[k].at[j], send.at[n], recv.at[n], to)]
        place = (self.mz + s) % self.places
        out = []
        for i, m in enumerate(span(order[1:][::-1])):
            slot = flip(self.me, m | (1 << order[0]))
            out.append(
                remote(
                    self.sources[a].at[place, slot],
                    self.landing[0].at[j, i],
                    send.at[base + i],
                    recv.at[base + i],
                    to,
                )
            )
        return out

    def loads(self, j):
        a, s, order = self.chunks[j]
        place = (self.mz + s) % self.places
        return [
            pltpu.make_async_copy(
                self.sources[a].at[place, flip(self.me, m)],
                self.acc.at[j, i],
                self.local.at[j * half_of(self.count) + i],
            )
            for i, m in enumerate(span(order[1:][::-1]))
        ]

    def start(self, j):
        for copy in self.copies(j, 0) + self.loads(j):
            copy.start()

    def stage(self, j, k, final=None):
        if k == 0:
            for copy in self.loads(j):
                copy.wait()
        for copy in self.copies(j, k):
            copy.wait_recv()
        half = self.count >> (k + 1)
        rows = self.acc.shape[2]
        step = 32 if rows % 32 == 0 else rows
        parts = rows // step
        target = self.acc.at[j] if final is None else final

        def body(i, carry):
            shard, at = i // parts, pl.ds(pl.multiple_of(i % parts * step, step), step)
            mine = self.acc[j, shard, at, :].astype(F32)
            other = self.landing[k][j, shard, at, :].astype(F32)
            target[shard, at, :] = (mine + other).astype(BF)
            return carry

        lax.fori_loop(0, half * parts, body, 0)
        if k + 1 < self.nbits:
            for copy in self.copies(j, k + 1):
                copy.start()

    def drain(self):
        for j in range(len(self.chunks)):
            for k in range(self.nbits):
                for copy in self.copies(j, k):
                    copy.wait_send()

    @staticmethod
    def scratch(count, chunks, rows, width):
        nbits = count.bit_length() - 1
        sem = pltpu.SemaphoreType.DMA
        copies = chunks * (half_of(count) + nbits - 1)
        return (
            [pltpu.VMEM((chunks, half_of(count), rows, width), BF)]
            + [pltpu.VMEM((chunks, count >> (k + 1), rows, width), BF) for k in range(nbits)]
            + [sem((copies,)), sem((copies,)), sem((chunks * half_of(count),))]
        )


def half_of(count):
    return count // 2


def middle_kernel(count, places, heads, wq, wk, *refs):
    y_ref, begin_ref, cs_ref, gu_ref, gd_ref, z_ref, bias_ref, red_ref = refs[:8]
    r_buf, qh, kh, vh, oh, kt, vt, s_scr, dq, dk, dv, at_scr, table_ref = refs[8:21]
    ss, rs, ls, acc = refs[21:25]
    nbits = count.bit_length() - 1
    landing = refs[25 : 25 + nbits]
    send, recv, local = refs[25 + nbits :]
    me, mz = lax.axis_index("dp"), lax.axis_index("tensor")
    total = y_ref.shape[1]
    rows = total // places
    scale = HD**-0.5
    nq = total // wq

    chunks = []
    for s in list(range(1, places)) + [0]:
        for a in range(2):
            chunks.append((a, s, Scatter.orders(count)[a]))
    scatter = Scatter(
        count, places, chunks, (gu_ref, gd_ref), acc, landing, (send, recv), local
    )
    events = {}
    last_step = heads * nq
    for k in range(nbits):
        for pair in range(len(chunks) // 2):
            when = (2 + pair // 2, 5 + pair)[k] if k < 2 else 9 + pair + 4 * (k - 2)
            events.setdefault(min(when * nq // 4, last_step), []).append((pair, k))

    def run_events(step):
        for pair, k in events.get(step, []):
            for j in (2 * pair, 2 * pair + 1):
                a, s, _ = chunks[j]
                final = red_ref.at[a, pl.ds(s, 1)] if k == nbits - 1 else None
                scatter.stage(j, k, final)

    for j in range(len(chunks)):
        scatter.start(j)

    def tables(i, carry):
        at = pl.ds(pl.multiple_of(i * wk, wk), wk)
        cosine, low, high = spread_turns(cs_ref[:, at])
        table_ref[0, at, :] = cosine
        table_ref[1, at, :] = -low
        table_ref[2, at, :] = -high
        return carry

    lax.fori_loop(0, total // wk, tables, 0)

    def back_copy(h, s, sending):
        to = (mz + s) % places
        slot = mz if sending else (mz + places - s) % places
        n = h * places + s
        return remote(r_buf.at[h, to], z_ref.at[slot, h], ss.at[n], rs.at[n], (me, to))

    def keep_own(h):
        return pltpu.make_async_copy(r_buf.at[h, mz], z_ref.at[mz, h], ls.at[h])

    def flat(t, carry):
        h, i = t // nq, t % nq
        for step in sorted(events):
            if step < last_step:

                @pl.when(t == step)
                def _(step=step):
                    run_events(step)

        @pl.when(i == 0)
        def _():
            def prepare(b, carry):
                at = pl.ds(pl.multiple_of(b * wk, wk), wk)
                both = y_ref[h, at, :LANES].astype(F32)
                q, k = both[:, :HD] * scale, both[:, HD:]
                both = y_ref[h, at, LANES:].astype(F32)
                v, o = both[:, :HD], both[:, HD:]
                qh[at, :] = q.astype(BF)
                kh[at, :] = k.astype(BF)
                vh[at, :] = v.astype(BF)
                oh[at, :] = o.astype(BF)
                kt[:, at] = k.T.astype(BF)
                vt[:, at] = v.T.astype(BF)
                dk[at, :] = jnp.zeros((wk, HD), F32)
                dv[at, :] = jnp.zeros((wk, HD), F32)
                return carry

            lax.fori_loop(0, total // wk, prepare, 0)

        at = pl.ds(pl.multiple_of(i * wq, wq), wq)
        begin = begin_ref[0:1, at]
        last = i * wq + lax.broadcasted_iota(jnp.int32, (1, wq), 1)
        query, grad = qh[at, :], oh[at, :]
        trips = ((i + 1) * wq + wk - 1) // wk

        def scores(j, peak):
            keys = pl.ds(pl.multiple_of(j * wk, wk), wk)
            place = j * wk + lax.broadcasted_iota(jnp.int32, (wk, wq), 0)
            s = dot(kh[keys, :], query, 1, 1)
            s = jnp.where((place >= begin) & (place <= last), s, NEGATIVE)
            s_scr[keys, :] = s
            return jnp.maximum(peak, jnp.max(s.reshape(wk // 8, 8, wq), axis=0))

        peak = lax.fori_loop(0, trips, scores, jnp.full((8, wq), NEGATIVE, F32))
        peak = jnp.max(peak, axis=0, keepdims=True)

        def weigh(j, state):
            mass, out = state
            keys = pl.ds(pl.multiple_of(j * wk, wk), wk)
            p = jnp.exp(s_scr[keys, :] - peak)
            s_scr[keys, :] = p
            mass = mass + jnp.sum(p.reshape(wk // 8, 8, wq), axis=0)
            return mass, out + dot(vt[:, keys], p.astype(BF), 1, 0)

        mass, out = lax.fori_loop(
            0, trips, weigh, (jnp.zeros((8, wq), F32), jnp.zeros((HD, wq), F32))
        )
        inverse = 1.0 / jnp.sum(mass, axis=0, keepdims=True)
        attended = (out * inverse).astype(BF).astype(F32)
        delta = jnp.sum(attended * grad.astype(F32).T, axis=0, keepdims=True)
        at_scr[at, :] = attended.T

        def back(j, out):
            keys = pl.ds(pl.multiple_of(j * wk, wk), wk)
            p = s_scr[keys, :] * inverse
            dv[keys, :] += dot(p.astype(BF), grad, 1, 0)
            g = dot(vh[keys, :], grad, 1, 1)
            ds = (p * (g - delta)).astype(BF)
            dk[keys, :] += dot(ds, query, 1, 0)
            return out + dot(kt[:, keys], ds, 1, 0)

        out = lax.fori_loop(0, trips, back, jnp.zeros((HD, wq), F32))
        dq[at, :] = (out * scale).T

        @pl.when(i == nq - 1)
        def _():
            per = rows // wk

            def finish(b, sums):
                at = pl.ds(pl.multiple_of(b * wk, wk), wk)
                inside = pl.ds(pl.multiple_of(b % per * wk, wk), wk)
                tile = jnp.concatenate([dq[at, :], dk[at, :]], axis=1)
                tile = turn_tiles(
                    [tile], table_ref[0, at, :], table_ref[1, at, :], table_ref[2, at, :]
                )[0]
                r_buf[h, b // per, inside, :LANES] = tile.astype(BF)
                other = jnp.concatenate([dv[at, :], at_scr[at, :]], axis=1)
                r_buf[h, b // per, inside, LANES:] = other.astype(BF)
                return tuple(
                    total + jnp.sum(x.reshape(wk // 8, 8, LANES), axis=0)
                    for total, x in zip(sums, (tile, other))
                )

            zero = jnp.zeros((8, LANES), F32)
            sums = lax.fori_loop(0, total // wk, finish, (zero, zero))
            for c, value in enumerate(sums):
                bias_ref[h, :, c * LANES : (c + 1) * LANES] = value
            for s in range(1, places):
                back_copy(h, s, True).start()
            keep_own(h).start()

        return carry

    lax.fori_loop(0, last_step, flat, 0)
    run_events(last_step)
    for h in range(heads):
        keep_own(h).wait()
        for s in range(1, places):
            back_copy(h, s, False).wait_recv()
        for s in range(1, places):
            back_copy(h, s, True).wait_send()
    scatter.drain()


def middle(y, begin, turns, up_grad, down_grad):
    heads, total, group = y.shape
    places, count, depth, ff = up_grad.shape
    wq, wk = min(512, total), min(512, total)
    vmem = pltpu.VMEM
    sem = pltpu.SemaphoreType.DMA
    shape = jax.ShapeDtypeStruct
    return pl.pallas_call(
        functools.partial(middle_kernel, count, places, heads, wq, wk),
        out_shape=(
            shape((places, heads, total // places, group), BF),
            shape((heads, 8, group), F32),
            shape((2, places, depth, ff), BF),
        ),
        in_specs=[VMEM, VMEM, VMEM, ANY, ANY],
        out_specs=(ANY, VMEM, VMEM),
        scratch_shapes=[vmem((heads, places, total // places, group), BF)]
        + [vmem((total, HD), BF)] * 4
        + [vmem((HD, total), BF)] * 2
        + [vmem((total, wq), F32)]
        + [vmem((total, HD), F32)] * 4
        + [vmem((3, total, LANES), F32)]
        + [sem((heads * places,)), sem((heads * places,)), sem((heads,))]
        + Scatter.scratch(count, 2 * places, depth, ff),
        compiler_params=pltpu.CompilerParams(
            has_side_effects=True, vmem_limit_bytes=VMEM_LIMIT
        ),
        name="middle",
    )(y, begin, turns, up_grad, down_grad)


def place_rows(values, pick, keep):
    return lax.dot_general(
        jnp.where(keep, values, 0.0),
        pick,
        (((1,), (0,)), ((), ())),
        precision=lax.Precision.HIGHEST,
        preferred_element_type=F32,
    )


def tail_kernel(count, places, wide, piece, *refs):
    x_hbm, cot_hbm, z_hbm, w_hbm, two_hbm, grad_hbm, small_ref, red_ref, qb_ref, gb_ref = refs[:10]
    y_ref, dx_ref, gq_ref, gp_ref, gu_ref, gd_ref, vout_ref = refs[10:17]
    x_ref, cot_ref, z_ref, w_ref, two_ref, grad_ref = refs[17:23]
    normal_ref, inverse_ref, n1t_ref, cbt_ref, out_ref, back_ref, g_ref = refs[23:30]
    sums_ref, vec_ref, zb, vb, zs, zr, vs, vr, ls, acc = refs[30:40]
    nbits = count.bit_length() - 1
    landing = refs[40 : 40 + nbits]
    send, recv, local = refs[40 + nbits :]
    me, mz = lax.axis_index("dp"), lax.axis_index("tensor")
    total = count * places
    rows, model = x_ref.shape
    heads = z_ref.shape[1]
    depth, ff = acc.shape[2:]

    chunks = [
        (0, s, Scatter.orders(count)[i % 2])
        for i, s in enumerate(list(range(1, places)) + [0])
    ]
    scatter = Scatter(count, places, chunks, (g_ref,), acc, landing, (send, recv), local)

    def z_copy(a, s):
        n = a * (places - 1) + s - 1
        src = acc.at[s - 1, 0] if a == 0 else red_ref.at[a - 1, s]
        return remote(src, zb.at[a, s - 1], zs.at[n], zr.at[n], (me, (mz + s) % places))

    def vec_copy(i, sending):
        to = ((me + i // places) % count, (mz + i % places) % places)
        return remote(
            vec_ref.at[to[0] * places + to[1]], vb.at[i], vs.at[i], vr.at[i], to
        )

    def fetch(i):
        at = (mz + 1 + i) % places
        return [
            pltpu.make_async_copy(z_hbm.at[at], z_ref.at[at], ls.at[4 + 2 * i]),
            pltpu.make_async_copy(w_hbm.at[at], w_ref.at[at], ls.at[5 + 2 * i]),
        ]

    inputs = [
        pltpu.make_async_copy(src, dst, ls.at[i])
        for i, (src, dst) in enumerate(
            ((x_hbm, x_ref), (cot_hbm, cot_ref), (two_hbm, two_ref), (grad_hbm, grad_ref))
        )
    ]
    for copy in inputs[:2]:
        copy.start()
    for i in range(places):
        for copy in fetch(i):
            copy.start()
    for copy in inputs[2:]:
        copy.start()
    for s in range(1, places):
        for a in (1, 2):
            z_copy(a, s).start()

    blocks = 4
    block = rows // blocks
    for copy in inputs[:2]:
        copy.wait()
    for i in range(blocks):
        here = slice(i * block, (i + 1) * block)
        values = x_ref[here, :]
        center = values - jnp.mean(values, axis=1, keepdims=True)
        inverse = lax.rsqrt(jnp.mean(center * center, axis=1, keepdims=True) + EPSILON)
        normal = center * inverse
        normal_ref[here, :] = normal
        inverse_ref[here, :] = jnp.broadcast_to(inverse, (block, LANES))
        mixed = normal * small_ref[0:1, :] + small_ref[1:2, :]
        n1t_ref[:, here] = mixed.T.astype(BF)
        cbt_ref[:, here] = cot_ref[here, :].T.astype(BF)
    out_ref[...] = jnp.zeros_like(out_ref)
    back_ref[...] = jnp.zeros_like(back_ref)

    def steps(slot):
        for k in range(nbits - 1, -1, -1):
            pair = slot - k
            for j in (2 * pair, 2 * pair + 1):
                if 0 <= pair and j < len(chunks):
                    scatter.stage(j, k)
                    if k == nbits - 1 and chunks[j][1] > 0:
                        z_copy(0, chunks[j][1]).start()

    left = lax.broadcasted_iota(jnp.int32, (rows, LANES), 1) < HD
    wide_left = lax.broadcasted_iota(jnp.int32, (model, LANES), 1) < HD

    def source(i, carry):
        at = (mz + 1 + i) % places
        for n in range(places):

            @pl.when(i == n)
            def _():
                for copy in fetch(n):
                    copy.wait()

        def head(h, carry):
            z = z_ref[at, h]
            start = pl.multiple_of(h * GROUP, GROUP)
            w = w_ref[at, :, :, pl.ds(start, GROUP)].reshape(model, GROUP)
            late = z[:, LANES:]
            none = jnp.zeros_like(late)
            ours = jnp.concatenate([z[:, :LANES], jnp.where(left, late, none)], axis=1)
            back_ref[...] += dot(ours, w, 1, 1)
            out_ref[...] += dot(jnp.where(left, none, late), w[:, LANES:], 1, 1)
            first = dot(n1t_ref[...], z, 1, 0)
            second = dot(cbt_ref[...], late, 1, 0)
            g_ref[at, :, :, pl.ds(start, LANES)] = (
                first[:, :LANES].astype(BF).reshape(count, depth, LANES)
            )
            second = jnp.where(wide_left, first[:, LANES:], second)
            g_ref[at, :, :, pl.ds(start + LANES, LANES)] = second.astype(BF).reshape(
                count, depth, LANES
            )
            return carry

        lax.fori_loop(0, heads, head, 0)
        for n in range(places):

            @pl.when(i == n)
            def _():
                scatter.start(n)
                if n % 2 == 0 and n > 0:
                    steps(n // 2 - 1)

        return carry

    lax.fori_loop(0, places, source, 0)
    slot = max((places - 1) // 2, 0)
    last = (len(chunks) + 1) // 2 + nbits - 1

    for copy in inputs[2:]:
        copy.wait()
    sums = [jnp.zeros((8, model), F32) for _ in range(5)]

    def norm_rows_back(grad, gain, normal, inverse):
        scaled = grad * gain
        first = jnp.mean(scaled, axis=1, keepdims=True)
        second = jnp.mean(scaled * normal, axis=1, keepdims=True)
        return inverse * (scaled - first - normal * second)

    def fold(values):
        return jnp.sum(values.reshape(block // 8, 8, model), axis=0)

    for i in range(blocks):
        here = slice(i * block, (i + 1) * block)
        normal, inverse = normal_ref[here, :], inverse_ref[here, 0:1]
        cot, one, two = cot_ref[here, :], back_ref[here, :], grad_ref[here, :]
        y_ref[here, :] = (
            x_ref[here, :] + (out_ref[here, :] + two_ref[here, :]) + small_ref[4:5, :]
        )
        dx_ref[here, :] = (
            cot
            + norm_rows_back(one, small_ref[0:1, :], normal, inverse)
            + norm_rows_back(two, small_ref[2:3, :], normal, inverse)
        )
        for r, values in enumerate((one * normal, one, two * normal, two, cot)):
            sums[r] = sums[r] + fold(values)
        if slot < last:
            steps(slot)
            slot += 1
    sums_ref[...] = jnp.zeros_like(sums_ref)
    for r in range(5):
        sums_ref[r : r + 1, :] = jnp.sum(sums[r], axis=0, keepdims=True)

    lane = lax.broadcasted_iota(jnp.int32, (1, ff), 1)
    line = lax.broadcasted_iota(jnp.int32, (ff, 1), 0)
    out_lane = lax.broadcasted_iota(jnp.int32, (1, LANES), 1)
    sub = lax.broadcasted_iota(jnp.int32, (total * 8, 1), 0)
    who, what = sub // 8, sub % 8
    spread = jnp.broadcast_to(sums_ref[...][None], (total, 8, model)).reshape(total * 8, model)
    parts = place_rows(
        spread,
        jnp.where(line % piece == out_lane, 1.0, 0.0),
        (what < 5) & (who == lane // piece),
    )
    each = wide // count
    kind, inner = lane % GROUP // HD, lane // GROUP * HD + lane % HD
    kind_line, inner_line = line % GROUP // HD, line // GROUP * HD + line % HD
    qkv = jnp.concatenate(
        [jnp.sum(qb_ref[h], axis=0, keepdims=True) for h in range(heads)], axis=1
    )
    parts += place_rows(
        jnp.broadcast_to(qkv, (total * 8, ff)),
        jnp.where(kind_line * each + inner_line % each == out_lane, 1.0, 0.0),
        (what == 5) & (kind < 3) & (who == inner // each * places + mz),
    )
    each = ff // count
    up = jnp.zeros((total * 8, ff), F32)
    for z in range(places):
        up = jnp.where(who % places == z, gb_ref[z : z + 1, :], up)
    parts += place_rows(
        up,
        jnp.where(line % each == out_lane, 1.0, 0.0),
        (what == 6) & (who // places == lane // each),
    )
    vec_ref[...] = parts.reshape(total, 8, LANES)

    def send_vec(i, carry):
        vec_copy(i, True).start()
        return carry

    lax.fori_loop(1, total, send_vec, 0)
    own_vec = pltpu.make_async_copy(vec_ref.at[me * places + mz], vb.at[0], ls.at[4 + 2 * places])
    own_vec.start()
    while slot < last:
        steps(slot)
        slot += 1

    own_vec.wait()

    def wait_vec(i, carry):
        vec_copy(i, False).wait_recv()
        vec_copy(i, True).wait_send()
        return carry

    lax.fori_loop(1, total, wait_vec, 0)
    vout_ref[...] = jnp.sum(vb[...], axis=0)
    for a in (1, 2, 0):
        for s in range(1, places):
            z_copy(a, s).wait_recv()
        own = acc[places - 1, 0] if a == 0 else red_ref[a - 1, 0]
        result = own.astype(F32)
        for s in range(1, places):
            result = result + zb[a, s - 1].astype(F32)
        if a == 1:
            gu_ref[...] = result
        elif a == 2:
            gd_ref[...] = result.T
        else:
            for h in range(heads):
                for c, ref in enumerate((gq_ref.at[0], gq_ref.at[1], gq_ref.at[2])):
                    ref[:, h * HD : (h + 1) * HD] = result[
                        :, h * GROUP + c * HD : h * GROUP + (c + 1) * HD
                    ]
                gp_ref[h * HD : (h + 1) * HD, :] = result[
                    :, h * GROUP + 3 * HD : (h + 1) * GROUP
                ].T
    scatter.drain()
    for a in range(3):
        for s in range(1, places):
            z_copy(a, s).wait_send()


def tail(x, cot, z, w, two, grad, small, partly, qkv_sums, up_sums, wide, piece):
    places, heads, rows, group = z.shape
    count, depth, ff = w.shape[1:]
    model = x.shape[1]
    total = count * places
    sem = pltpu.SemaphoreType.DMA
    shape = jax.ShapeDtypeStruct
    vmem = pltpu.VMEM
    return pl.pallas_call(
        functools.partial(tail_kernel, count, places, wide, piece),
        out_shape=(
            shape((rows, model), F32),
            shape((rows, model), F32),
            shape((3, depth, wide), F32),
            shape((wide, depth), F32),
            shape((depth, ff), F32),
            shape((ff, depth), F32),
            shape((8, LANES), F32),
        ),
        in_specs=[ANY] * 6 + [VMEM] * 4,
        out_specs=(VMEM,) * 7,
        scratch_shapes=[
            vmem((rows, model), F32),
            vmem((rows, model), F32),
            vmem((places, heads, rows, group), BF),
            vmem((places, count, depth, ff), BF),
            vmem((rows, model), F32),
            vmem((rows, model), F32),
            vmem((rows, model), F32),
            vmem((rows, LANES), F32),
            vmem((model, rows), BF),
            vmem((model, rows), BF),
            vmem((rows, model), F32),
            vmem((rows, model), F32),
            vmem((places, count, depth, ff), BF),
            vmem((8, model), F32),
            vmem((total, 8, LANES), F32),
            vmem((3, places - 1, depth, ff), BF),
            vmem((total, 8, LANES), F32),
            sem((3 * (places - 1),)),
            sem((3 * (places - 1),)),
            sem((total,)),
            sem((total,)),
            sem((5 + 2 * places,)),
        ]
        + Scatter.scratch(count, places, depth, ff),
        compiler_params=pltpu.CompilerParams(
            has_side_effects=True, vmem_limit_bytes=VMEM_LIMIT
        ),
        name="tail",
    )(x, cot, z, w, two, grad, small, partly, qkv_sums, up_sums)


def lanes(values, width=LANES):
    return jnp.pad(values, [(0, 0)] * (values.ndim - 1) + [(0, width - values.shape[-1])])


def shards(
    count,
    places,
    block_input,
    cotangent,
    segment_ids,
    token_offset,
    first_gain,
    first_shift,
    second_gain,
    second_shift,
    qkv_weight,
    qkv_bias,
    proj_weight,
    up_weight,
    up_bias,
    down_weight,
    out_bias,
):
    rows, model = block_input.shape
    depth = qkv_weight.shape[1]
    wide = qkv_weight.shape[2]
    heads = wide // HD
    ff = up_weight.shape[1]
    piece = first_gain.shape[0]
    total = segment_ids.shape[0]

    attn = jnp.stack([qkv_weight[0], qkv_weight[1], qkv_weight[2], proj_weight.T])
    attn = attn.reshape(4, depth, heads, HD).transpose(1, 2, 0, 3).reshape(depth, 4 * wide)
    packed = jnp.stack([attn, up_weight, down_weight.T])
    vector = jnp.stack(
        [lanes(v) for v in (first_gain, first_shift, second_gain, second_shift, out_bias)]
        + [lanes(qkv_bias.astype(F32).reshape(-1)), lanes(up_bias.astype(F32))]
        + [jnp.zeros((LANES,), F32)]
    )
    turns = rotary_turns(token_offset)
    begin = (jnp.arange(total, dtype=jnp.int32) - token_offset)[None, :]
    y, attn_weights, small, out_two, grad_two, up_grad, down_grad, up_bias_part = front(
        block_input, cotangent, packed, vector, turns, count, places, wide, piece
    )
    z, qkv_bias_part, partly = middle(
        y.reshape(heads, total, GROUP),
        begin,
        turns,
        up_grad.reshape(places, count, depth, ff),
        down_grad.reshape(places, count, depth, ff),
    )
    block_output, input_grad, gq, gp, gu, gd, vec = tail(
        block_input,
        cotangent,
        z,
        attn_weights,
        out_two,
        grad_two,
        small,
        partly,
        qkv_bias_part,
        up_bias_part,
        wide,
        piece,
    )
    return (
        block_output,
        input_grad,
        vec[0, :piece],
        vec[1, :piece],
        vec[2, :piece],
        vec[3, :piece],
        gq,
        vec[5, : 3 * wide // count].reshape(3, wide // count),
        gp,
        gu,
        vec[6, : ff // count],
        gd,
        vec[4, :piece],
    )


def solution(mesh):
    both = P(("dp", "tensor"))
    return jax.shard_map(
        functools.partial(shards, mesh.shape["dp"], mesh.shape["tensor"]),
        mesh=mesh,
        in_specs=(
            P(("dp", "tensor"), None),
            P(("dp", "tensor"), None),
            P("dp"),
            P("dp"),
            both,
            both,
            both,
            both,
            P(None, "dp", "tensor"),
            P(None, ("tensor", "dp")),
            P("tensor", "dp"),
            P("dp", "tensor"),
            P(("tensor", "dp")),
            P("tensor", "dp"),
            both,
        ),
        out_specs=(
            P(("dp", "tensor"), None),
            P(("dp", "tensor"), None),
            both,
            both,
            both,
            both,
            P(None, "dp", "tensor"),
            P(None, ("tensor", "dp")),
            P("tensor", "dp"),
            P("dp", "tensor"),
            P(("tensor", "dp")),
            P("tensor", "dp"),
            both,
        ),
        check_vma=False,
    )
```
